32 devices in a mesh: dp: 2 (over x), tp: 4 (over z), cp: 4 (over y, core).
Axes of the slice: x: 2, y: 2, z: 4, core: 2. Of those that a mesh axis runs over, the one named last changes fastest.
Arguments:
- tokens: bfloat16 [6144, 3584], P(('dp', 'tp', 'cp')), parts along dimension 0
- norm_attn: bfloat16 [2, 3584], replicated
- norm_mlp: bfloat16 [2, 3584], replicated
- w_q: bfloat16 [2, 3584, 28, 128], P(None, None, 'tp')
- w_k: bfloat16 [2, 3584, 512], P(None, None, 'tp')
- w_v: bfloat16 [2, 3584, 512], P(None, None, 'tp')
- w_o: bfloat16 [2, 28, 128, 3584], P(None, 'tp')
- w_gate: bfloat16 [2, 3584, 18944], P(None, None, 'tp')
- w_up: bfloat16 [2, 3584, 18944], P(None, None, 'tp')
- w_down: bfloat16 [2, 18944, 3584], P(None, 'tp')
Outputs:
- output: bfloat16 [6144, 3584], P(('dp', 'tp', 'cp')), parts along dimension 0
There are 2 independent parts. The reference program is written for one: setup_inputs(seed, part) draws one part's arguments, and reference() takes and returns one part's arrays. A program takes and returns all parts, laid end to end along the dimension named above; an argument that names none is the same for every part.
All inputs are finite; a program needn't handle non-finite values.
Results may differ from the reference program's by a relative error of at most 0.02.
Values are sent between devices in bfloat16 or wider.
A program may use at most 1 GiB of HBM per device.

```python
import math
import jax
import jax.numpy as jnp
from jax import lax

D = 3584
FF = 18944
HEADS = 28
KV_HEADS = 4
HEAD = 128
SEQ = 3072
SEGMENT = 96
LAYERS = 2

GROUP = HEADS // KV_HEADS
GROUP_DEVICES = SEQ // (2 * SEGMENT)


def row_positions():
    row_idx = jnp.arange(SEQ)
    device_idx = row_idx // (2 * SEGMENT)
    offset = row_idx % (2 * SEGMENT)
    seg_idx = jnp.where(offset < SEGMENT, device_idx, 2 * GROUP_DEVICES - 1 - device_idx)
    return seg_idx * SEGMENT + offset % SEGMENT


def rms_norm(hidden, gain):
    hidden_f = hidden.astype(jnp.float32)
    inv_rms = lax.rsqrt(jnp.mean(hidden_f * hidden_f, axis=-1, keepdims=True) + 1e-5)
    return (hidden_f * inv_rms * gain.astype(jnp.float32)).astype(jnp.bfloat16)


def rotary(values, positions):
    half_dim = values.shape[-1] // 2
    inv_freq = 500000.0 ** (-(jnp.arange(half_dim, dtype=jnp.float32) * 2.0 / values.shape[-1]))
    angles = positions.astype(jnp.float32)[:, None] * inv_freq[None, :]
    cos_ang = jnp.cos(angles)[:, None, :]
    sin_ang = jnp.sin(angles)[:, None, :]
    first = values[..., :half_dim]
    second = values[..., half_dim:]
    return jnp.concatenate([first * cos_ang - second * sin_ang, second * cos_ang + first * sin_ang], axis=-1)


def attention(queries, keys, value_rows, positions):
    keys_f = keys.astype(jnp.float32)
    values_f = value_rows.astype(jnp.float32)
    q_blocks = queries.reshape(SEQ // SEGMENT, SEGMENT, KV_HEADS, GROUP, HEAD)
    pos_blocks = positions.reshape(SEQ // SEGMENT, SEGMENT)
    scale = 1.0 / math.sqrt(HEAD)

    def one_block(block):
        q_blk, pos_blk = block
        scores = jnp.einsum('bkgd,tkd->bkgt', q_blk.astype(jnp.float32), keys_f) * scale
        visible = positions[None, None, None, :] <= pos_blk[:, None, None, None]
        scores = jnp.where(visible, scores, -jnp.inf)
        row_max = jnp.max(scores, axis=-1, keepdims=True)
        weights = jnp.exp(scores - row_max)
        row_sum = jnp.sum(weights, axis=-1, keepdims=True)
        mixed = jnp.einsum('bkgt,tkd->bkgd', weights.astype(jnp.bfloat16).astype(jnp.float32), values_f)
        return (mixed / row_sum).astype(jnp.bfloat16)

    return lax.map(one_block, (q_blocks, pos_blocks)).reshape(SEQ, HEADS * HEAD)


def layer(hidden, params, positions):
    norm_attn, norm_mlp, w_q, w_k, w_v, w_o, w_gate, w_up, w_down = params
    normed = rms_norm(hidden, norm_attn)
    q_proj = jnp.dot(normed, w_q.reshape(D, HEADS * HEAD), preferred_element_type=jnp.float32)
    queries = rotary(q_proj.reshape(SEQ, HEADS, HEAD), positions).astype(jnp.bfloat16)
    k_proj = jnp.dot(normed, w_k, preferred_element_type=jnp.float32)
    keys = rotary(k_proj.reshape(SEQ, KV_HEADS, HEAD), positions).astype(jnp.bfloat16)
    value_rows = jnp.dot(normed, w_v, preferred_element_type=jnp.float32).astype(jnp.bfloat16).reshape(SEQ, KV_HEADS, HEAD)
    mixed = attention(queries.reshape(SEQ, KV_HEADS, GROUP, HEAD), keys, value_rows, positions)
    attn_out = jnp.dot(mixed, w_o.reshape(HEADS * HEAD, D), preferred_element_type=jnp.float32)
    hidden_mid = (hidden.astype(jnp.float32) + attn_out).astype(jnp.bfloat16)
    normed_mlp = rms_norm(hidden_mid, norm_mlp)
    gate_pre = jnp.dot(normed_mlp, w_gate, preferred_element_type=jnp.float32)
    up_proj = jnp.dot(normed_mlp, w_up, preferred_element_type=jnp.float32)
    hidden_act = (jax.nn.silu(gate_pre) * up_proj).astype(jnp.bfloat16)
    mlp_out = jnp.dot(hidden_act, w_down, preferred_element_type=jnp.float32)
    return (hidden_mid.astype(jnp.float32) + mlp_out).astype(jnp.bfloat16)


def setup_inputs(seed: int = 0, part: int = 0) -> dict:
    key_list = jax.random.split(jax.random.key(seed), 10)
    score_gain = math.sqrt(max(math.log(SEQ) - 2.0, 1.0))
    tokens = jax.random.normal(jax.random.fold_in(key_list[0], part), (SEQ, D), jnp.float32)
    norm_attn = 1.0 + 0.3 * jax.random.normal(key_list[1], (LAYERS, D), jnp.float32)
    norm_mlp = 1.0 + 0.3 * jax.random.normal(key_list[2], (LAYERS, D), jnp.float32)
    w_q = jax.random.normal(key_list[3], (LAYERS, D, HEADS, HEAD), jnp.float32) * (score_gain / math.sqrt(D))
    w_k = jax.random.normal(key_list[4], (LAYERS, D, KV_HEADS * HEAD), jnp.float32) / math.sqrt(D)
    w_v = jax.random.normal(key_list[5], (LAYERS, D, KV_HEADS * HEAD), jnp.float32) / math.sqrt(D)
    w_o = jax.random.normal(key_list[6], (LAYERS, HEADS, HEAD, D), jnp.float32) / math.sqrt(HEADS * HEAD)
    w_gate = jax.random.normal(key_list[7], (LAYERS, D, FF), jnp.float32) / math.sqrt(D)
    w_up = jax.random.normal(key_list[8], (LAYERS, D, FF), jnp.float32) / math.sqrt(D)
    w_down = jax.random.normal(key_list[9], (LAYERS, FF, D), jnp.float32) * (1.5 / math.sqrt(FF))
    return dict(
        tokens=tokens.astype(jnp.bfloat16),
        norm_attn=norm_attn.astype(jnp.bfloat16),
        norm_mlp=norm_mlp.astype(jnp.bfloat16),
        w_q=w_q.astype(jnp.bfloat16),
        w_k=w_k.astype(jnp.bfloat16),
        w_v=w_v.astype(jnp.bfloat16),
        w_o=w_o.astype(jnp.bfloat16),
        w_gate=w_gate.astype(jnp.bfloat16),
        w_up=w_up.astype(jnp.bfloat16),
        w_down=w_down.astype(jnp.bfloat16),
    )


def reference(tokens, norm_attn, norm_mlp, w_q, w_k, w_v, w_o, w_gate, w_up, w_down):
    positions = row_positions()

    def layer_step(hidden, params):
        return layer(hidden, params, positions), None

    stacked = (norm_attn, norm_mlp, w_q, w_k, w_v, w_o, w_gate, w_up, w_down)
    return lax.scan(layer_step, tokens, stacked)[0]
```

```python
import functools
import math
import jax
import jax.numpy as jnp
from jax import lax
from jax.experimental import pallas as pl
from jax.experimental.pallas import tpu as pltpu
from jax.sharding import PartitionSpec as P


F32 = jnp.float32
BF16 = jnp.bfloat16


def normed(x, gain):
    xf = x.astype(F32)
    inv = lax.rsqrt(jnp.mean(xf * xf, axis=-1, keepdims=True) + 1e-5)
    return (xf * inv * gain.astype(F32)).astype(BF16)


def fetch(z, n, p, own, ups, dns, src_of, dst, sem):
    @pl.when(z == p)
    def _():
        pltpu.make_async_copy(src_of(own), dst, sem).start()

    for k in range(1, n):
        if p + k < n:
            @pl.when(z == p + k)
            def _(k=k):
                pltpu.make_async_copy(src_of(ups[k - 1]), dst, sem).start()
        if p - k >= 0:
            @pl.when(z == p - k)
            def _(k=k):
                pltpu.make_async_copy(src_of(dns[k - 1]), dst, sem).start()


def rows_kernel(n, z_ref, gain_ref, own, *rest):
    ups, dns = rest[: n - 1], rest[n - 1 : 2 * (n - 1)]
    a_ref, cols_ref, buf, sems = rest[2 * (n - 1) :]
    z = z_ref[0]
    step = pl.program_id(0)

    @pl.when(step == 0)
    def _():
        for p in range(n):
            fetch(z, n, p, own, ups, dns, lambda r: r, buf.at[p], sems.at[p])

    pltpu.make_async_copy(own, buf.at[step], sems.at[step]).wait()
    x = buf[step]
    a_ref[0] = normed(x, gain_ref[...])
    width = cols_ref.shape[-1]
    cols_ref[0] = buf[step, :, pl.ds(pl.multiple_of(z * width, 128), width)]


def gather_rows_norm(z, gain, own, ups, dns):
    n = len(ups) + 1
    rows, d = own.shape
    width = d // n
    return pl.pallas_call(
        functools.partial(rows_kernel, n),
        grid=(n,),
        out_shape=(jax.ShapeDtypeStruct((n, rows, d), BF16), jax.ShapeDtypeStruct((n, rows, width), BF16)),
        in_specs=[pl.BlockSpec(memory_space=pltpu.SMEM), pl.BlockSpec((1, d), lambda i: (0, 0))]
        + [pl.BlockSpec(memory_space=pl.ANY)] * (2 * n - 1),
        out_specs=(pl.BlockSpec((1, rows, d), lambda i: (i, 0, 0)), pl.BlockSpec((1, rows, width), lambda i: (i, 0, 0))),
        scratch_shapes=[pltpu.VMEM((n, rows, d), BF16), pltpu.SemaphoreType.DMA((n,))],
        compiler_params=pltpu.CompilerParams(vmem_limit_bytes=24 << 20),
        cost_estimate=pl.CostEstimate(flops=8 * n * rows * d, bytes_accessed=5 * n * rows * d, transcendentals=0),
        name="gather_rows_norm",
    )(z, gain, own, *ups, *dns)


def cols_kernel(n, z_ref, gain_ref, own, *rest):
    ups, dns = rest[: n - 1], rest[n - 1 : 2 * (n - 1)]
    b_ref, home_ref, buf, sems = rest[2 * (n - 1) :]
    z = z_ref[0]
    step = pl.program_id(0)
    width = own.shape[-1]

    @pl.when(step == 0)
    def _():
        for r in range(n):
            for p in range(n):
                fetch(z, n, p, own, ups, dns, lambda ref, r=r: ref.at[r], buf.at[r, :, pl.ds(p * width, width)], sems.at[r])

    for _ in range(n):
        pltpu.make_async_copy(own.at[step], buf.at[step, :, pl.ds(0, width)], sems.at[step]).wait()
    x = buf[step]
    b_ref[0] = normed(x, gain_ref[...])

    @pl.when(step == z)
    def _():
        home_ref[...] = x


def gather_cols_norm(z, gain, own, ups, dns):
    n = len(ups) + 1
    _, rows, width = own.shape
    d = width * n
    return pl.pallas_call(
        functools.partial(cols_kernel, n),
        grid=(n,),
        out_shape=(jax.ShapeDtypeStruct((n, rows, d), BF16), jax.ShapeDtypeStruct((rows, d), BF16)),
        in_specs=[pl.BlockSpec(memory_space=pltpu.SMEM), pl.BlockSpec((1, d), lambda i: (0, 0))]
        + [pl.BlockSpec(memory_space=pl.ANY)] * (2 * n - 1),
        out_specs=(pl.BlockSpec((1, rows, d), lambda i: (i, 0, 0)), pl.BlockSpec((rows, d), lambda i: (0, 0))),
        scratch_shapes=[pltpu.VMEM((n, rows, d), BF16), pltpu.SemaphoreType.DMA((n,))],
        compiler_params=pltpu.CompilerParams(vmem_limit_bytes=24 << 20),
        cost_estimate=pl.CostEstimate(flops=8 * n * rows * d, bytes_accessed=5 * n * rows * d, transcendentals=0),
        name="gather_cols_norm",
    )(z, gain, own, *ups, *dns)


def attention_kernel(n, slots, heads, low, c_ref, q_ref, cos_ref, sin_ref, *rest):
    n_kv = slots if low else 2 * slots
    kv_refs = rest[:n_kv]
    o_ref, qs, ks, vs, m_ref, l_ref, acc = rest[n_kv:]
    plane = pl.program_id(0)
    c = c_ref[0]
    rows = q_ref.shape[1]
    hd = qs.shape[1]
    to_log2 = math.log2(math.e) / math.sqrt(hd)

    @pl.when(plane == 0)
    def _():
        for i in range(n_kv):
            half, s = divmod(i, slots)
            for g in range(n):
                ks[half * n + g, s * rows : (s + 1) * rows] = kv_refs[i][g, :, :hd]
                vs[half * n + g, s * rows : (s + 1) * rows] = kv_refs[i][g, :, hd:]

    cos = cos_ref[0]
    sin = sin_ref[0]
    for h in range(heads):
        qh = q_ref[0, :, h * hd : (h + 1) * hd]
        turned = qh * cos + pltpu.roll(qh, hd // 2, 1) * sin
        qs[h * rows : (h + 1) * rows] = turned.astype(BF16)

    def scores(j):
        return lax.dot_general(qs[...], ks[j], (((1,), (1,)), ((), ())), preferred_element_type=F32)

    diag = plane if low else n + plane
    s = scores(diag)
    shape = (rows, slots * rows)
    row = lax.broadcasted_iota(jnp.int32, shape, 0)
    col = lax.broadcasted_iota(jnp.int32, shape, 1)
    slot = col // rows
    other = lax.rem(c - slot + slots, slots)
    limit = jnp.where(slot == 0, row, jnp.where((other < c) if low else (other > c), slots * rows, -1))
    bias = jnp.where(col <= limit, 0.0, -jnp.inf)
    s = (s.reshape(heads, rows, slots * rows) + bias[None]).reshape(heads * rows, slots * rows)
    m = jnp.max(s, axis=-1, keepdims=True)
    e = jnp.exp2(s * to_log2 - m * to_log2)
    m_ref[...] = m
    l_ref[...] = jnp.sum(e, axis=-1, keepdims=True)
    acc[...] = jnp.dot(e.astype(BF16), vs[diag], preferred_element_type=F32)

    @pl.loop(0, plane if low else 2 * n - 1 - plane)
    def _(i):
        j = i if low else i + jnp.where(i >= n, plane + 1, 0)
        s = scores(j)
        old = m_ref[...]
        m = jnp.maximum(old, jnp.max(s, axis=-1, keepdims=True))
        alpha = jnp.exp2((old - m) * to_log2)
        e = jnp.exp2(s * to_log2 - m * to_log2)
        m_ref[...] = m
        l_ref[...] = l_ref[...] * alpha + jnp.sum(e, axis=-1, keepdims=True)
        acc[...] = acc[...] * alpha + jnp.dot(e.astype(BF16), vs[j], preferred_element_type=F32)

    out = (acc[...] / l_ref[...]).astype(BF16)
    for h in range(heads):
        o_ref[0, :, h * hd : (h + 1) * hd] = out[h * rows : (h + 1) * rows]


def attention(c, q, cos, sin, kvs, low, slots, hd):
    n, rows, width = q.shape
    heads = width // hd
    blocks = n * (n + 1) // 2 if low else n * n + n * (n + 1) // 2
    work = blocks * heads * rows * slots * rows
    return pl.pallas_call(
        functools.partial(attention_kernel, n, slots, heads, low),
        grid=(n,),
        out_shape=jax.ShapeDtypeStruct((n, rows, width), BF16),
        in_specs=[
            pl.BlockSpec(memory_space=pltpu.SMEM),
            pl.BlockSpec((1, rows, width), lambda i: (i, 0, 0)),
            pl.BlockSpec((1, rows, hd), lambda i: (i, 0, 0)),
            pl.BlockSpec((1, rows, hd), lambda i: (i, 0, 0)),
        ]
        + [pl.BlockSpec((n, rows, 2 * hd), lambda i: (0, 0, 0))] * len(kvs),
        out_specs=pl.BlockSpec((1, rows, width), lambda i: (i, 0, 0)),
        scratch_shapes=[
            pltpu.VMEM((heads * rows, hd), BF16),
            pltpu.VMEM((2 * n, slots * rows, hd), BF16),
            pltpu.VMEM((2 * n, slots * rows, hd), BF16),
            pltpu.VMEM((heads * rows, 1), F32),
            pltpu.VMEM((heads * rows, 1), F32),
            pltpu.VMEM((heads * rows, hd), F32),
        ],
        compiler_params=pltpu.CompilerParams(vmem_limit_bytes=32 << 20),
        cost_estimate=pl.CostEstimate(flops=16 * work * hd, bytes_accessed=8 * n * rows * width, transcendentals=work),
        name="attention_low" if low else "attention_high",
    )(c, q, cos, sin, *kvs)


def solution(mesh):
    n = mesh.shape['tp']
    slots = mesh.shape['cp']
    segs = n * slots
    row_spec = P(('dp', 'tp', 'cp'), None)
    gain_spec = P(None, None)
    q_spec = P(None, None, 'tp', None)
    col_spec = P(None, None, 'tp')
    o_spec = P(None, 'tp', None, None)
    down_spec = P(None, 'tp', None)

    def up_pairs(lo, hi):
        return [(i, i + 1) for i in range(lo, hi)]

    def down_pairs(lo, hi):
        return [(i + 1, i) for i in range(lo, hi)]

    def line_gather(own):
        ups, dns = [], []
        up = down = own
        for k in range(1, n):
            up = lax.ppermute(up, 'tp', up_pairs(k - 1, n - 1))
            down = lax.ppermute(down, 'tp', down_pairs(0, n - k))
            ups.append(up)
            dns.append(down)
        return ups, dns

    def line_scatter(part, z):
        def block(i):
            return lax.dynamic_index_in_dim(part, lax.rem(i + 2 * n, n), 0, keepdims=False)

        up = down = None
        for t in range(1, n):
            up_out = block(z - t)
            down_out = block(z + t)
            if t > 1:
                up_out = up_out + up
                down_out = down_out + down
            up = lax.ppermute(up_out, 'tp', up_pairs(0, t))
            down = lax.ppermute(down_out, 'tp', down_pairs(n - 1 - t, n - 1))
        return block(z), up, down

    def body(tokens, norm_attn, norm_mlp, w_q, w_k, w_v, w_o, w_gate, w_up, w_down):
        rows = tokens.shape[0] // 2
        layers, d, heads, hd = w_q.shape
        width = d // n
        z = lax.axis_index('tp')
        c = lax.axis_index('cp')
        z_arr = z.astype(jnp.int32).reshape(1)
        c_arr = c.astype(jnp.int32).reshape(1)

        inv_freq = 500000.0 ** (-(jnp.arange(hd // 2, dtype=F32) * 2.0 / hd))
        tables = []
        for low in (True, False):
            seg = jnp.arange(n) * slots + c
            if not low:
                seg = 2 * segs - 1 - seg
            pos = seg[:, None] * rows + jnp.arange(rows)[None, :]
            angle = pos.astype(F32)[..., None] * inv_freq
            cos, sin = jnp.cos(angle), jnp.sin(angle)
            tables.append((jnp.concatenate([cos, cos], -1), jnp.concatenate([-sin, sin], -1)))

        def reshard_wo(layer):
            wo = w_o[layer].reshape(heads * hd, d)
            part = heads * hd // slots
            out = [lax.dynamic_slice(wo, (0, z * width), (heads * hd, width))]
            for s in range(1, n):
                to = lax.rem(z + s, n)
                mine = lax.dynamic_slice(wo, (c * part, to * width), (part, width))
                got = lax.ppermute(mine, 'tp', [(i, (i + s) % n) for i in range(n)])
                out.append(lax.all_gather(got, 'cp', axis=0, tiled=True))
            return out

        wos = [reshard_wo(layer) for layer in range(layers)]
        wqs = [w_q[layer].reshape(d, heads * hd) for layer in range(layers)]
        wkvs = [jnp.concatenate([w_k[layer], w_v[layer]], axis=1) for layer in range(layers)]

        def front(layer, half, x, kv_low):
            cos, sin = tables[half]
            ups, dns = line_gather(x)
            a, x_cols = gather_rows_norm(z_arr, norm_attn[layer][None], x, ups, dns)
            a = a.reshape(n * rows, d)
            kv = jnp.dot(a, wkvs[layer], preferred_element_type=F32).reshape(n, rows, 2 * hd)
            k = kv[..., :hd]
            k = k * cos + jnp.roll(k, hd // 2, axis=-1) * sin
            kv = jnp.concatenate([k, kv[..., hd:]], axis=-1).astype(BF16)
            kvs = [kv] + [lax.ppermute(kv, 'cp', [(i, (i + s) % slots) for i in range(slots)]) for s in range(1, slots)]
            q = jnp.dot(a, wqs[layer], preferred_element_type=F32).reshape(n, rows, heads * hd)
            o = attention(c_arr, q, cos, sin, (kv_low or []) + kvs, half == 0, slots, hd)
            return o, x_cols, kvs

        def middle(layer, o, x_cols):
            ups, dns = line_gather(o)
            pieces = [o] + [jnp.where(z >= k, ups[k - 1], dns[n - k - 1]) for k in range(1, n)]
            total = x_cols.astype(F32)
            for piece, w in zip(pieces, wos[layer]):
                total = total + jnp.einsum('nrk,kd->nrd', piece, w, preferred_element_type=F32)
            h = total.astype(BF16)
            ups, dns = line_gather(h)
            return gather_cols_norm(z_arr, norm_mlp[layer][None], h, ups, dns)

        def back(layer, b, h_home):
            b = b.reshape(n * rows, d)
            gate = jnp.dot(b, w_gate[layer], preferred_element_type=F32)
            up = jnp.dot(b, w_up[layer], preferred_element_type=F32)
            act = (jax.nn.silu(gate) * up).astype(BF16)
            part = jnp.dot(act, w_down[layer], preferred_element_type=F32).reshape(n, rows, d)
            mine, from_up, from_down = line_scatter(part, z)
            return (h_home.astype(F32) + mine + from_up + from_down).astype(BF16)

        xs = [tokens[:rows], tokens[rows:]]
        for layer in range(layers):
            kv_low = None
            for half in range(2):
                o, x_cols, kvs = front(layer, half, xs[half], kv_low)
                if half == 0:
                    kv_low = kvs
                b, h_home = middle(layer, o, x_cols)
                xs[half] = back(layer, b, h_home)
        return jnp.concatenate(xs, axis=0)

    return jax.shard_map(
        body,
        mesh=mesh,
        in_specs=(row_spec, gain_spec, gain_spec, q_spec, col_spec, col_spec, o_spec, col_spec, col_spec, down_spec),
        out_specs=row_spec,
        check_vma=False,
    )
```

```python
import functools
import math
import jax
import jax.numpy as jnp
from jax import lax
from jax.experimental import pallas as pl
from jax.experimental.pallas import tpu as pltpu
from jax.sharding import PartitionSpec as P

F32 = jnp.float32
BF16 = jnp.bfloat16
MESH = pl.DeviceIdType.MESH
UP, DOWN = 0, 1
X, O, H = 0, 1, 2
LOW, HIGH = 0, 1
SLOTS = 3
PARTS = 2
TILE = 256


def ring(i, n):
    return lax.rem(i + n, n)


def both(*conditions):
    out = conditions[0]
    for c in conditions[1:]:
        out = jnp.logical_and(out, c)
    return out


def kernel(n, m, layers, tokens, gain_a, gain_m, cos_ref, sin_ref, w_q, w_k, w_v, w_o, w_gate, w_up, w_down,
           y_out, g_x, g_o, g_h, wo_cols,
           stage, lhs, act, part, sums, scores, ks, vs, kvs, qs, x_cols, pieces, home, wbuf, row_max, row_sum, acc_ref,
           wsem, lsem, gsend, grecv, ksend, krecv, rsend, rrecv, osend, orecv, psend, precv):
    z = lax.axis_index("tp")
    c = lax.axis_index("cp")
    rows = tokens.shape[0] // 2
    d = tokens.shape[1]
    all_rows = n * rows
    hc = w_q.shape[2]
    hd = w_k.shape[2]
    heads = hc // hd
    width = d // n
    ff = w_gate.shape[2]
    above = jnp.minimum(z + 1, n - 1)
    below = jnp.maximum(z - 1, 0)

    def remote(src, dst, send, recv, **where):
        return pltpu.make_async_remote_copy(src_ref=src, dst_ref=dst, send_sem=send, recv_sem=recv, device_id=where,
                                            device_id_type=MESH)

    def row_block(p):
        return pl.ds(pl.multiple_of(p * rows, 16), rows)

    def col_block(p, w):
        return pl.ds(pl.multiple_of(p * w, 128), w)

    class Gather:
        def __init__(self, layer, half, kind, buf, own):
            self.i = (layer * 2 + half) * 3 + kind
            self.buf, self.own = buf, own

        def copy(self, way, k, plane):
            src = self.own if k == 0 else self.buf.at[plane]
            return remote(src, self.buf.at[plane], gsend.at[self.i, way, k], grecv.at[self.i, way, k],
                          tp=above if way == UP else below)

        def start(self):
            @pl.when(z < n - 1)
            def _():
                self.copy(UP, 0, z).start()

            @pl.when(z > 0)
            def _():
                self.copy(DOWN, 0, z).start()

        def event(self, k):
            up, down = jnp.maximum(z - k, 0), jnp.minimum(z + k, n - 1)

            @pl.when(z >= k)
            def _():
                self.copy(UP, k - 1, up).wait_recv()

            if k < n - 1:
                @pl.when(both(z >= k, z < n - 1))
                def _():
                    self.copy(UP, k, up).start()

            @pl.when(z + k < n)
            def _():
                self.copy(DOWN, k - 1, down).wait_recv()

            if k < n - 1:
                @pl.when(both(z + k < n, z > 0))
                def _():
                    self.copy(DOWN, k, down).start()

        def drain(self, ks):
            for k in ks:
                @pl.when(both(z >= k, z < n - 1))
                def _(k=k):
                    self.copy(UP, k, z).wait_send()

                @pl.when(both(z + k < n, z > 0))
                def _(k=k):
                    self.copy(DOWN, k, z).wait_send()

    def own_x(layer, half):
        return tokens.at[pl.ds(half * rows, rows)] if layer == 0 else home.at[half]

    gx = {(l, h): Gather(l, h, X, g_x.at[l, h], own_x(l, h)) for l in range(layers) for h in (LOW, HIGH)}
    go = {(l, h): Gather(l, h, O, g_o.at[l, h], pieces.at[h]) for l in range(layers) for h in (LOW, HIGH)}
    gh = {(l, h): Gather(l, h, H, g_h.at[l, h], pieces.at[h]) for l in range(layers) for h in (LOW, HIGH)}

    def load(buf, own, where):
        copies = [pltpu.make_async_copy(own, stage.at[where(z)], lsem.at[0])]
        for k in range(1, n):
            p = ring(z + k, n)
            copies.append(pltpu.make_async_copy(buf.at[p], stage.at[where(p)], lsem.at[k]))
        for copy in copies:
            copy.start()
        for copy in copies:
            copy.wait()

    def load_rows(gather):
        load(gather.buf, gather.own, row_block)

    def load_cols(gather, w):
        load(gather.buf, gather.own, lambda p: (slice(None), col_block(p, w)))

    def norm(gain):
        step = 32

        @pl.loop(0, all_rows // step)
        def _(i):
            r = pl.ds(pl.multiple_of(i * step, step), step)
            x = stage[r].astype(F32)
            inv = lax.rsqrt(jnp.mean(x * x, axis=-1, keepdims=True) + 1e-5)
            lhs[r] = (x * inv * gain[...].astype(F32)).astype(BF16)

    def norm_x(layer, half):
        load_rows(gx[layer, half])
        norm(gain_a.at[pl.ds(layer, 1)])
        x_cols[half] = stage[:, col_block(z, width)]

    def norm_h(layer, half):
        load_cols(gh[layer, half], width)
        norm(gain_m.at[pl.ds(layer, 1)])
        gh[layer, half].drain((0,))
        if layer > 0:
            gx[layer, half].drain((0,))
        home[half] = stage[row_block(z)]

    class Op:
        base = None

        def start(self, i, slot):
            for copy in self.copies(i, slot):
                copy.start()

        def prefetch(self):
            for i in range(2):
                self.start(i, (self.base + i) % SLOTS)

        def run(self, follow, hooks):
            @pl.loop(0, self.tiles)
            def _(i):
                for at, event in hooks:
                    pl.when(i == at)(event)
                slot, later = lax.rem(self.base + i, SLOTS), lax.rem(self.base + i + 2, SLOTS)

                @pl.when(i + 2 < self.tiles)
                def _():
                    self.start(i + 2, later)

                if follow is not None:
                    @pl.when(i + 2 >= self.tiles)
                    def _():
                        follow.start(i + 2 - self.tiles, later)

                for copy in self.copies(i, slot):
                    copy.wait()
                self.compute(i, slot)

    def dot(a, slot, depth):
        return jnp.dot(a, wbuf[slot, :depth], preferred_element_type=F32)

    def tile_start(i, total):
        return pl.multiple_of(jnp.minimum(i * TILE, total - TILE), 128)

    class Qkv(Op):
        def __init__(self, layer, half):
            self.layer, self.half = layer, half
            self.tiles = 1 + -(-hc // TILE)

        def start(self, i, slot):
            def pair(a, b):
                pltpu.make_async_copy(a, wbuf.at[slot, pl.ds(0, d), pl.ds(0, hd)], wsem.at[slot, 0]).start()
                pltpu.make_async_copy(b, wbuf.at[slot, pl.ds(0, d), pl.ds(hd, hd)], wsem.at[slot, 1]).start()

            @pl.when(i == 0)
            def _():
                pair(w_k.at[self.layer], w_v.at[self.layer])

            @pl.when(i > 0)
            def _():
                at = tile_start(i - 1, hc)
                pair(w_q.at[self.layer, :, pl.ds(at, hd)], w_q.at[self.layer, :, pl.ds(at + hd, hd)])

        def copies(self, i, slot):
            return [pltpu.make_async_copy(w_k.at[self.layer], wbuf.at[slot, pl.ds(0, d), pl.ds(j * hd, hd)], wsem.at[slot, j])
                    for j in range(2)]

        def compute(self, i, slot):
            out = dot(lhs[...], slot, d)

            def turned(x):
                return (x * cos_ref[self.half] + pltpu.roll(x, hd // 2, 1) * sin_ref[self.half]).astype(BF16)

            @pl.when(i == 0)
            def _():
                kvs[self.layer, self.half, 0, :, :hd] = turned(out[:, :hd])
                kvs[self.layer, self.half, 0, :, hd:] = out[:, hd:].astype(BF16)

            @pl.when(i > 0)
            def _():
                h = tile_start(i - 1, hc) // hd
                for j in range(2):
                    q = turned(out[:, j * hd : (j + 1) * hd])
                    for p in range(n):
                        qs[p, row_block(h + j)] = q[p * rows : (p + 1) * rows]

    class Wo(Op):
        def __init__(self, layer, half):
            self.layer, self.half = layer, half
            self.tiles = -(-width // TILE)

        def copies(self, i, slot):
            at = tile_start(i, width)
            out = [pltpu.make_async_copy(w_o.at[self.layer, :, pl.ds(pl.multiple_of(z * width + at, 128), TILE)],
                                         wbuf.at[slot, pl.ds(pl.multiple_of(z * hc, 128), hc)], wsem.at[slot, 0])]
            for k in range(1, n):
                p = ring(z + k, n)
                block = pl.ds(pl.multiple_of(p * hc, 128), hc)
                out.append(pltpu.make_async_copy(wo_cols.at[self.layer, block, pl.ds(at, TILE)], wbuf.at[slot, block],
                                                 wsem.at[slot, k]))
            return out

        def compute(self, i, slot):
            cols = pl.ds(tile_start(i, width), TILE)
            out = dot(stage[...], slot, d) + x_cols[self.half, :, cols].astype(F32)
            pieces[self.half, :, cols] = out.astype(BF16)

    class GateUp(Op):
        def __init__(self, layer, half):
            self.layer, self.half = layer, half
            self.tiles = ff // 128

        def copies(self, i, slot):
            cols = pl.ds(pl.multiple_of(i * 128, 128), 128)
            return [pltpu.make_async_copy(w.at[self.layer, :, cols], wbuf.at[slot, pl.ds(0, d), pl.ds(128 * j, 128)], wsem.at[slot, j])
                    for j, w in enumerate((w_gate, w_up))]

        def compute(self, i, slot):
            out = dot(lhs[...], slot, d)
            gate = out[:, :128]
            act[:, pl.ds(pl.multiple_of(i * 128, 128), 128)] = (gate * lax.logistic(gate) * out[:, 128:]).astype(BF16)

    class Down(Op):
        def __init__(self, layer, half):
            self.layer, self.half = layer, half
            self.tiles = d // TILE

        def copies(self, i, slot):
            cols = pl.ds(pl.multiple_of(i * TILE, TILE), TILE)
            return [pltpu.make_async_copy(w_down.at[self.layer, :, cols], wbuf.at[slot, pl.ds(0, ff)], wsem.at[slot, 0])]

        def compute(self, i, slot):
            part[self.half, :, pl.ds(pl.multiple_of(i * TILE, TILE), TILE)] = dot(act[...], slot, ff)

    def kv_copy(layer, half, s):
        return remote(kvs.at[layer, half, 0], kvs.at[layer, half, s], ksend.at[layer, half, s - 1], krecv.at[layer, half, s - 1],
                      cp=ring(c + s, m))

    def kv_start(layer, half):
        for s in range(1, m):
            kv_copy(layer, half, s).start()

    def kv_wait(layer, half):
        for s in range(1, m):
            kv_copy(layer, half, s).wait_recv()

    def attend(layer, half):
        kv_wait(layer, half)
        keys = m * rows
        for s in range(m):
            for g in range(n):
                block = slice(g * rows, (g + 1) * rows)
                ks[half * n + g, s * rows : (s + 1) * rows] = kvs[layer, half, s, block, :hd]
                vs[half * n + g, s * rows : (s + 1) * rows] = kvs[layer, half, s, block, hd:]
        to_log2 = math.log2(math.e) / math.sqrt(hd)
        lanes = range(0, keys, 128)

        @pl.loop(0, n)
        def _(plane):
            count = plane if half == LOW else 2 * n - 1 - plane

            def group(i):
                if half == LOW:
                    return jnp.where(i == 0, plane, i - 1)
                return jnp.where(i == 0, n + plane, jnp.where(i <= n, i - 1, i + plane))

            def score(i):
                return lax.dot_general(qs[plane], ks[group(i)], (((1,), (1,)), ((), ())), preferred_element_type=F32)

            row = lax.broadcasted_iota(jnp.int32, (rows, keys), 0)
            col = lax.broadcasted_iota(jnp.int32, (rows, keys), 1)
            slot = col // rows
            other = lax.rem(c - slot + m, m)
            limit = jnp.where(slot == 0, row, jnp.where((other < c) if half == LOW else (other > c), keys, -1))
            bias = jnp.where(col <= limit, 0.0, -jnp.inf)
            s = (score(0).reshape(heads, rows, keys) + bias[None]).reshape(heads * rows, keys)
            scores[0] = s
            row_max[...] = functools.reduce(jnp.maximum, [s[:, a : a + 128] for a in lanes])

            @pl.loop(1, count + 1)
            def _(i):
                s = score(i)
                scores[i] = s
                row_max[...] = functools.reduce(jnp.maximum, [s[:, a : a + 128] for a in lanes], row_max[...])

            top = jnp.max(row_max[...], axis=-1, keepdims=True) * to_log2
            row_max[...] = jnp.broadcast_to(top, row_max.shape)
            row_sum[...] = jnp.zeros_like(row_sum)
            acc_ref[...] = jnp.zeros_like(acc_ref)

            @pl.loop(0, count + 1)
            def _(i):
                top = row_max[...]
                e = [jnp.exp2(scores[i, :, a : a + 128] * to_log2 - top) for a in lanes]
                row_sum[...] += functools.reduce(jnp.add, e)
                weights = jnp.concatenate([x.astype(BF16) for x in e], axis=-1)
                acc_ref[...] += jnp.dot(weights, vs[group(i)], preferred_element_type=F32)

            out = (acc_ref[...] / jnp.sum(row_sum[...], axis=-1, keepdims=True)).astype(BF16)
            for h in range(heads):
                pieces[half, row_block(plane), h * hd : (h + 1) * hd] = out[h * rows : (h + 1) * rows]

    share = hc // m

    def wo_rows(plane, quarter):
        return pl.ds(pl.multiple_of(plane * hc + quarter * share, 16), share)

    def wo_copy(layer, s):
        src = w_o.at[layer, pl.ds(pl.multiple_of(c * share, 16), share), col_block(ring(z + s, n), width)]
        return remote(src, wo_cols.at[layer, wo_rows(z, c)], osend.at[layer, s - 1], orecv.at[layer, s - 1], tp=ring(z + s, n))

    def wo_pass(layer, s, j):
        here = wo_cols.at[layer, wo_rows(ring(z - s, n), c)]
        return remote(here, here, psend.at[layer, s - 1, j - 1], precv.at[layer, s - 1, j - 1], cp=ring(c + j, m))

    def wo_start(layer):
        for s in range(1, n):
            wo_copy(layer, s).start()

    def wo_event(layer):
        for s in range(1, n):
            wo_copy(layer, s).wait_recv()
            for j in range(1, m):
                wo_pass(layer, s, j).start()

    def wo_wait(layer):
        for s in range(1, n):
            for j in range(1, m):
                wo_pass(layer, s, j).wait_recv()

    span = d // PARTS

    def sum_slot(way, k):
        return k - 1 if way == UP else (0, 3, 4)[k - 1]

    def sum_copy(layer, half, way, q, k, block):
        cols = pl.ds(q * span, span)
        return remote(part.at[half, row_block(block), cols], sums.at[half, sum_slot(way, k), :, cols],
                      rsend.at[layer, half, way, q, k - 1], rrecv.at[layer, half, way, q, k - 1], tp=above if way == UP else below)

    def sum_start(layer, half, q):
        @pl.when(z == 0)
        def _():
            for k in range(1, n):
                sum_copy(layer, half, UP, q, k, n - k).start()

        @pl.when(z == n - 1)
        def _():
            for k in range(1, n):
                sum_copy(layer, half, DOWN, q, k, k - 1).start()

    def sum_event(layer, half, q, k):
        for way, here, block, more in ((UP, both(z >= 1, k >= z), n - 1 + z - k, z < n - 1),
                                       (DOWN, both(z <= n - 2, k >= n - 1 - z), z + k - n + 1, z > 0)):
            block = jnp.clip(block, 0, n - 1)

            @pl.when(here)
            def _(way=way, block=block):
                sum_copy(layer, half, way, q, k, block).wait_recv()
                step = 16

                @pl.loop(0, rows // step)
                def _(i):
                    to = pl.ds(pl.multiple_of(block * rows + i * step, step), step)
                    frm = pl.ds(pl.multiple_of(i * step, step), step)
                    part[half, to, q * span : (q + 1) * span] += sums[half, sum_slot(way, k), frm, q * span : (q + 1) * span]

            if k < n - 1:
                @pl.when(both(here, more))
                def _(way=way, block=block):
                    sum_copy(layer, half, way, q, k + 1, block).start()

    def sum_drain(layer, half):
        for q in range(PARTS):
            for k in range(1, n):
                @pl.when(both(z < n - 1, jnp.logical_or(z == 0, k - 1 >= z)))
                def _(q=q, k=k):
                    sum_copy(layer, half, UP, q, k, 0).wait_send()

                @pl.when(both(z > 0, jnp.logical_or(z == n - 1, k - 1 >= n - 1 - z)))
                def _(q=q, k=k):
                    sum_copy(layer, half, DOWN, q, k, 0).wait_send()

    def finish(half):
        step = 16

        @pl.loop(0, rows // step)
        def _(i):
            r = pl.ds(pl.multiple_of(i * step, step), step)
            mine = part[half, pl.ds(pl.multiple_of(z * rows + i * step, step), step)]
            home[half, r] = (home[half, r].astype(F32) + mine).astype(BF16)

    barrier = pltpu.get_barrier_semaphore()
    for s in (1, n - 1):
        pl.semaphore_signal(barrier, inc=1, device_id={"tp": ring(z + s, n)}, device_id_type=MESH)
    if n > 3:
        pl.semaphore_signal(barrier, inc=1, device_id={"tp": ring(z + 2, n)}, device_id_type=MESH)
    for s in range(1, m):
        pl.semaphore_signal(barrier, inc=1, device_id={"cp": ring(c + s, m)}, device_id_type=MESH)
    pl.semaphore_wait(barrier, n - 1 + m - 1)

    items = []

    def do(f, *args):
        items.append(("do", functools.partial(f, *args), None))

    def op(o, *hooks):
        items.append(("op", o, hooks))
        return o

    def pre(o):
        items.append(("pre", o, None))

    def ev(gather, k):
        return functools.partial(gather.event, k)

    def sums_ev(layer, half, k):
        def f():
            for q in range(PARTS):
                sum_event(layer, half, q, k)
        return f

    A, B = LOW, HIGH
    gate_tiles = ff // 128
    down_tiles = d // TILE

    def part_of(tiles, share):
        return min(tiles - 1, int(tiles * share))

    l = 0
    do(gx[l, A].start)
    qa = Qkv(l, A)
    pre(qa)
    do(gx[l, A].event, 1)
    do(gx[l, A].event, 2)
    do(wo_start, l)
    do(gx[l, B].start)
    do(gx[l, A].event, 3)
    do(norm_x, l, A)
    op(qa, (2, functools.partial(kv_start, l, A)))
    do(gx[l, B].event, 1)
    do(attend, l, A)
    do(go[l, A].start)
    do(wo_event, l)
    do(gx[l, B].event, 2)
    do(gx[l, B].event, 3)
    do(norm_x, l, B)
    op(Qkv(l, B), (2, functools.partial(kv_start, l, B)))
    do(go[l, A].event, 1)
    do(attend, l, B)
    do(go[l, A].event, 2)
    do(wo_wait, l)
    wa = Wo(l, A)
    pre(wa)
    do(go[l, A].event, 3)

    def o_to_h(l, half, o):
        do(load_cols, go[l, half], hc)
        do(go[l, half].drain, (0,))
        op(o)
        do(gh[l, half].start)

    def back_a(l):
        do(gh[l, A].event, 1)
        do(gh[l, A].event, 2)
        do(go[l, B].start)
        do(gh[l, A].event, 3)
        do(norm_h, l, A)
        op(GateUp(l, A), (part_of(gate_tiles, 0.35), ev(go[l, B], 1)), (part_of(gate_tiles, 0.9), ev(go[l, B], 2)))
        if l > 0:
            do(sum_drain, l - 1, A)
        op(Down(l, A), (down_tiles // 2, functools.partial(sum_start, l, A, 0)), (part_of(down_tiles, 0.75), ev(go[l, B], 3)))
        do(sum_start, l, A, 1)
        o_to_h(l, B, Wo(l, B))
        do(gh[l, B].event, 1)
        do(sums_ev(l, A, 1))
        do(gh[l, B].event, 2)
        do(gh[l, B].event, 3)
        do(norm_h, l, B)

    o_to_h(l, A, wa)
    back_a(l)
    do(wo_start, 1)
    op(GateUp(l, B), (part_of(gate_tiles, 0.3), sums_ev(l, A, 2)), (part_of(gate_tiles, 0.6), functools.partial(wo_event, 1)))
    op(Down(l, B), (part_of(down_tiles, 0.3), sums_ev(l, A, 3)), (down_tiles // 2, functools.partial(sum_start, l, B, 0)))
    do(sum_start, l, B, 1)
    do(finish, A)
    do(gx[1, A].start)

    l = 1
    do(gx[l, A].event, 1)
    do(gx[l, A].event, 2)
    do(wo_wait, l)
    do(gx[l, A].event, 3)
    do(norm_x, l, A)
    op(Qkv(l, A), (2, functools.partial(kv_start, l, A)))
    do(sums_ev(0, B, 1))
    do(attend, l, A)
    do(go[l, A].start)
    do(sums_ev(0, B, 2))
    do(go[l, A].event, 1)
    do(sums_ev(0, B, 3))
    do(finish, B)
    do(go[l, A].event, 2)
    do(gx[l, B].start)
    do(go[l, A].event, 3)
    o_to_h(l, A, Wo(l, A))
    do(gx[l, B].event, 1)
    do(gh[l, A].event, 1)
    do(gx[l, B].event, 2)
    do(gx[l, B].event, 3)
    do(norm_x, l, B)
    op(Qkv(l, B), (2, functools.partial(kv_start, l, B)))
    do(gh[l, A].event, 2)
    do(attend, l, B)
    do(go[l, B].start)
    do(gh[l, A].event, 3)
    do(norm_h, l, A)
    op(GateUp(l, A), (part_of(gate_tiles, 0.1), ev(go[l, B], 1)), (part_of(gate_tiles, 0.5), ev(go[l, B], 2)),
       (part_of(gate_tiles, 0.9), ev(go[l, B], 3)))
    do(sum_drain, 0, A)
    op(Down(l, A), (down_tiles // 2, functools.partial(sum_start, l, A, 0)))
    do(sum_start, l, A, 1)
    o_to_h(l, B, Wo(l, B))
    do(gh[l, B].event, 1)
    do(sums_ev(l, A, 1))
    do(gh[l, B].event, 2)
    do(gh[l, B].event, 3)
    do(norm_h, l, B)
    op(GateUp(l, B), (part_of(gate_tiles, 0.4), sums_ev(l, A, 2)))
    do(sum_drain, 0, B)
    op(Down(l, B), (part_of(down_tiles, 0.3), sums_ev(l, A, 3)), (down_tiles // 2, functools.partial(sum_start, l, B, 0)))
    do(sum_start, l, B, 1)
    do(finish, A)

    def put(half, wait):
        copy = pltpu.make_async_copy(home.at[half], y_out.at[pl.ds(half * rows, rows)], lsem.at[half])
        copy.wait() if wait else copy.start()

    do(put, A, False)
    for k in range(1, n):
        do(sums_ev(l, B, k))
    do(finish, B)
    do(put, B, False)
    do(sum_drain, l, A)
    do(sum_drain, l, B)
    for i in range(layers):
        for half in (A, B):
            do(gx[i, half].drain, (0, 1, 2) if i == 0 else (1, 2))
            do(go[i, half].drain, (1, 2))
            do(gh[i, half].drain, (1, 2))

    def last_sends():
        for i in range(layers):
            for half in (A, B):
                for s in range(1, m):
                    kv_copy(i, half, s).wait_send()
            for s in range(1, n):
                wo_copy(i, s).wait_send()
                for j in range(1, m):
                    wo_pass(i, s, j).wait_send()

    do(last_sends)
    do(put, A, True)
    do(put, B, True)

    ops = [o for what, o, _ in items if what == "op"]
    named = [o for what, o, _ in items if what == "pre"]
    base = 0
    for o in ops:
        o.base = base % SLOTS
        base += o.tiles
    follow = {id(o): (f if f not in named else None) for o, f in zip(ops, ops[1:])}
    for what, o, hooks in items:
        if what == "do":
            o()
        elif what == "pre":
            o.prefetch()
        else:
            o.run(follow.get(id(o)), hooks)


def solution(mesh):
    n = mesh.shape['tp']
    m = mesh.shape['cp']
    row_spec = P(('dp', 'tp', 'cp'), None)
    gain_spec = P(None, None)
    q_spec = P(None, None, 'tp', None)
    col_spec = P(None, None, 'tp')
    o_spec = P(None, 'tp', None, None)
    down_spec = P(None, 'tp', None)

    def body(tokens, norm_attn, norm_mlp, w_q, w_k, w_v, w_o, w_gate, w_up, w_down):
        layers, d, heads, hd = w_q.shape
        rows = tokens.shape[0] // 2
        hc = heads * hd
        width = d // n
        ff = w_gate.shape[2]
        all_rows = n * rows
        c = lax.axis_index('cp')

        inv_freq = 500000.0 ** (-(jnp.arange(hd // 2, dtype=F32) * 2.0 / hd))
        seg = jnp.arange(n) * m + c
        seg = jnp.stack([seg, 2 * n * m - 1 - seg])
        pos = (seg[:, :, None] * rows + jnp.arange(rows)).reshape(2, all_rows)
        angle = pos.astype(F32)[..., None] * inv_freq
        cos, sin = jnp.cos(angle), jnp.sin(angle)
        cos, sin = jnp.concatenate([cos, cos], -1), jnp.concatenate([-sin, sin], -1)

        hbm = pl.BlockSpec(memory_space=pl.ANY)
        vmem = pl.BlockSpec(memory_space=pltpu.VMEM)
        dma = pltpu.SemaphoreType.DMA
        out = pl.pallas_call(
            functools.partial(kernel, n, m, layers),
            out_shape=(
                jax.ShapeDtypeStruct(tokens.shape, BF16),
                jax.ShapeDtypeStruct((layers, 2, n, rows, d), BF16),
                jax.ShapeDtypeStruct((layers, 2, n, all_rows, hc), BF16),
                jax.ShapeDtypeStruct((layers, 2, n, all_rows, width), BF16),
                jax.ShapeDtypeStruct((layers, n * hc, width), BF16),
            ),
            in_specs=[hbm, vmem, vmem, vmem, vmem] + [hbm] * 7,
            out_specs=(hbm,) * 5,
            scratch_shapes=[
                pltpu.VMEM((all_rows, d), BF16),
                pltpu.VMEM((all_rows, d), BF16),
                pltpu.VMEM((all_rows, ff), BF16),
                pltpu.VMEM((2, all_rows, d), F32),
                pltpu.VMEM((2, 5, rows, d), F32),
                pltpu.VMEM((2 * n, heads * rows, m * rows), F32),
                pltpu.VMEM((2 * n, m * rows, hd), BF16),
                pltpu.VMEM((2 * n, m * rows, hd), BF16),
                pltpu.VMEM((layers, 2, m, all_rows, 2 * hd), BF16),
                pltpu.VMEM((n, heads * rows, hd), BF16),
                pltpu.VMEM((2, all_rows, width), BF16),
                pltpu.VMEM((2, all_rows, width), BF16),
                pltpu.VMEM((2, rows, d), BF16),
                pltpu.VMEM((SLOTS, max(d, ff), TILE), BF16),
                pltpu.VMEM((heads * rows, 128), F32),
                pltpu.VMEM((heads * rows, 128), F32),
                pltpu.VMEM((heads * rows, hd), F32),
                dma((SLOTS, n)),
                dma((n,)),
                dma((layers * 6, 2, n - 1)),
                dma((layers * 6, 2, n - 1)),
                dma((layers, 2, m - 1)),
                dma((layers, 2, m - 1)),
                dma((layers, 2, 2, PARTS, n - 1)),
                dma((layers, 2, 2, PARTS, n - 1)),
                dma((layers, n - 1)),
                dma((layers, n - 1)),
                dma((layers, n - 1, m - 1)),
                dma((layers, n - 1, m - 1)),
            ],
            compiler_params=pltpu.CompilerParams(collective_id=0, has_side_effects=True, vmem_limit_bytes=67043328),
            name="two_layers",
        )(tokens, norm_attn, norm_mlp, cos, sin, w_q.reshape(layers, d, hc), w_k, w_v, w_o.reshape(layers, hc, d), w_gate, w_up, w_down)
        return out[0]

    return jax.shard_map(
        body,
        mesh=mesh,
        in_specs=(row_spec, gain_spec, gain_spec, q_spec, col_spec, col_spec, o_spec, col_spec, col_spec, down_spec),
        out_specs=row_spec,
        check_vma=False,
    )
```

```python
import functools
import math
import jax
import jax.numpy as jnp
from jax import lax
from jax.experimental import pallas as pl
from jax.experimental.pallas import tpu as pltpu
from jax.sharding import PartitionSpec as P

F32 = jnp.float32
BF16 = jnp.bfloat16
MESH = pl.DeviceIdType.MESH
UP, DOWN = 0, 1
X, O, H = 0, 1, 2
LOW, HIGH = 0, 1
SLOTS = 3
PARTS = 2
TILE = 256


def ring(i, n):
    return lax.rem(i + n, n)


def both(*conditions):
    out = conditions[0]
    for c in conditions[1:]:
        out = jnp.logical_and(out, c)
    return out


TILES = {"qkv": 5, "wo": 4, "gate": 37, "down": 14}
ORDER = (
    ("x_start", 0, 0),
    ("x_start", 0, 1),
    ("x", 0, 0, 1, "U"),
    ("x", 0, 0, 1, "D"),
    ("x", 0, 1, 1, "D"),
    ("x", 0, 0, 2, "D"),
    ("x", 0, 1, 1, "U"),
    ("x", 0, 0, 2, "U"),
    ("x", 0, 1, 2, "D"),
    ("wo_start", 0, 0),
    ("x", 0, 0, 3, "D"),
    ("x", 0, 0, 3, "U"),
    ("norm_x", 0, 0),
    ("qkv", 0, 0, ((2, ("x", 0, 1, 2, "U"), ("kv_start", 0, 0)), (4, ("x", 0, 1, 3, "U")),), "late"),
    ("attend", 0, 0),
    ("o_start", 0, 0),
    ("x", 0, 1, 3, "D"),
    ("norm_x", 0, 1),
    ("qkv", 0, 1, ((3, ("wo_event", 0, 0)), (4, ("kv_start", 0, 1)),)),
    ("o", 0, 0, 1, "D"),
    ("o", 0, 0, 1, "U"),
    ("attend", 0, 1),
    ("o", 0, 0, 2, "D"),
    ("o", 0, 0, 2, "U"),
    ("o_start", 0, 1),
    ("o", 0, 0, 3, "U"),
    ("o", 0, 0, 3, "D"),
    ("load_o", 0, 0),
    ("wo_wait", 0, 0),
    ("wo", 0, 0, (), "late"),
    ("h_start", 0, 0),
    ("h", 0, 0, 1, "U"),
    ("h", 0, 0, 1, "D"),
    ("h", 0, 0, 2, "U"),
    ("h", 0, 0, 2, "D"),
    ("h", 0, 0, 3, "U"),
    ("h", 0, 0, 3, "D"),
    ("norm_h", 0, 0),
    ("gate", 0, 0, ((2, ("o", 0, 1, 1, "D"), ("o", 0, 1, 1, "U")), (11, ("o", 0, 1, 2, "D")), (16, ("o", 0, 1, 2, "U")), (17, ("wo_start", 1, 0)),)),
    ("down", 0, 0, ((6, ("o", 0, 1, 3, "U")), (7, ("sum_send", 0, 0, 0, 1), ("o", 0, 1, 3, "D")),)),
    ("load_o", 0, 1),
    ("wo", 0, 1, ()),
    ("h_start", 0, 1),
    ("sum", 0, 0, 0, 1, "U"),
    ("h", 0, 1, 1, "U"),
    ("sum_send", 0, 0, 1, 1),
    ("wo_event", 1, 0),
    ("sum_send", 0, 0, 1, 2),
    ("sum_send", 0, 0, 0, 2),
    ("h", 0, 1, 1, "D"),
    ("sum", 0, 0, 1, 1, "D"),
    ("h", 0, 1, 2, "D"),
    ("h", 0, 1, 2, "U"),
    ("h", 0, 1, 3, "U"),
    ("h", 0, 1, 3, "D"),
    ("norm_h", 0, 1),
    ("sum_send", 0, 0, 1, 3),
    ("sum", 0, 0, 1, 1, "U"),
    ("sum", 0, 0, 0, 1, "D"),
    ("gate", 0, 1, ((7, ("sum", 0, 0, 1, 2, "U")), (8, ("sum", 0, 0, 1, 2, "D")), (21, ("sum_send", 0, 0, 0, 3), ("sum", 0, 0, 0, 2, "U")), (26, ("sum", 0, 0, 0, 2, "D"), ("sum", 0, 0, 1, 3, "U")),)),
    ("sum", 0, 0, 1, 3, "D"),
    ("sum", 0, 0, 0, 3, "U"),
    ("wo_wait", 1, 0),
    ("down", 0, 1, ((1, ("sum", 0, 0, 0, 3, "D")), (2, ("finish", 0, 0), ("x_start", 1, 0)), (4, ("sum_drain", 0, 0)), (8, ("sum_send", 0, 1, 0, 1), ("x", 1, 0, 1, "D"), ("x", 1, 0, 1, "U")), (9, ("sum", 0, 1, 0, 1, "D")), (11, ("sum_send", 0, 1, 0, 2)), (12, ("sum_send", 0, 1, 0, 3), ("sum", 0, 1, 0, 1, "U"), ("x", 1, 0, 2, "D")),)),
    ("x", 1, 0, 2, "U"),
    ("x", 1, 0, 3, "D"),
    ("x", 1, 0, 3, "U"),
    ("norm_x", 1, 0),
    ("qkv", 1, 0, ((2, ("kv_start", 1, 0), ("sum", 0, 1, 0, 2, "D"), ("sum", 0, 1, 0, 2, "U"), ("sum_send", 0, 1, 1, 1)),)),
    ("attend", 1, 0),
    ("o_start", 1, 0),
    ("sum", 0, 1, 1, 1, "D"),
    ("sum", 0, 1, 0, 3, "U"),
    ("sum_send", 0, 1, 1, 2),
    ("sum", 0, 1, 1, 1, "U"),
    ("o", 1, 0, 1, "U"),
    ("sum", 0, 1, 0, 3, "D"),
    ("sum_send", 0, 1, 1, 3),
    ("o", 1, 0, 1, "D"),
    ("sum", 0, 1, 1, 2, "U"),
    ("sum", 0, 1, 1, 2, "D"),
    ("o", 1, 0, 2, "U"),
    ("o", 1, 0, 2, "D"),
    ("sum", 0, 1, 1, 3, "D"),
    ("o", 1, 0, 3, "U"),
    ("sum", 0, 1, 1, 3, "U"),
    ("finish", 0, 1),
    ("x_start", 1, 1),
    ("o", 1, 0, 3, "D"),
    ("load_o", 1, 0),
    ("wo", 1, 0, ((1, ("x", 1, 1, 1, "U"), ("x", 1, 1, 1, "D"), ("x", 1, 1, 2, "D")), (3, ("x", 1, 1, 2, "U")),)),
    ("h_start", 1, 0),
    ("x", 1, 1, 3, "U"),
    ("x", 1, 1, 3, "D"),
    ("norm_x", 1, 1),
    ("qkv", 1, 1, ((4, ("kv_start", 1, 1), ("h", 1, 0, 1, "U")),)),
    ("sum_drain", 0, 1),
    ("h", 1, 0, 1, "D"),
    ("attend", 1, 1),
    ("h", 1, 0, 2, "D"),
    ("h", 1, 0, 2, "U"),
    ("o_start", 1, 1),
    ("h", 1, 0, 3, "D"),
    ("h", 1, 0, 3, "U"),
    ("norm_h", 1, 0),
    ("gate", 1, 0, ((25, ("o", 1, 1, 1, "D")), (26, ("o", 1, 1, 1, "U")), (29, ("o", 1, 1, 2, "U")), (36, ("o", 1, 1, 2, "D")),)),
    ("down", 1, 0, ((7, ("sum_send", 1, 0, 0, 1)), (11, ("o", 1, 1, 3, "U")), (12, ("o", 1, 1, 3, "D")),)),
    ("load_o", 1, 1),
    ("wo", 1, 1, ()),
    ("h_start", 1, 1),
    ("h", 1, 1, 1, "U"),
    ("h", 1, 1, 1, "D"),
    ("sum_send", 1, 0, 1, 1),
    ("h", 1, 1, 2, "U"),
    ("h", 1, 1, 2, "D"),
    ("sum_send", 1, 0, 0, 2),
    ("sum_send", 1, 0, 1, 2),
    ("sum_send", 1, 0, 1, 3),
    ("h", 1, 1, 3, "D"),
    ("h", 1, 1, 3, "U"),
    ("sum_send", 1, 0, 0, 3),
    ("norm_h", 1, 1),
    ("gate", 1, 1, ((2, ("sum", 1, 0, 1, 1, "U")), (5, ("sum", 1, 0, 1, 1, "D")), (10, ("sum", 1, 0, 0, 1, "D")), (13, ("sum", 1, 0, 0, 1, "U")), (18, ("sum", 1, 0, 1, 2, "D")), (30, ("sum", 1, 0, 0, 2, "U")), (32, ("sum", 1, 0, 1, 2, "U")), (33, ("sum", 1, 0, 0, 2, "D")),)),
    ("sum", 1, 0, 1, 3, "D"),
    ("down", 1, 1, ((7, ("sum_send", 1, 1, 0, 1), ("sum", 1, 0, 0, 3, "D")), (10, ("sum", 1, 0, 0, 3, "U"), ("sum", 1, 0, 1, 3, "U")), (11, ("finish", 1, 0)), (13, ("sum", 1, 1, 0, 1, "D"), ("put", 1, 0), ("sum", 1, 1, 0, 1, "U")),)),
    ("sum_send", 1, 1, 1, 1),
    ("sum", 1, 1, 1, 1, "U"),
    ("sum", 1, 1, 1, 1, "D"),
    ("sum", 1, 1, 0, 2, "D"),
    ("sum", 1, 1, 0, 2, "U"),
    ("sum", 1, 1, 1, 2, "U"),
    ("sum_send", 1, 1, 0, 2),
    ("sum_send", 1, 1, 1, 2),
    ("sum_send", 1, 1, 1, 3),
    ("sum_send", 1, 1, 0, 3),
    ("sum", 1, 1, 1, 2, "D"),
    ("sum", 1, 1, 0, 3, "U"),
    ("sum", 1, 1, 1, 3, "U"),
    ("sum", 1, 1, 1, 3, "D"),
    ("sum", 1, 1, 0, 3, "D"),
    ("finish", 1, 1),
    ("put", 1, 1),
)


def kernel(n, m, layers, tokens, gain_a, gain_m, cos_ref, sin_ref, w_q, w_k, w_v, w_o, w_gate, w_up, w_down,
           y_out, g_x, g_o, g_h, wo_cols,
           stage, lhs, act, part, sums, scores, ks, vs, kvs, qs, x_cols, pieces, home, wbuf, row_max, row_sum, acc_ref,
           wsem, lsem, gsend, grecv, ksend, krecv, rsend, rrecv, osend, orecv, psend, precv):
    z = lax.axis_index("tp")
    c = lax.axis_index("cp")
    rows = tokens.shape[0] // 2
    d = tokens.shape[1]
    all_rows = n * rows
    heads, hd = w_q.shape[1], w_q.shape[3]
    hc = heads * hd
    width = d // n
    ff = w_gate.shape[2]
    above = jnp.minimum(z + 1, n - 1)
    below = jnp.maximum(z - 1, 0)

    def remote(src, dst, send, recv, **where):
        return pltpu.make_async_remote_copy(src_ref=src, dst_ref=dst, send_sem=send, recv_sem=recv, device_id=where,
                                            device_id_type=MESH)

    def row_block(p):
        return pl.ds(pl.multiple_of(p * rows, 16), rows)

    def col_block(p, w):
        return pl.ds(pl.multiple_of(p * w, 128), w)

    class Gather:
        def __init__(self, layer, half, kind, buf, own):
            self.i = (layer * 2 + half) * 3 + kind
            self.buf, self.own = buf, own

        def copy(self, way, k, plane):
            src = self.own if k == 0 else self.buf.at[plane]
            return remote(src, self.buf.at[plane], gsend.at[self.i, way, k], grecv.at[self.i, way, k],
                          tp=above if way == UP else below)

        def start(self):
            @pl.when(z < n - 1)
            def _():
                self.copy(UP, 0, z).start()

            @pl.when(z > 0)
            def _():
                self.copy(DOWN, 0, z).start()

        def event(self, k, way):
            plane = jnp.maximum(z - k, 0) if way == UP else jnp.minimum(z + k, n - 1)
            here = z >= k if way == UP else z + k < n

            @pl.when(here)
            def _():
                self.copy(way, k - 1, plane).wait_recv()

            if k < n - 1:
                @pl.when(both(here, z < n - 1 if way == UP else z > 0))
                def _():
                    self.copy(way, k, plane).start()

        def drain(self, ks):
            for k in ks:
                @pl.when(both(z >= k, z < n - 1))
                def _(k=k):
                    self.copy(UP, k, z).wait_send()

                @pl.when(both(z + k < n, z > 0))
                def _(k=k):
                    self.copy(DOWN, k, z).wait_send()

    def own_x(layer, half):
        return tokens.at[pl.ds(half * rows, rows)] if layer == 0 else home.at[half]

    gx = {(l, h): Gather(l, h, X, g_x.at[l, h], own_x(l, h)) for l in range(layers) for h in (LOW, HIGH)}
    go = {(l, h): Gather(l, h, O, g_o.at[l, h], pieces.at[h]) for l in range(layers) for h in (LOW, HIGH)}
    gh = {(l, h): Gather(l, h, H, g_h.at[l, h], pieces.at[h]) for l in range(layers) for h in (LOW, HIGH)}

    def load(buf, own, where):
        copies = [pltpu.make_async_copy(own, stage.at[where(z)], lsem.at[0])]
        for k in range(1, n):
            p = ring(z + k, n)
            copies.append(pltpu.make_async_copy(buf.at[p], stage.at[where(p)], lsem.at[k]))
        for copy in copies:
            copy.start()
        for copy in copies:
            copy.wait()

    def load_rows(gather):
        load(gather.buf, gather.own, row_block)

    def load_cols(gather, w):
        load(gather.buf, gather.own, lambda p: (slice(None), col_block(p, w)))

    def norm(gain):
        step = 32

        @pl.loop(0, all_rows // step)
        def _(i):
            r = pl.ds(pl.multiple_of(i * step, step), step)
            x = stage[r].astype(F32)
            inv = lax.rsqrt(jnp.mean(x * x, axis=-1, keepdims=True) + 1e-5)
            lhs[r] = (x * inv * gain[...].astype(F32)).astype(BF16)

    def norm_x(layer, half):
        load_rows(gx[layer, half])
        norm(gain_a.at[pl.ds(layer, 1)])
        x_cols[half] = stage[:, col_block(z, width)]

    def norm_h(layer, half):
        load_cols(gh[layer, half], width)
        norm(gain_m.at[pl.ds(layer, 1)])
        gh[layer, half].drain((0,))
        if layer > 0:
            gx[layer, half].drain((0,))
        home[half] = stage[row_block(z)]

    class Op:
        base = None

        def start(self, i, slot):
            for copy in self.copies(i, slot):
                copy.start()

        def prefetch(self):
            for i in range(2):
                self.start(i, (self.base + i) % SLOTS)

        def run(self, follow, hooks):
            @pl.loop(0, self.tiles)
            def _(i):
                for at, event in hooks:
                    pl.when(i == at)(event)
                slot, later = lax.rem(self.base + i, SLOTS), lax.rem(self.base + i + 2, SLOTS)

                @pl.when(i + 2 < self.tiles)
                def _():
                    self.start(i + 2, later)

                if follow is not None:
                    @pl.when(i + 2 >= self.tiles)
                    def _():
                        follow.start(i + 2 - self.tiles, later)

                for copy in self.copies(i, slot):
                    copy.wait()
                self.compute(i, slot)

    def dot(a, slot, depth):
        return jnp.dot(a, wbuf[slot, :depth], preferred_element_type=F32)

    def tile_start(i, total):
        return pl.multiple_of(jnp.minimum(i * TILE, total - TILE), 128)

    class Qkv(Op):
        def __init__(self, layer, half):
            self.layer, self.half = layer, half
            self.tiles = 1 + -(-hc // TILE)

        def start(self, i, slot):
            def pair(a, b):
                pltpu.make_async_copy(a, wbuf.at[slot, pl.ds(0, d), pl.ds(0, hd)], wsem.at[slot, 0]).start()
                pltpu.make_async_copy(b, wbuf.at[slot, pl.ds(0, d), pl.ds(hd, hd)], wsem.at[slot, 1]).start()

            @pl.when(i == 0)
            def _():
                pair(w_k.at[self.layer], w_v.at[self.layer])

            @pl.when(i > 0)
            def _():
                h = tile_start(i - 1, hc) // hd
                pair(w_q.at[self.layer, h], w_q.at[self.layer, h + 1])

        def copies(self, i, slot):
            return [pltpu.make_async_copy(w_k.at[self.layer], wbuf.at[slot, pl.ds(0, d), pl.ds(j * hd, hd)], wsem.at[slot, j])
                    for j in range(2)]

        def compute(self, i, slot):
            out = dot(lhs[...], slot, d)

            def turned(x):
                return (x * cos_ref[self.half] + pltpu.roll(x, hd // 2, 1) * sin_ref[self.half]).astype(BF16)

            @pl.when(i == 0)
            def _():
                kvs[self.layer, self.half, 0, :, :hd] = turned(out[:, :hd])
                kvs[self.layer, self.half, 0, :, hd:] = out[:, hd:].astype(BF16)

            @pl.when(i > 0)
            def _():
                h = tile_start(i - 1, hc) // hd
                for j in range(2):
                    q = turned(out[:, j * hd : (j + 1) * hd])
                    for p in range(n):
                        qs[p, row_block(h + j)] = q[p * rows : (p + 1) * rows]

    class Wo(Op):
        def __init__(self, layer, half):
            self.layer, self.half = layer, half
            self.tiles = -(-width // TILE)

        def copies(self, i, slot):
            at = tile_start(i, width)
            out = [pltpu.make_async_copy(w_o.at[self.layer, :, pl.ds(pl.multiple_of(z * width + at, 128), TILE)],
                                         wbuf.at[slot, pl.ds(pl.multiple_of(z * hc, 128), hc)], wsem.at[slot, 0])]
            for k in range(1, n):
                p = ring(z + k, n)
                block = pl.ds(pl.multiple_of(p * hc, 128), hc)
                out.append(pltpu.make_async_copy(wo_cols.at[self.layer, block, pl.ds(at, TILE)], wbuf.at[slot, block],
                                                 wsem.at[slot, k]))
            return out

        def compute(self, i, slot):
            cols = pl.ds(tile_start(i, width), TILE)
            out = dot(stage[...], slot, d) + x_cols[self.half, :, cols].astype(F32)
            pieces[self.half, :, cols] = out.astype(BF16)

    class GateUp(Op):
        def __init__(self, layer, half):
            self.layer, self.half = layer, half
            self.tiles = ff // 128

        def copies(self, i, slot):
            cols = pl.ds(pl.multiple_of(i * 128, 128), 128)
            return [pltpu.make_async_copy(w.at[self.layer, :, cols], wbuf.at[slot, pl.ds(0, d), pl.ds(128 * j, 128)], wsem.at[slot, j])
                    for j, w in enumerate((w_gate, w_up))]

        def compute(self, i, slot):
            out = dot(lhs[...], slot, d)
            gate = out[:, :128]
            act[:, pl.ds(pl.multiple_of(i * 128, 128), 128)] = (gate * lax.logistic(gate) * out[:, 128:]).astype(BF16)

    class Down(Op):
        def __init__(self, layer, half):
            self.layer, self.half = layer, half
            self.tiles = d // TILE

        def copies(self, i, slot):
            cols = pl.ds(pl.multiple_of(i * TILE, TILE), TILE)
            return [pltpu.make_async_copy(w_down.at[self.layer, :, cols], wbuf.at[slot, pl.ds(0, ff)], wsem.at[slot, 0])]

        def compute(self, i, slot):
            part[self.half, :, pl.ds(pl.multiple_of(i * TILE, TILE), TILE)] = dot(act[...], slot, ff)

    def kv_copy(layer, half, s):
        return remote(kvs.at[layer, half, 0], kvs.at[layer, half, s], ksend.at[layer, half, s - 1], krecv.at[layer, half, s - 1],
                      cp=ring(c + s, m))

    def kv_start(layer, half):
        for s in range(1, m):
            kv_copy(layer, half, s).start()

    def kv_wait(layer, half):
        for s in range(1, m):
            kv_copy(layer, half, s).wait_recv()

    def attend(layer, half):
        kv_wait(layer, half)
        keys = m * rows
        for s in range(m):
            for g in range(n):
                block = slice(g * rows, (g + 1) * rows)
                ks[half * n + g, s * rows : (s + 1) * rows] = kvs[layer, half, s, block, :hd]
                vs[half * n + g, s * rows : (s + 1) * rows] = kvs[layer, half, s, block, hd:]
        to_log2 = math.log2(math.e) / math.sqrt(hd)
        lanes = range(0, keys, 128)

        @pl.loop(0, n)
        def _(plane):
            count = plane if half == LOW else 2 * n - 1 - plane

            def group(i):
                if half == LOW:
                    return jnp.where(i == 0, plane, i - 1)
                return jnp.where(i == 0, n + plane, jnp.where(i <= n, i - 1, i + plane))

            def score(i):
                return lax.dot_general(qs[plane], ks[group(i)], (((1,), (1,)), ((), ())), preferred_element_type=F32)

            row = lax.broadcasted_iota(jnp.int32, (rows, keys), 0)
            col = lax.broadcasted_iota(jnp.int32, (rows, keys), 1)
            slot = col // rows
            other = lax.rem(c - slot + m, m)
            limit = jnp.where(slot == 0, row, jnp.where((other < c) if half == LOW else (other > c), keys, -1))
            bias = jnp.where(col <= limit, 0.0, -jnp.inf)
            s = (score(0).reshape(heads, rows, keys) + bias[None]).reshape(heads * rows, keys)
            scores[0] = s
            row_max[...] = functools.reduce(jnp.maximum, [s[:, a : a + 128] for a in lanes])

            @pl.loop(1, count + 1)
            def _(i):
                s = score(i)
                scores[i] = s
                row_max[...] = functools.reduce(jnp.maximum, [s[:, a : a + 128] for a in lanes], row_max[...])

            top = jnp.max(row_max[...], axis=-1, keepdims=True) * to_log2
            row_max[...] = jnp.broadcast_to(top, row_max.shape)
            row_sum[...] = jnp.zeros_like(row_sum)
            acc_ref[...] = jnp.zeros_like(acc_ref)

            @pl.loop(0, count + 1)
            def _(i):
                top = row_max[...]
                e = [jnp.exp2(scores[i, :, a : a + 128] * to_log2 - top) for a in lanes]
                row_sum[...] += functools.reduce(jnp.add, e)
                weights = jnp.concatenate([x.astype(BF16) for x in e], axis=-1)
                acc_ref[...] += jnp.dot(weights, vs[group(i)], preferred_element_type=F32)

            out = (acc_ref[...] / jnp.sum(row_sum[...], axis=-1, keepdims=True)).astype(BF16)
            for h in range(heads):
                pieces[half, row_block(plane), h * hd : (h + 1) * hd] = out[h * rows : (h + 1) * rows]

    share = hc // m

    def wo_rows(plane, quarter):
        return pl.ds(pl.multiple_of(plane * hc + quarter * share, 16), share)

    def wo_copy(layer, s):
        src = w_o.at[layer, pl.ds(pl.multiple_of(c * share, 16), share), col_block(ring(z + s, n), width)]
        return remote(src, wo_cols.at[layer, wo_rows(z, c)], osend.at[layer, s - 1], orecv.at[layer, s - 1], tp=ring(z + s, n))

    def wo_pass(layer, s, j):
        here = wo_cols.at[layer, wo_rows(ring(z - s, n), c)]
        return remote(here, here, psend.at[layer, s - 1, j - 1], precv.at[layer, s - 1, j - 1], cp=ring(c + j, m))

    def wo_start(layer):
        for s in range(1, n):
            wo_copy(layer, s).start()

    def wo_event(layer):
        for s in range(1, n):
            wo_copy(layer, s).wait_recv()
            for j in range(1, m):
                wo_pass(layer, s, j).start()

    def wo_wait(layer):
        for s in range(1, n):
            for j in range(1, m):
                wo_pass(layer, s, j).wait_recv()

    span = d // PARTS

    def sum_slot(way, k):
        return k - 1 if way == UP else (0, 3, 4)[k - 1]

    def sum_copy(layer, half, way, q, k, block):
        cols = pl.ds(q * span, span)
        return remote(part.at[half, row_block(block), cols], sums.at[half, sum_slot(way, k), :, cols],
                      rsend.at[layer, half, way, q, k - 1], rrecv.at[layer, half, way, q, k - 1], tp=above if way == UP else below)

    def sum_send(layer, half, q, k):
        @pl.when(z == 0)
        def _():
            sum_copy(layer, half, UP, q, k, n - k).start()

        @pl.when(z == n - 1)
        def _():
            sum_copy(layer, half, DOWN, q, k, k - 1).start()

    def sum_event(layer, half, q, k, way):
        if way == UP:
            here, block, more = both(z >= 1, k >= z), n - 1 + z - k, z < n - 1
        else:
            here, block, more = both(z <= n - 2, k >= n - 1 - z), z + k - n + 1, z > 0
        block = jnp.clip(block, 0, n - 1)

        @pl.when(here)
        def _():
            sum_copy(layer, half, way, q, k, block).wait_recv()
            step = 16

            @pl.loop(0, rows // step)
            def _(i):
                to = pl.ds(pl.multiple_of(block * rows + i * step, step), step)
                frm = pl.ds(pl.multiple_of(i * step, step), step)
                part[half, to, q * span : (q + 1) * span] += sums[half, sum_slot(way, k), frm, q * span : (q + 1) * span]

        if k < n - 1:
            @pl.when(both(here, more))
            def _():
                sum_copy(layer, half, way, q, k + 1, block).start()

    def sum_drain(layer, half):
        for q in range(PARTS):
            for k in range(1, n):
                @pl.when(both(z < n - 1, jnp.logical_or(z == 0, k - 1 >= z)))
                def _(q=q, k=k):
                    sum_copy(layer, half, UP, q, k, 0).wait_send()

                @pl.when(both(z > 0, jnp.logical_or(z == n - 1, k - 1 >= n - 1 - z)))
                def _(q=q, k=k):
                    sum_copy(layer, half, DOWN, q, k, 0).wait_send()

    def finish(half):
        step = 16

        @pl.loop(0, rows // step)
        def _(i):
            r = pl.ds(pl.multiple_of(i * step, step), step)
            mine = part[half, pl.ds(pl.multiple_of(z * rows + i * step, step), step)]
            home[half, r] = (home[half, r].astype(F32) + mine).astype(BF16)

    barrier = pltpu.get_barrier_semaphore()
    for s in (1, n - 1):
        pl.semaphore_signal(barrier, inc=1, device_id={"tp": ring(z + s, n)}, device_id_type=MESH)
    if n > 3:
        pl.semaphore_signal(barrier, inc=1, device_id={"tp": ring(z + 2, n)}, device_id_type=MESH)
    for s in range(1, m):
        pl.semaphore_signal(barrier, inc=1, device_id={"cp": ring(c + s, m)}, device_id_type=MESH)
    pl.semaphore_wait(barrier, n - 1 + m - 1)

    def put(half):
        copy = pltpu.make_async_copy(home.at[half], y_out.at[pl.ds(half * rows, rows)], lsem.at[0])
        copy.start()
        copy.wait()

    def last_sends():
        for i in range(layers):
            for half in (LOW, HIGH):
                gx[i, half].drain((0, 1, 2) if i == 0 else (1, 2))
                go[i, half].drain((1, 2))
                gh[i, half].drain((1, 2))
                for s in range(1, m):
                    kv_copy(i, half, s).wait_send()
            for s in range(1, n):
                wo_copy(i, s).wait_send()
                for j in range(1, m):
                    wo_pass(i, s, j).wait_send()
        for half in (LOW, HIGH):
            sum_drain(layers - 1, half)

    def load_o(layer, half):
        load_cols(go[layer, half], hc)
        go[layer, half].drain((0,))

    ways = {"U": UP, "D": DOWN}
    actions = {
        "x_start": lambda l, h: gx[l, h].start(), "x": lambda l, h, k, way: gx[l, h].event(k, ways[way]), "norm_x": norm_x,
        "o_start": lambda l, h: go[l, h].start(), "o": lambda l, h, k, way: go[l, h].event(k, ways[way]), "load_o": load_o,
        "h_start": lambda l, h: gh[l, h].start(), "h": lambda l, h, k, way: gh[l, h].event(k, ways[way]), "norm_h": norm_h,
        "kv_start": kv_start, "attend": attend, "finish": lambda l, h: finish(h), "put": lambda l, h: put(h),
        "sum_send": sum_send, "sum": lambda l, h, q, k, way: sum_event(l, h, q, k, ways[way]), "sum_drain": sum_drain,
        "wo_start": lambda l, h: wo_start(l), "wo_event": lambda l, h: wo_event(l), "wo_wait": lambda l, h: wo_wait(l),
    }
    kinds = {"qkv": Qkv, "wo": Wo, "gate": GateUp, "down": Down}
    items = []
    for name, l, h, *more in ORDER:
        if name in kinds:
            o = kinds[name](l, h)
            hooks = [(min(o.tiles - 1, tile * o.tiles // TILES[name]), event) for tile, *events in more[0] for event in events]
            items.append((f"{name}_{l}{'AB'[h]}", o, hooks, len(more) > 1))
        else:
            items.append((f"{name}_{l}{'AB'[h]}{''.join(map(str, more))}", functools.partial(actions[name], l, h, *more), None, False))

    ops = [item for item in items if item[2] is not None]
    base = 0
    for _, o, _, _ in ops:
        o.base = base % SLOTS
        base += o.tiles
    follow = {id(o): None if late else o for _, o, _, late in ops}
    after = {id(a[1]): follow[id(b[1])] for a, b in zip(ops, ops[1:])}
    for name, o, hooks, late in items:
        with jax.named_scope(name):
            if hooks is None:
                o()
            else:
                if late:
                    o.prefetch()
                o.run(after.get(id(o)), [(at, functools.partial(actions[event], *args)) for at, (event, *args) in hooks])
    last_sends()


def solution(mesh):
    n = mesh.shape['tp']
    m = mesh.shape['cp']
    row_spec = P(('dp', 'tp', 'cp'), None)
    gain_spec = P(None, None)
    q_spec = P(None, None, 'tp', None)
    col_spec = P(None, None, 'tp')
    o_spec = P(None, 'tp', None, None)
    down_spec = P(None, 'tp', None)

    def body(tokens, norm_attn, norm_mlp, w_q, w_k, w_v, w_o, w_gate, w_up, w_down):
        layers, d, heads, hd = w_q.shape
        rows = tokens.shape[0] // 2
        hc = heads * hd
        width = d // n
        ff = w_gate.shape[2]
        all_rows = n * rows
        c = lax.axis_index('cp')

        inv_freq = 500000.0 ** (-(jnp.arange(hd // 2, dtype=F32) * 2.0 / hd))
        seg = jnp.arange(n) * m + c
        seg = jnp.stack([seg, 2 * n * m - 1 - seg])
        pos = (seg[:, :, None] * rows + jnp.arange(rows)).reshape(2, all_rows)
        angle = pos.astype(F32)[..., None] * inv_freq
        cos, sin = jnp.cos(angle), jnp.sin(angle)
        cos, sin = jnp.concatenate([cos, cos], -1), jnp.concatenate([-sin, sin], -1)

        hbm = pl.BlockSpec(memory_space=pl.ANY)
        vmem = pl.BlockSpec(memory_space=pltpu.VMEM)
        dma = pltpu.SemaphoreType.DMA
        out = pl.pallas_call(
            functools.partial(kernel, n, m, layers),
            out_shape=(
                jax.ShapeDtypeStruct(tokens.shape, BF16),
                jax.ShapeDtypeStruct((layers, 2, n, rows, d), BF16),
                jax.ShapeDtypeStruct((layers, 2, n, all_rows, hc), BF16),
                jax.ShapeDtypeStruct((layers, 2, n, all_rows, width), BF16),
                jax.ShapeDtypeStruct((layers, n * hc, width), BF16),
            ),
            in_specs=[hbm, vmem, vmem, vmem, vmem] + [hbm] * 7,
            out_specs=(hbm,) * 5,
            scratch_shapes=[
                pltpu.VMEM((all_rows, d), BF16),
                pltpu.VMEM((all_rows, d), BF16),
                pltpu.VMEM((all_rows, ff), BF16),
                pltpu.VMEM((2, all_rows, d), F32),
                pltpu.VMEM((2, 5, rows, d), F32),
                pltpu.VMEM((2 * n, heads * rows, m * rows), F32),
                pltpu.VMEM((2 * n, m * rows, hd), BF16),
                pltpu.VMEM((2 * n, m * rows, hd), BF16),
                pltpu.VMEM((layers, 2, m, all_rows, 2 * hd), BF16),
                pltpu.VMEM((n, heads * rows, hd), BF16),
                pltpu.VMEM((2, all_rows, width), BF16),
                pltpu.VMEM((2, all_rows, width), BF16),
                pltpu.VMEM((2, rows, d), BF16),
                pltpu.VMEM((SLOTS, max(d, ff), TILE), BF16),
                pltpu.VMEM((heads * rows, 128), F32),
                pltpu.VMEM((heads * rows, 128), F32),
                pltpu.VMEM((heads * rows, hd), F32),
                dma((SLOTS, n)),
                dma((n,)),
                dma((layers * 6, 2, n - 1)),
                dma((layers * 6, 2, n - 1)),
                dma((layers, 2, m - 1)),
                dma((layers, 2, m - 1)),
                dma((layers, 2, 2, PARTS, n - 1)),
                dma((layers, 2, 2, PARTS, n - 1)),
                dma((layers, n - 1)),
                dma((layers, n - 1)),
                dma((layers, n - 1, m - 1)),
                dma((layers, n - 1, m - 1)),
            ],
            compiler_params=pltpu.CompilerParams(collective_id=0, has_side_effects=True, vmem_limit_bytes=67043328),
            name="two_layers",
        )(tokens, norm_attn, norm_mlp, cos, sin, jnp.swapaxes(w_q, 1, 2), w_k, w_v, w_o.reshape(layers, hc, d), w_gate, w_up, w_down)
        return out[0]

    return jax.shard_map(
        body,
        mesh=mesh,
        in_specs=(row_spec, gain_spec, gain_spec, q_spec, col_spec, col_spec, o_spec, col_spec, col_spec, down_spec),
        out_specs=row_spec,
        check_vma=False,
    )
```

```python
import functools
import math
import jax
import jax.numpy as jnp
from jax import lax
from jax.experimental import pallas as pl
from jax.experimental.pallas import tpu as pltpu
from jax.sharding import PartitionSpec as P

F32 = jnp.float32
BF16 = jnp.bfloat16
MESH = pl.DeviceIdType.MESH
UP, DOWN = 0, 1
X, O, H = 0, 1, 2
LOW, HIGH = 0, 1
SLOTS = 3
PARTS = 2
TILE = 256


def ring(i, n):
    return lax.rem(i + n, n)


def both(*conditions):
    out = conditions[0]
    for c in conditions[1:]:
        out = jnp.logical_and(out, c)
    return out


TILES = {"qkv": 5, "wo": 4, "gate": 37, "down": 14}
ORDER = (
    ("x_start", 0, 0),
    ("x", 0, 0, 1, "D"),
    ("x", 0, 0, 1, "U"),
    ("x_start", 0, 1),
    ("x", 0, 0, 2, "U"),
    ("x", 0, 1, 1, "U"),
    ("x", 0, 0, 3, "U"),
    ("x", 0, 0, 2, "D"),
    ("x", 0, 0, 3, "D"),
    ("x", 0, 1, 1, "D"),
    ("norm_x", 0, 0),
    ("qkv", 0, 0, ((2, ("x", 0, 1, 2, "U"), ("wo_start", 0, 0), ("kv_start", 0, 0)), (3, ("x", 0, 1, 2, "D")),), "late"),
    ("attend", 0, 0),
    ("x", 0, 1, 3, "U"),
    ("x", 0, 1, 3, "D"),
    ("o_start", 0, 0),
    ("norm_x", 0, 1),
    ("qkv", 0, 1, ((3, ("wo_groups", 0, 0), ("kv_start", 0, 1)),)),
    ("wo_chips", 0, 0),
    ("o", 0, 0, 1, "D"),
    ("o", 0, 0, 1, "U"),
    ("attend", 0, 1),
    ("wo_cores", 0, 0),
    ("o", 0, 0, 2, "U"),
    ("o", 0, 0, 2, "D"),
    ("wo_wait", 0, 0),
    ("o", 0, 0, 3, "U"),
    ("o", 0, 0, 3, "D"),
    ("load_o", 0, 0),
    ("wo", 0, 0, (), "late"),
    ("h_start", 0, 0),
    ("o_start", 0, 1),
    ("h", 0, 0, 1, "D"),
    ("h", 0, 0, 1, "U"),
    ("h", 0, 0, 2, "U"),
    ("h", 0, 0, 2, "D"),
    ("o", 0, 1, 1, "D"),
    ("h", 0, 0, 3, "D"),
    ("h", 0, 0, 3, "U"),
    ("o", 0, 1, 1, "U"),
    ("norm_h", 0, 0),
    ("gate", 0, 0, ((17, ("o", 0, 1, 2, "D"), ("o", 0, 1, 2, "U")), (27, ("wo_start", 1, 0)), (35, ("o", 0, 1, 3, "D"), ("o", 0, 1, 3, "U")),)),
    ("load_o", 0, 1),
    ("wo", 0, 1, ()),
    ("h_start", 0, 1),
    ("down", 0, 0, ((9, ("h", 0, 1, 1, "D"), ("h", 0, 1, 1, "U")), (11, ("sum_send", 0, 0, 0, 1)), (12, ("sum_send", 0, 0, 0, 2), ("h", 0, 1, 2, "U"), ("h", 0, 1, 2, "D")), (13, ("sum", 0, 0, 0, 1, "U"), ("wo_groups", 1, 0), ("sum", 0, 0, 0, 1, "D"), ("sum", 0, 0, 0, 2, "U")),)),
    ("sum_send", 0, 0, 1, 1),
    ("h", 0, 1, 3, "D"),
    ("h", 0, 1, 3, "U"),
    ("norm_h", 0, 1),
    ("gate", 0, 1, ((2, ("sum", 0, 0, 1, 1, "D")), (4, ("sum_send", 0, 0, 1, 2)), (10, ("sum", 0, 0, 0, 2, "D")), (19, ("sum_send", 0, 0, 1, 3)), (20, ("sum", 0, 0, 1, 1, "U")), (21, ("wo_chips", 1, 0)), (26, ("sum_send", 0, 0, 0, 3)), (29, ("sum", 0, 0, 1, 2, "U")), (34, ("sum", 0, 0, 1, 2, "D")),)),
    ("down", 0, 1, ((2, ("sum", 0, 0, 0, 3, "D"), ("sum", 0, 0, 0, 3, "U"), ("sum", 0, 0, 1, 3, "D"), ("sum", 0, 0, 1, 3, "U"), ("finish", 0, 0)), (3, ("x_start", 1, 0)), (8, ("wo_cores", 1, 0), ("sum_send", 0, 1, 0, 1)), (10, ("sum_send", 0, 1, 0, 2)), (11, ("x", 1, 0, 1, "D"), ("x", 1, 0, 1, "U"), ("sum", 0, 1, 0, 1, "D")),)),
    ("x", 1, 0, 2, "D"),
    ("sum_send", 0, 1, 1, 1),
    ("x", 1, 0, 3, "D"),
    ("sum", 0, 1, 0, 1, "U"),
    ("sum_send", 0, 1, 0, 3),
    ("x", 1, 0, 2, "U"),
    ("x", 1, 0, 3, "U"),
    ("sum", 0, 1, 0, 2, "U"),
    ("norm_x", 1, 0),
    ("sum", 0, 1, 0, 2, "D"),
    ("qkv", 1, 0, ((2, ("kv_start", 1, 0), ("sum_send", 0, 1, 1, 2), ("wo_wait", 1, 0)), (4, ("sum", 0, 1, 1, 1, "D")),)),
    ("attend", 1, 0),
    ("o_start", 1, 0),
    ("sum", 0, 1, 1, 2, "D"),
    ("sum", 0, 1, 1, 1, "U"),
    ("o", 1, 0, 1, "U"),
    ("sum", 0, 1, 1, 2, "U"),
    ("o", 1, 0, 1, "D"),
    ("sum", 0, 1, 0, 3, "D"),
    ("sum_send", 0, 1, 1, 3),
    ("o", 1, 0, 2, "U"),
    ("sum", 0, 1, 1, 3, "U"),
    ("sum", 0, 1, 0, 3, "U"),
    ("sum", 0, 1, 1, 3, "D"),
    ("finish", 0, 1),
    ("x_start", 1, 1),
    ("o", 1, 0, 2, "D"),
    ("o", 1, 0, 3, "D"),
    ("sum_drain", 0, 0),
    ("o", 1, 0, 3, "U"),
    ("x", 1, 1, 1, "U"),
    ("x", 1, 1, 1, "D"),
    ("load_o", 1, 0),
    ("x", 1, 1, 2, "U"),
    ("wo", 1, 0, ((2, ("x", 1, 1, 2, "D")),)),
    ("h_start", 1, 0),
    ("x", 1, 1, 3, "D"),
    ("x", 1, 1, 3, "U"),
    ("norm_x", 1, 1),
    ("qkv", 1, 1, ((2, ("kv_start", 1, 1)), (4, ("h", 1, 0, 1, "U"), ("h", 1, 0, 1, "D")),)),
    ("attend", 1, 1),
    ("h", 1, 0, 2, "U"),
    ("h", 1, 0, 2, "D"),
    ("o_start", 1, 1),
    ("h", 1, 0, 3, "D"),
    ("h", 1, 0, 3, "U"),
    ("norm_h", 1, 0),
    ("gate", 1, 0, ((14, ("o", 1, 1, 1, "U")), (24, ("o", 1, 1, 1, "D")), (35, ("o", 1, 1, 2, "U")),)),
    ("down", 1, 0, ((4, ("o", 1, 1, 2, "D")), (7, ("sum_send", 1, 0, 0, 1)), (11, ("o", 1, 1, 3, "U")),)),
    ("o", 1, 1, 3, "D"),
    ("load_o", 1, 1),
    ("wo", 1, 1, ()),
    ("h_start", 1, 1),
    ("sum_send", 1, 0, 1, 1),
    ("sum_send", 1, 0, 0, 2),
    ("sum_send", 1, 0, 1, 2),
    ("h", 1, 1, 1, "D"),
    ("h", 1, 1, 1, "U"),
    ("h", 1, 1, 2, "D"),
    ("h", 1, 1, 2, "U"),
    ("h", 1, 1, 3, "D"),
    ("h", 1, 1, 3, "U"),
    ("norm_h", 1, 1),
    ("gate", 1, 1, ((4, ("sum_send", 1, 0, 0, 3)), (5, ("sum", 1, 0, 0, 1, "D")), (14, ("sum_drain", 0, 1), ("sum_send", 1, 0, 1, 3)), (23, ("sum", 1, 0, 1, 1, "D")), (24, ("sum", 1, 0, 1, 1, "U")),)),
    ("sum", 1, 0, 0, 2, "D"),
    ("down", 1, 1, ((1, ("sum", 1, 0, 1, 2, "U")), (2, ("sum", 1, 0, 0, 1, "U")), (3, ("sum", 1, 0, 0, 3, "D")), (4, ("sum", 1, 0, 0, 2, "U")), (6, ("sum", 1, 0, 1, 2, "D")), (7, ("sum_send", 1, 1, 0, 1)), (8, ("sum", 1, 1, 0, 1, "U")), (9, ("sum", 1, 1, 0, 1, "D"), ("sum_send", 1, 1, 0, 2)), (10, ("sum", 1, 1, 0, 2, "U"), ("sum", 1, 0, 1, 3, "U")), (13, ("sum", 1, 1, 0, 2, "D")),)),
    ("sum", 1, 0, 1, 3, "D"),
    ("sum_send", 1, 1, 1, 1),
    ("sum", 1, 0, 0, 3, "U"),
    ("sum", 1, 1, 1, 1, "U"),
    ("finish", 1, 0),
    ("sum_send", 1, 1, 0, 3),
    ("sum_send", 1, 1, 1, 2),
    ("sum_send", 1, 1, 1, 3),
    ("put", 1, 0),
    ("sum", 1, 1, 1, 1, "D"),
    ("sum", 1, 1, 0, 3, "D"),
    ("sum", 1, 1, 0, 3, "U"),
    ("sum", 1, 1, 1, 2, "U"),
    ("sum", 1, 1, 1, 2, "D"),
    ("sum", 1, 1, 1, 3, "U"),
    ("sum", 1, 1, 1, 3, "D"),
    ("finish", 1, 1),
    ("put", 1, 1),
)


def kernel(n, m, groups, layers, tokens, gain_a, gain_m, cos_ref, sin_ref, w_q, w_k, w_v, w_o, w_gate, w_up, w_down,
           y_out, g_x, g_o, g_h, wo_cols,
           stage, lhs, act, part, sums, scores, ks, vs, kvs, qs, x_cols, pieces, home, wbuf, row_max, row_sum, acc_ref,
           wsem, lsem, gsend, grecv, ksend, krecv, rsend, rrecv, osend, orecv, psend, precv):
    z = lax.axis_index("tp")
    c = lax.axis_index("cp")
    g = lax.axis_index("dp")
    rows = tokens.shape[0] // 2
    d = tokens.shape[1]
    all_rows = n * rows
    heads, hd = w_q.shape[1], w_q.shape[3]
    hc = heads * hd
    width = d // n
    ff = w_gate.shape[2]
    above = jnp.minimum(z + 1, n - 1)
    below = jnp.maximum(z - 1, 0)

    def remote(src, dst, send, recv, **where):
        return pltpu.make_async_remote_copy(src_ref=src, dst_ref=dst, send_sem=send, recv_sem=recv, device_id=where,
                                            device_id_type=MESH)

    def row_block(p):
        return pl.ds(pl.multiple_of(p * rows, 16), rows)

    def col_block(p, w):
        return pl.ds(pl.multiple_of(p * w, 128), w)

    class Gather:
        def __init__(self, layer, half, kind, buf, own):
            self.i = (layer * 2 + half) * 3 + kind
            self.buf, self.own = buf, own

        def copy(self, way, k, plane):
            src = self.own if k == 0 else self.buf.at[plane]
            return remote(src, self.buf.at[plane], gsend.at[self.i, way, k], grecv.at[self.i, way, k],
                          tp=above if way == UP else below)

        def start(self):
            @pl.when(z < n - 1)
            def _():
                self.copy(UP, 0, z).start()

            @pl.when(z > 0)
            def _():
                self.copy(DOWN, 0, z).start()

        def event(self, k, way):
            plane = jnp.maximum(z - k, 0) if way == UP else jnp.minimum(z + k, n - 1)
            here = z >= k if way == UP else z + k < n

            @pl.when(here)
            def _():
                self.copy(way, k - 1, plane).wait_recv()

            if k < n - 1:
                @pl.when(both(here, z < n - 1 if way == UP else z > 0))
                def _():
                    self.copy(way, k, plane).start()

        def drain(self, ks):
            for k in ks:
                @pl.when(both(z >= k, z < n - 1))
                def _(k=k):
                    self.copy(UP, k, z).wait_send()

                @pl.when(both(z + k < n, z > 0))
                def _(k=k):
                    self.copy(DOWN, k, z).wait_send()

    def own_x(layer, half):
        return tokens.at[pl.ds(half * rows, rows)] if layer == 0 else home.at[half]

    gx = {(l, h): Gather(l, h, X, g_x.at[l, h], own_x(l, h)) for l in range(layers) for h in (LOW, HIGH)}
    go = {(l, h): Gather(l, h, O, g_o.at[l, h], pieces.at[h]) for l in range(layers) for h in (LOW, HIGH)}
    gh = {(l, h): Gather(l, h, H, g_h.at[l, h], pieces.at[h]) for l in range(layers) for h in (LOW, HIGH)}

    def load(buf, own, where):
        copies = [pltpu.make_async_copy(own, stage.at[where(z)], lsem.at[0])]
        for k in range(1, n):
            p = ring(z + k, n)
            copies.append(pltpu.make_async_copy(buf.at[p], stage.at[where(p)], lsem.at[k]))
        for copy in copies:
            copy.start()
        for copy in copies:
            copy.wait()

    def load_rows(gather):
        load(gather.buf, gather.own, row_block)

    def load_cols(gather, w):
        load(gather.buf, gather.own, lambda p: (slice(None), col_block(p, w)))

    def norm(gain):
        step = 32

        @pl.loop(0, all_rows // step)
        def _(i):
            r = pl.ds(pl.multiple_of(i * step, step), step)
            x = stage[r].astype(F32)
            inv = lax.rsqrt(jnp.mean(x * x, axis=-1, keepdims=True) + 1e-5)
            lhs[r] = (x * inv * gain[...].astype(F32)).astype(BF16)

    def norm_x(layer, half):
        load_rows(gx[layer, half])
        norm(gain_a.at[pl.ds(layer, 1)])
        x_cols[half] = stage[:, col_block(z, width)]

    def norm_h(layer, half):
        load_cols(gh[layer, half], width)
        norm(gain_m.at[pl.ds(layer, 1)])
        gh[layer, half].drain((0,))
        if layer > 0:
            gx[layer, half].drain((0,))
        home[half] = stage[row_block(z)]

    class Op:
        base = None

        def start(self, i, slot):
            for copy in self.copies(i, slot):
                copy.start()

        def prefetch(self):
            for i in range(2):
                self.start(i, (self.base + i) % SLOTS)

        def run(self, follow, hooks):
            @pl.loop(0, self.tiles)
            def _(i):
                for at, event in hooks:
                    pl.when(i == at)(event)
                slot, later = lax.rem(self.base + i, SLOTS), lax.rem(self.base + i + 2, SLOTS)

                @pl.when(i + 2 < self.tiles)
                def _():
                    self.start(i + 2, later)

                if follow is not None:
                    @pl.when(i + 2 >= self.tiles)
                    def _():
                        follow.start(i + 2 - self.tiles, later)

                for copy in self.copies(i, slot):
                    copy.wait()
                self.compute(i, slot)

    def dot(a, slot, depth):
        return jnp.dot(a, wbuf[slot, :depth], preferred_element_type=F32)

    def tile_start(i, total):
        return pl.multiple_of(jnp.minimum(i * TILE, total - TILE), 128)

    class Qkv(Op):
        def __init__(self, layer, half):
            self.layer, self.half = layer, half
            self.tiles = 1 + -(-hc // TILE)

        def start(self, i, slot):
            def pair(a, b):
                pltpu.make_async_copy(a, wbuf.at[slot, pl.ds(0, d), pl.ds(0, hd)], wsem.at[slot, 0]).start()
                pltpu.make_async_copy(b, wbuf.at[slot, pl.ds(0, d), pl.ds(hd, hd)], wsem.at[slot, 1]).start()

            @pl.when(i == 0)
            def _():
                pair(w_k.at[self.layer], w_v.at[self.layer])

            @pl.when(i > 0)
            def _():
                h = tile_start(i - 1, hc) // hd
                pair(w_q.at[self.layer, h], w_q.at[self.layer, h + 1])

        def copies(self, i, slot):
            return [pltpu.make_async_copy(w_k.at[self.layer], wbuf.at[slot, pl.ds(0, d), pl.ds(j * hd, hd)], wsem.at[slot, j])
                    for j in range(2)]

        def compute(self, i, slot):
            out = dot(lhs[...], slot, d)

            def turned(x):
                return (x * cos_ref[self.half] + pltpu.roll(x, hd // 2, 1) * sin_ref[self.half]).astype(BF16)

            @pl.when(i == 0)
            def _():
                kvs[self.layer, self.half, 0, :, :hd] = turned(out[:, :hd])
                kvs[self.layer, self.half, 0, :, hd:] = out[:, hd:].astype(BF16)

            @pl.when(i > 0)
            def _():
                h = tile_start(i - 1, hc) // hd
                for j in range(2):
                    q = turned(out[:, j * hd : (j + 1) * hd])
                    for p in range(n):
                        qs[p, row_block(h + j)] = q[p * rows : (p + 1) * rows]

    class Wo(Op):
        def __init__(self, layer, half):
            self.layer, self.half = layer, half
            self.tiles = -(-width // TILE)

        def copies(self, i, slot):
            at = tile_start(i, width)
            out = [pltpu.make_async_copy(w_o.at[self.layer, :, pl.ds(pl.multiple_of(z * width + at, 128), TILE)],
                                         wbuf.at[slot, pl.ds(pl.multiple_of(z * hc, 128), hc)], wsem.at[slot, 0])]
            for k in range(1, n):
                p = ring(z + k, n)
                block = pl.ds(pl.multiple_of(p * hc, 128), hc)
                out.append(pltpu.make_async_copy(wo_cols.at[self.layer, block, pl.ds(at, TILE)], wbuf.at[slot, block],
                                                 wsem.at[slot, k]))
            return out

        def compute(self, i, slot):
            cols = pl.ds(tile_start(i, width), TILE)
            out = dot(stage[...], slot, d) + x_cols[self.half, :, cols].astype(F32)
            pieces[self.half, :, cols] = out.astype(BF16)

    class GateUp(Op):
        def __init__(self, layer, half):
            self.layer, self.half = layer, half
            self.tiles = ff // 128

        def copies(self, i, slot):
            cols = pl.ds(pl.multiple_of(i * 128, 128), 128)
            return [pltpu.make_async_copy(w.at[self.layer, :, cols], wbuf.at[slot, pl.ds(0, d), pl.ds(128 * j, 128)], wsem.at[slot, j])
                    for j, w in enumerate((w_gate, w_up))]

        def compute(self, i, slot):
            out = dot(lhs[...], slot, d)
            gate = out[:, :128]
            act[:, pl.ds(pl.multiple_of(i * 128, 128), 128)] = (gate * lax.logistic(gate) * out[:, 128:]).astype(BF16)

    class Down(Op):
        def __init__(self, layer, half):
            self.layer, self.half = layer, half
            self.tiles = d // TILE

        def copies(self, i, slot):
            cols = pl.ds(pl.multiple_of(i * TILE, TILE), TILE)
            return [pltpu.make_async_copy(w_down.at[self.layer, :, cols], wbuf.at[slot, pl.ds(0, ff)], wsem.at[slot, 0])]

        def compute(self, i, slot):
            part[self.half, :, pl.ds(pl.multiple_of(i * TILE, TILE), TILE)] = dot(act[...], slot, ff)

    def kv_copy(layer, half, s):
        return remote(kvs.at[layer, half, 0], kvs.at[layer, half, s], ksend.at[layer, half, s - 1], krecv.at[layer, half, s - 1],
                      cp=ring(c + s, m))

    def kv_start(layer, half):
        for s in range(1, m):
            kv_copy(layer, half, s).start()

    def kv_wait(layer, half):
        for s in range(1, m):
            kv_copy(layer, half, s).wait_recv()

    def attend(layer, half):
        kv_wait(layer, half)
        keys = m * rows
        for s in range(m):
            for g in range(n):
                block = slice(g * rows, (g + 1) * rows)
                ks[half * n + g, s * rows : (s + 1) * rows] = kvs[layer, half, s, block, :hd]
                vs[half * n + g, s * rows : (s + 1) * rows] = kvs[layer, half, s, block, hd:]
        to_log2 = math.log2(math.e) / math.sqrt(hd)
        lanes = range(0, keys, 128)

        @pl.loop(0, n)
        def _(plane):
            count = plane if half == LOW else 2 * n - 1 - plane

            def group(i):
                if half == LOW:
                    return jnp.where(i == 0, plane, i - 1)
                return jnp.where(i == 0, n + plane, jnp.where(i <= n, i - 1, i + plane))

            def score(i):
                return lax.dot_general(qs[plane], ks[group(i)], (((1,), (1,)), ((), ())), preferred_element_type=F32)

            row = lax.broadcasted_iota(jnp.int32, (rows, keys), 0)
            col = lax.broadcasted_iota(jnp.int32, (rows, keys), 1)
            slot = col // rows
            other = lax.rem(c - slot + m, m)
            limit = jnp.where(slot == 0, row, jnp.where((other < c) if half == LOW else (other > c), keys, -1))
            bias = jnp.where(col <= limit, 0.0, -jnp.inf)
            s = (score(0).reshape(heads, rows, keys) + bias[None]).reshape(heads * rows, keys)
            scores[0] = s
            row_max[...] = functools.reduce(jnp.maximum, [s[:, a : a + 128] for a in lanes])

            @pl.loop(1, count + 1)
            def _(i):
                s = score(i)
                scores[i] = s
                row_max[...] = functools.reduce(jnp.maximum, [s[:, a : a + 128] for a in lanes], row_max[...])

            top = jnp.max(row_max[...], axis=-1, keepdims=True) * to_log2
            row_max[...] = jnp.broadcast_to(top, row_max.shape)
            row_sum[...] = jnp.zeros_like(row_sum)
            acc_ref[...] = jnp.zeros_like(acc_ref)

            @pl.loop(0, count + 1)
            def _(i):
                top = row_max[...]
                e = [jnp.exp2(scores[i, :, a : a + 128] * to_log2 - top) for a in lanes]
                row_sum[...] += functools.reduce(jnp.add, e)
                weights = jnp.concatenate([x.astype(BF16) for x in e], axis=-1)
                acc_ref[...] += jnp.dot(weights, vs[group(i)], preferred_element_type=F32)

            out = (acc_ref[...] / jnp.sum(row_sum[...], axis=-1, keepdims=True)).astype(BF16)
            for h in range(heads):
                pieces[half, row_block(plane), h * hd : (h + 1) * hd] = out[h * rows : (h + 1) * rows]

    share = hc // m // groups
    other_chip, other_core = ring(c + 2, m), c + 1 - 2 * lax.rem(c, 2)

    def wo_rows(plane, quarter):
        return pl.ds(pl.multiple_of(plane * hc + quarter * (hc // m), 16), hc // m)

    def wo_share(layer, plane, group):
        return wo_cols.at[layer, pl.ds(pl.multiple_of(plane * hc + c * (hc // m) + group * share, 16), share)]

    def wo_copy(layer, s):
        src = w_o.at[layer, pl.ds(pl.multiple_of(c * (hc // m) + g * share, 16), share), col_block(ring(z + s, n), width)]
        return remote(src, wo_share(layer, z, g), osend.at[layer, s - 1], orecv.at[layer, s - 1], tp=ring(z + s, n))

    def wo_swap(layer, s):
        here = wo_share(layer, ring(z - s, n), g)
        return remote(here, here, psend.at[layer, s - 1, 3], precv.at[layer, s - 1, 3], dp=ring(g + 1, groups))

    def wo_pass(layer, s, j):
        here = wo_cols.at[layer, wo_rows(ring(z - s, n), other_chip if j == 2 else c)]
        return remote(here, here, psend.at[layer, s - 1, j], precv.at[layer, s - 1, j], cp=other_chip if j == 0 else other_core)

    def wo_start(layer):
        for s in range(1, n):
            wo_copy(layer, s).start()

    def wo_groups(layer):
        for s in range(1, n):
            wo_copy(layer, s).wait_recv()
            if groups > 1:
                wo_swap(layer, s).start()

    def wo_chips(layer):
        for s in range(1, n):
            if groups > 1:
                wo_swap(layer, s).wait_recv()
            wo_pass(layer, s, 0).start()
            wo_pass(layer, s, 1).start()

    def wo_cores(layer):
        for s in range(1, n):
            wo_pass(layer, s, 0).wait_recv()
            wo_pass(layer, s, 2).start()

    def wo_wait(layer):
        for s in range(1, n):
            wo_pass(layer, s, 1).wait_recv()
            wo_pass(layer, s, 2).wait_recv()

    span = d // PARTS

    def sum_slot(way, k):
        return k - 1 if way == UP else (0, 3, 4)[k - 1]

    def sum_copy(layer, half, way, q, k, block):
        cols = pl.ds(q * span, span)
        return remote(part.at[half, row_block(block), cols], sums.at[half, sum_slot(way, k), :, cols],
                      rsend.at[layer, half, way, q, k - 1], rrecv.at[layer, half, way, q, k - 1], tp=above if way == UP else below)

    def sum_send(layer, half, q, k):
        @pl.when(z == 0)
        def _():
            sum_copy(layer, half, UP, q, k, n - k).start()

        @pl.when(z == n - 1)
        def _():
            sum_copy(layer, half, DOWN, q, k, k - 1).start()

    def sum_event(layer, half, q, k, way):
        if way == UP:
            here, block, more = both(z >= 1, k >= z), n - 1 + z - k, z < n - 1
        else:
            here, block, more = both(z <= n - 2, k >= n - 1 - z), z + k - n + 1, z > 0
        block = jnp.clip(block, 0, n - 1)

        @pl.when(here)
        def _():
            sum_copy(layer, half, way, q, k, block).wait_recv()
            step = 16

            @pl.loop(0, rows // step)
            def _(i):
                to = pl.ds(pl.multiple_of(block * rows + i * step, step), step)
                frm = pl.ds(pl.multiple_of(i * step, step), step)
                part[half, to, q * span : (q + 1) * span] += sums[half, sum_slot(way, k), frm, q * span : (q + 1) * span]

        if k < n - 1:
            @pl.when(both(here, more))
            def _():
                sum_copy(layer, half, way, q, k + 1, block).start()

    def sum_drain(layer, half):
        for q in range(PARTS):
            for k in range(1, n):
                @pl.when(both(z < n - 1, jnp.logical_or(z == 0, k - 1 >= z)))
                def _(q=q, k=k):
                    sum_copy(layer, half, UP, q, k, 0).wait_send()

                @pl.when(both(z > 0, jnp.logical_or(z == n - 1, k - 1 >= n - 1 - z)))
                def _(q=q, k=k):
                    sum_copy(layer, half, DOWN, q, k, 0).wait_send()

    def finish(half):
        step = 16

        @pl.loop(0, rows // step)
        def _(i):
            r = pl.ds(pl.multiple_of(i * step, step), step)
            mine = part[half, pl.ds(pl.multiple_of(z * rows + i * step, step), step)]
            home[half, r] = (home[half, r].astype(F32) + mine).astype(BF16)

    barrier = pltpu.get_barrier_semaphore()
    partners = [{axis: ring(i + s, size)} for axis, i, size in (("tp", z, n), ("cp", c, m), ("dp", g, groups)) for s in range(1, size)]
    for partner in partners:
        pl.semaphore_signal(barrier, inc=1, device_id=partner, device_id_type=MESH)
    pl.semaphore_wait(barrier, len(partners))

    def put(half):
        copy = pltpu.make_async_copy(home.at[half], y_out.at[pl.ds(half * rows, rows)], lsem.at[0])
        copy.start()
        copy.wait()

    def last_sends():
        for i in range(layers):
            for half in (LOW, HIGH):
                gx[i, half].drain((0, 1, 2) if i == 0 else (1, 2))
                go[i, half].drain((1, 2))
                gh[i, half].drain((1, 2))
                for s in range(1, m):
                    kv_copy(i, half, s).wait_send()
            for s in range(1, n):
                wo_copy(i, s).wait_send()
                for j in range(3):
                    wo_pass(i, s, j).wait_send()
                if groups > 1:
                    wo_swap(i, s).wait_send()
        for half in (LOW, HIGH):
            sum_drain(layers - 1, half)

    def load_o(layer, half):
        load_cols(go[layer, half], hc)
        go[layer, half].drain((0,))

    ways = {"U": UP, "D": DOWN}
    actions = {
        "x_start": lambda l, h: gx[l, h].start(), "x": lambda l, h, k, way: gx[l, h].event(k, ways[way]), "norm_x": norm_x,
        "o_start": lambda l, h: go[l, h].start(), "o": lambda l, h, k, way: go[l, h].event(k, ways[way]), "load_o": load_o,
        "h_start": lambda l, h: gh[l, h].start(), "h": lambda l, h, k, way: gh[l, h].event(k, ways[way]), "norm_h": norm_h,
        "kv_start": kv_start, "attend": attend, "finish": lambda l, h: finish(h), "put": lambda l, h: put(h),
        "sum_send": sum_send, "sum": lambda l, h, q, k, way: sum_event(l, h, q, k, ways[way]), "sum_drain": sum_drain,
        "wo_start": lambda l, h: wo_start(l), "wo_groups": lambda l, h: wo_groups(l), "wo_chips": lambda l, h: wo_chips(l),
        "wo_cores": lambda l, h: wo_cores(l), "wo_wait": lambda l, h: wo_wait(l),
    }
    kinds = {"qkv": Qkv, "wo": Wo, "gate": GateUp, "down": Down}
    items = []
    for name, l, h, *more in ORDER:
        if name in kinds:
            o = kinds[name](l, h)
            hooks = [(min(o.tiles - 1, tile * o.tiles // TILES[name]), event) for tile, *events in more[0] for event in events]
            items.append((f"{name}_{l}{'AB'[h]}", o, hooks, len(more) > 1))
        else:
            items.append((f"{name}_{l}{'AB'[h]}{''.join(map(str, more))}", functools.partial(actions[name], l, h, *more), None, False))

    ops = [item for item in items if item[2] is not None]
    base = 0
    for _, o, _, _ in ops:
        o.base = base % SLOTS
        base += o.tiles
    follow = {id(o): None if late else o for _, o, _, late in ops}
    after = {id(a[1]): follow[id(b[1])] for a, b in zip(ops, ops[1:])}
    for name, o, hooks, late in items:
        with jax.named_scope(name):
            if hooks is None:
                o()
            else:
                if late:
                    o.prefetch()
                o.run(after.get(id(o)), [(at, functools.partial(actions[event], *args)) for at, (event, *args) in hooks])
    last_sends()


def solution(mesh):
    n = mesh.shape['tp']
    m = mesh.shape['cp']
    groups = mesh.shape['dp']
    row_spec = P(('dp', 'tp', 'cp'), None)
    gain_spec = P(None, None)
    q_spec = P(None, None, 'tp', None)
    col_spec = P(None, None, 'tp')
    o_spec = P(None, 'tp', None, None)
    down_spec = P(None, 'tp', None)

    def body(tokens, norm_attn, norm_mlp, w_q, w_k, w_v, w_o, w_gate, w_up, w_down):
        layers, d, heads, hd = w_q.shape
        rows = tokens.shape[0] // 2
        hc = heads * hd
        width = d // n
        ff = w_gate.shape[2]
        all_rows = n * rows
        c = lax.axis_index('cp')

        inv_freq = 500000.0 ** (-(jnp.arange(hd // 2, dtype=F32) * 2.0 / hd))
        seg = jnp.arange(n) * m + c
        seg = jnp.stack([seg, 2 * n * m - 1 - seg])
        pos = (seg[:, :, None] * rows + jnp.arange(rows)).reshape(2, all_rows)
        angle = pos.astype(F32)[..., None] * inv_freq
        cos, sin = jnp.cos(angle), jnp.sin(angle)
        cos, sin = jnp.concatenate([cos, cos], -1), jnp.concatenate([-sin, sin], -1)

        hbm = pl.BlockSpec(memory_space=pl.ANY)
        vmem = pl.BlockSpec(memory_space=pltpu.VMEM)
        dma = pltpu.SemaphoreType.DMA
        out = pl.pallas_call(
            functools.partial(kernel, n, m, groups, layers),
            out_shape=(
                jax.ShapeDtypeStruct(tokens.shape, BF16),
                jax.ShapeDtypeStruct((layers, 2, n, rows, d), BF16),
                jax.ShapeDtypeStruct((layers, 2, n, all_rows, hc), BF16),
                jax.ShapeDtypeStruct((layers, 2, n, all_rows, width), BF16),
                jax.ShapeDtypeStruct((layers, n * hc, width), BF16),
            ),
            in_specs=[hbm, vmem, vmem, vmem, vmem] + [hbm] * 7,
            out_specs=(hbm,) * 5,
            scratch_shapes=[
                pltpu.VMEM((all_rows, d), BF16),
                pltpu.VMEM((all_rows, d), BF16),
                pltpu.VMEM((all_rows, ff), BF16),
                pltpu.VMEM((2, all_rows, d), F32),
                pltpu.VMEM((2, 5, rows, d), F32),
                pltpu.VMEM((2 * n, heads * rows, m * rows), F32),
                pltpu.VMEM((2 * n, m * rows, hd), BF16),
                pltpu.VMEM((2 * n, m * rows, hd), BF16),
                pltpu.VMEM((layers, 2, m, all_rows, 2 * hd), BF16),
                pltpu.VMEM((n, heads * rows, hd), BF16),
                pltpu.VMEM((2, all_rows, width), BF16),
                pltpu.VMEM((2, all_rows, width), BF16),
                pltpu.VMEM((2, rows, d), BF16),
                pltpu.VMEM((SLOTS, max(d, ff), TILE), BF16),
                pltpu.VMEM((heads * rows, 128), F32),
                pltpu.VMEM((heads * rows, 128), F32),
                pltpu.VMEM((heads * rows, hd), F32),
                dma((SLOTS, n)),
                dma((n,)),
                dma((layers * 6, 2, n - 1)),
                dma((layers * 6, 2, n - 1)),
                dma((layers, 2, m - 1)),
                dma((layers, 2, m - 1)),
                dma((layers, 2, 2, PARTS, n - 1)),
                dma((layers, 2, 2, PARTS, n - 1)),
                dma((layers, n - 1)),
                dma((layers, n - 1)),
                dma((layers, n - 1, 4)),
                dma((layers, n - 1, 4)),
            ],
            compiler_params=pltpu.CompilerParams(collective_id=0, has_side_effects=True, vmem_limit_bytes=67043328),
            name="two_layers",
        )(tokens, norm_attn, norm_mlp, cos, sin, jnp.swapaxes(w_q, 1, 2), w_k, w_v, w_o.reshape(layers, hc, d), w_gate, w_up, w_down)
        return out[0]

    return jax.shard_map(
        body,
        mesh=mesh,
        in_specs=(row_spec, gain_spec, gain_spec, q_spec, col_spec, col_spec, o_spec, col_spec, col_spec, down_spec),
        out_specs=row_spec,
        check_vma=False,
    )
```

```python
import functools
import math
import jax
import jax.numpy as jnp
from jax import lax
from jax.experimental import pallas as pl
from jax.experimental.pallas import tpu as pltpu
from jax.sharding import PartitionSpec as P

F32 = jnp.float32
BF16 = jnp.bfloat16
MESH = pl.DeviceIdType.MESH
UP, DOWN = 0, 1
LOW, HIGH = 0, 1
SLOTS = 4
PARTS = 2
TILE = 256


def ring(i, n):
    return lax.rem(i + n, n)


def both(*conditions):
    out = conditions[0]
    for c in conditions[1:]:
        out = jnp.logical_and(out, c)
    return out


TILES = {"qkv": 5, "wo": 7, "gate": 37, "down": 14}
ORDER = (
    ("x_start", 0, 0),
    ("x", 0, 0, 1, "L", "I"),
    ("x", 0, 0, 1, "R", "I"),
    ("x", 0, 0, 1, "R", "E"),
    ("wo_start", 0, 0),
    ("x", 0, 0, 2, "R", "E"),
    ("x", 0, 0, 2, "R", "I"),
    ("x_start", 0, 1),
    ("x", 0, 0, 3, "R", "E"),
    ("norm_x", 0, 0),
    ("qkv", 0, 0, ((2, ("kv_start", 0, 0), ("wo_groups", 0, 0), ("x", 0, 1, 1, "R", "E"), ("x", 0, 1, 1, "L", "I")), (4, ("wo_chips", 0, 0)),), "late"),
    ("attend", 0, 0),
    ("x", 0, 1, 1, "R", "I"),
    ("o_start", 0, 0),
    ("x", 0, 1, 2, "R", "E"),
    ("x", 0, 1, 3, "R", "E"),
    ("o", 0, 0, 1, "R", "I"),
    ("x", 0, 1, 2, "R", "I"),
    ("o", 0, 0, 1, "L", "I"),
    ("norm_x", 0, 1),
    ("qkv", 0, 1, ((2, ("wo_start", 1, 0), ("kv_start", 0, 1)),)),
    ("wo_cores", 0, 0),
    ("o", 0, 0, 2, "R", "I"),
    ("load_o", 0, 0),
    ("wo_wait", 0, 0),
    ("wo", 0, 0, ((5, ("h_start", 0, 0, 0)),), "late"),
    ("h_start", 0, 0, 1),
    ("attend", 0, 1),
    ("o_start", 0, 1),
    ("h", 0, 0, 0, 1, "R", "I"),
    ("h", 0, 0, 0, 1, "R", "E"),
    ("h", 0, 0, 1, 1, "R", "E"),
    ("h", 0, 0, 0, 2, "R", "E"),
    ("h", 0, 0, 1, 2, "R", "E"),
    ("h", 0, 0, 1, 1, "R", "I"),
    ("norm_h", 0, 0),
    ("gate", 0, 0, ((16, ("o", 0, 1, 1, "L", "I")), (18, ("wo_groups", 1, 0)), (28, ("o", 0, 1, 1, "R", "I")), (31, ("o", 0, 1, 2, "R", "I")),)),
    ("load_o", 0, 1),
    ("wo", 0, 1, ((6, ("h_start", 0, 1, 0)),)),
    ("down", 0, 0, ((7, ("sum_send", 0, 0, 0, 1)), (8, ("h_start", 0, 1, 1)), (10, ("h", 0, 1, 0, 1, "R", "E")), (11, ("h", 0, 1, 0, 1, "R", "I"), ("sum_send", 0, 0, 0, 2)), (12, ("h", 0, 1, 1, 1, "R", "E")), (13, ("h", 0, 1, 1, 1, "R", "I")),)),
    ("sum_send", 0, 0, 1, 1),
    ("sum", 0, 0, 0, 1, "L", "I"),
    ("h", 0, 1, 1, 2, "R", "E"),
    ("h", 0, 1, 0, 2, "R", "E"),
    ("norm_h", 0, 1),
    ("sum_send", 0, 0, 1, 2),
    ("gate", 0, 1, ((3, ("sum", 0, 0, 0, 2, "L", "I")), (6, ("sum", 0, 0, 0, 2, "R", "I")), (11, ("sum", 0, 0, 1, 1, "L", "I")), (17, ("sum_send", 0, 0, 0, 3)), (18, ("sum", 0, 0, 0, 3, "R", "E")), (19, ("sum", 0, 0, 1, 2, "L", "I")), (22, ("wo_chips", 1, 0), ("sum_send", 0, 0, 1, 3)),)),
    ("down", 0, 1, ((6, ("sum", 0, 0, 0, 3, "R", "I")), (7, ("sum", 0, 0, 1, 2, "R", "I"), ("sum", 0, 0, 0, 3, "L", "I")), (12, ("sum_send", 0, 1, 0, 1), ("sum", 0, 0, 1, 3, "R", "I"), ("sum", 0, 0, 1, 3, "R", "E"), ("sum", 0, 0, 1, 3, "L", "I"), ("finish", 0, 0), ("sum_drain", 0, 0)), (13, ("x_start", 1, 0)),)),
    ("sum", 0, 1, 0, 1, "L", "I"),
    ("x", 1, 0, 1, "L", "I"),
    ("sum_send", 0, 1, 0, 2),
    ("x", 1, 0, 1, "R", "I"),
    ("x", 1, 0, 1, "R", "E"),
    ("sum_send", 0, 1, 1, 1),
    ("x", 1, 0, 2, "R", "E"),
    ("sum_send", 0, 1, 1, 2),
    ("wo_cores", 1, 0),
    ("x", 1, 0, 3, "R", "E"),
    ("sum", 0, 1, 0, 2, "L", "I"),
    ("x", 1, 0, 2, "R", "I"),
    ("norm_x", 1, 0),
    ("sum", 0, 1, 1, 1, "L", "I"),
    ("qkv", 1, 0, ((1, ("sum", 0, 1, 0, 2, "R", "I"), ("sum_send", 0, 1, 0, 3)), (2, ("kv_start", 1, 0), ("sum", 0, 1, 0, 3, "R", "I"), ("sum", 0, 1, 1, 2, "L", "I")), (3, ("wo_wait", 1, 0), ("sum", 0, 1, 1, 2, "R", "I")),)),
    ("attend", 1, 0),
    ("o_start", 1, 0),
    ("sum", 0, 1, 0, 3, "R", "E"),
    ("sum_send", 0, 1, 1, 3),
    ("sum", 0, 1, 0, 3, "L", "I"),
    ("o", 1, 0, 1, "L", "I"),
    ("sum", 0, 1, 1, 3, "L", "I"),
    ("sum", 0, 1, 1, 3, "R", "E"),
    ("o", 1, 0, 1, "R", "I"),
    ("sum", 0, 1, 1, 3, "R", "I"),
    ("finish", 0, 1),
    ("x_start", 1, 1),
    ("o", 1, 0, 2, "R", "I"),
    ("load_o", 1, 0),
    ("wo", 1, 0, ((2, ("x", 1, 1, 1, "R", "E")), (5, ("x", 1, 1, 2, "R", "E"), ("x", 1, 1, 1, "L", "I"), ("x", 1, 1, 3, "R", "E")), (6, ("x", 1, 1, 1, "R", "I")),)),
    ("x", 1, 1, 2, "R", "I"),
    ("h_start", 1, 0, 0),
    ("norm_x", 1, 1),
    ("h_start", 1, 0, 1),
    ("qkv", 1, 1, ((2, ("kv_start", 1, 1)),)),
    ("h", 1, 0, 0, 1, "R", "I"),
    ("attend", 1, 1),
    ("h", 1, 0, 1, 1, "R", "E"),
    ("h", 1, 0, 0, 1, "R", "E"),
    ("h", 1, 0, 1, 1, "R", "I"),
    ("o_start", 1, 1),
    ("h", 1, 0, 1, 2, "R", "E"),
    ("h", 1, 0, 0, 2, "R", "E"),
    ("norm_h", 1, 0),
    ("gate", 1, 0, ((13, ("sum_drain", 0, 1)), (17, ("o", 1, 1, 1, "R", "I")), (31, ("o", 1, 1, 1, "L", "I")), (35, ("o", 1, 1, 2, "R", "I")),)),
    ("load_o", 1, 1),
    ("wo", 1, 1, ((6, ("h_start", 1, 1, 0)),)),
    ("down", 1, 0, ((4, ("h_start", 1, 1, 1)), (5, ("h", 1, 1, 0, 1, "R", "I"), ("h", 1, 1, 0, 1, "R", "E")), (7, ("sum_send", 1, 0, 0, 1)), (8, ("sum_send", 1, 0, 0, 2)), (9, ("h", 1, 1, 1, 1, "R", "I")), (13, ("h", 1, 1, 1, 1, "R", "E"), ("h", 1, 1, 0, 2, "R", "E")),)),
    ("sum_send", 1, 0, 1, 1),
    ("h", 1, 1, 1, 2, "R", "E"),
    ("norm_h", 1, 1),
    ("sum_send", 1, 0, 1, 2),
    ("sum", 1, 0, 0, 1, "L", "I"),
    ("gate", 1, 1, ((3, ("sum", 1, 0, 1, 1, "L", "I")), (8, ("sum", 1, 0, 0, 2, "R", "I")), (9, ("sum", 1, 0, 1, 2, "R", "I")), (10, ("sum_send", 1, 0, 0, 3)), (11, ("sum", 1, 0, 1, 2, "L", "I")), (15, ("sum", 1, 0, 0, 2, "L", "I")), (25, ("sum", 1, 0, 1, 3, "L", "I")), (27, ("sum", 1, 0, 0, 3, "L", "I")), (30, ("sum_send", 1, 0, 1, 3)), (32, ("sum", 1, 0, 0, 3, "R", "I")), (35, ("sum", 1, 0, 1, 3, "R", "I")),)),
    ("down", 1, 1, ((7, ("sum", 1, 0, 1, 3, "R", "E")), (8, ("sum_send", 1, 1, 0, 1)), (10, ("sum", 1, 1, 0, 1, "L", "I")),)),
    ("sum_send", 1, 1, 1, 1),
    ("sum_send", 1, 1, 0, 2),
    ("sum_send", 1, 1, 1, 2),
    ("sum_send", 1, 1, 0, 3),
    ("sum", 1, 1, 1, 1, "L", "I"),
    ("sum", 1, 1, 0, 2, "L", "I"),
    ("sum", 1, 1, 0, 2, "R", "I"),
    ("sum", 1, 0, 0, 3, "R", "E"),
    ("finish", 1, 0),
    ("put", 1, 0),
    ("sum", 1, 1, 1, 2, "L", "I"),
    ("sum", 1, 1, 1, 2, "R", "I"),
    ("sum", 1, 1, 0, 3, "L", "I"),
    ("sum", 1, 1, 1, 3, "R", "I"),
    ("sum", 1, 1, 0, 3, "R", "I"),
    ("sum", 1, 1, 1, 3, "L", "I"),
    ("sum_send", 1, 1, 1, 3),
    ("sum", 1, 1, 1, 3, "R", "E"),
    ("sum", 1, 1, 0, 3, "R", "E"),
    ("finish", 1, 1),
    ("put", 1, 1),
)


def kernel(n, m, groups, layers, tokens, gain_a, gain_m, cos_ref, sin_ref, w_q, w_k, w_v, w_o, w_gate, w_up, w_down,
           y_out, g_x, g_o, g_h, wo_cols,
           stage, lhs, act, part, sums, scores, ks, vs, kvs, qs, x_cols, pieces, home, wbuf, row_max, row_sum, acc_ref,
           wsem, lsem, gsend, grecv, ksend, krecv, rsend, rrecv, osend, orecv, psend, precv):
    z = lax.axis_index("tp")
    c = lax.axis_index("cp")
    g = lax.axis_index("dp")
    rows = tokens.shape[0] // 2
    d = tokens.shape[1]
    all_rows = n * rows
    heads, hd = w_q.shape[1], w_q.shape[3]
    hc = heads * hd
    width = d // n
    ff = w_gate.shape[2]
    above = jnp.minimum(z + 1, n - 1)
    below = jnp.maximum(z - 1, 0)

    def remote(src, dst, send, recv, **where):
        return pltpu.make_async_remote_copy(src_ref=src, dst_ref=dst, send_sem=send, recv_sem=recv, device_id=where,
                                            device_id_type=MESH)

    def row_block(p):
        return pl.ds(pl.multiple_of(p * rows, 16), rows)

    def col_block(p, w):
        return pl.ds(pl.multiple_of(p * w, 128), w)

    def mirrored(f, side, kind):
        low = 0 if kind == "E" else 1
        for here, way in ((low, UP if side == "L" else DOWN), (n - 1 - low, DOWN if side == "L" else UP)):
            @pl.when(z == here)
            def _(here=here, way=way):
                f(here, way)

    class Gather:
        def __init__(self, i, buf, own):
            self.i, self.buf, self.own = i, buf, own

        def copy(self, way, k, piece):
            src = self.own if k == 0 else self.buf.at[piece]
            return remote(src, self.buf.at[piece], gsend.at[self.i, way, k], grecv.at[self.i, way, k],
                          tp=above if way == UP else below)

        def sends(self, here):
            return ([(UP, k, here - k) for k in range(here + 1) if here < n - 1]
                    + [(DOWN, k, here + k) for k in range(n - here) if here > 0])

        def piece(self, here, k, way):
            return here - k if way == UP else here + k

        def start(self):
            for here in range(n):
                @pl.when(z == here)
                def _(here=here):
                    for way, k, piece in self.sends(here):
                        if k == 0:
                            self.copy(way, k, piece).start()

        def event(self, k, side, kind):
            def arrive(here, way):
                piece = self.piece(here, k, way)
                self.copy(way, k - 1, piece).wait_recv()
                if (way, k, piece) in self.sends(here):
                    self.copy(way, k, piece).start()

            mirrored(arrive, side, kind)

        def drain(self, own):
            for here in range(n):
                @pl.when(z == here)
                def _(here=here):
                    for way, k, piece in self.sends(here):
                        if (k == 0) == own:
                            self.copy(way, k, piece).wait_send()

    class ToInner(Gather):
        def sends(self, here):
            way = UP if here < n // 2 else DOWN
            return [(way, 0, here)] + ([(way, 1, 0 if way == UP else n - 1)] if here in INNER else [])

    class FromInner(Gather):
        def __init__(self, i, buf, own, j):
            super().__init__(i, buf, own)
            self.j = j

        def sends(self, here):
            if here not in INNER:
                return []
            mine, other = 2 * (here - 1) + self.j, 2 * (n - 2 - here) + self.j
            return [(UP, 0, mine), (DOWN, 0, mine), (DOWN if here < n // 2 else UP, 1, other)]

        def piece(self, here, k, way):
            return 2 * ((here - k if way == UP else here + k) - 1) + self.j

    INNER = (1, n - 2)
    inner = both(z >= 1, z <= n - 2)
    wide = 2 * width
    wide_at = jnp.clip(z - 1, 0, 1) * wide

    def own_x(layer, half):
        return tokens.at[pl.ds(half * rows, rows)] if layer == 0 else home.at[half]

    halves = [(l, h) for l in range(layers) for h in (LOW, HIGH)]
    gx = {(l, h): Gather((l * 2 + h) * 4, g_x.at[l, h], own_x(l, h)) for l, h in halves}
    go = {(l, h): ToInner((l * 2 + h) * 4 + 1, g_o.at[l, h], pieces.at[h, :, pl.ds(0, hc)]) for l, h in halves}
    gh = {(l, h): [FromInner((l * 2 + h) * 4 + 2 + j, g_h.at[l, h], pieces.at[h, :, pl.ds(j * width, width)], j) for j in range(2)]
          for l, h in halves}

    def fetch(*pairs):
        copies = [pltpu.make_async_copy(src, dst, lsem.at[i]) for i, (src, dst) in enumerate(pairs)]
        for copy in copies:
            copy.start()
        for copy in copies:
            copy.wait()

    others = [ring(z + k, n) for k in range(1, n)]

    def norm(gain):
        step = 32

        @pl.loop(0, all_rows // step)
        def _(i):
            r = pl.ds(pl.multiple_of(i * step, step), step)
            x = stage[r].astype(F32)
            inv = lax.rsqrt(jnp.mean(x * x, axis=-1, keepdims=True) + 1e-5)
            lhs[r] = (x * inv * gain[...].astype(F32)).astype(BF16)

    def norm_x(layer, half):
        x = gx[layer, half]
        fetch((x.own, stage.at[row_block(z)]), *((x.buf.at[p], stage.at[row_block(p)]) for p in others))
        norm(gain_a.at[pl.ds(layer, 1)])

    def load_o(layer, half):
        @pl.when(inner)
        def _():
            x, o = gx[layer, half], go[layer, half]
            cols = pl.ds(pl.multiple_of(wide_at, 128), wide)
            fetch((o.own, stage.at[:, col_block(z, hc)]), *((o.buf.at[p], stage.at[:, col_block(p, hc)]) for p in others),
                  (x.own.at[:, cols], x_cols.at[row_block(z)]), *((x.buf.at[p, :, cols], x_cols.at[row_block(p)]) for p in others))
            o.drain(True)

    def norm_h(layer, half):
        buf = g_h.at[layer, half]

        @pl.when(inner)
        def _():
            rest = [2 * (n - 2 - z) + j for j in range(2)]
            fetch((pieces.at[half], stage.at[:, pl.ds(pl.multiple_of(wide_at, 128), wide)]),
                  *((buf.at[p], stage.at[:, col_block(p, width)]) for p in rest))

        @pl.when(jnp.logical_not(inner))
        def _():
            fetch(*((buf.at[p], stage.at[:, col_block(p, width)]) for p in range(n)))
            go[layer, half].drain(True)

        norm(gain_m.at[pl.ds(layer, 1)])
        for h in gh[layer, half]:
            h.drain(True)
        if layer > 0:
            gx[layer, half].drain(True)
        home[half] = stage[row_block(z)]

    class Op:
        base = None
        everywhere = True

        def start(self, i, slot):
            for copy in self.copies(i, slot):
                copy.start()

        def fetch(self, unit, pair):
            self.start(2 * unit, 2 * pair)

            @pl.when(2 * unit + 1 < self.tiles)
            def _():
                self.start(2 * unit + 1, 2 * pair + 1)

        def prefetch(self):
            self.fetch(0, self.base % 2)

        def run(self, follow, hooks):
            units = -(-self.tiles // 2)

            def step(unit, count):
                pair, other = lax.rem(self.base + unit, 2), lax.rem(self.base + unit + 1, 2)

                @pl.when(unit + 1 < units)
                def _():
                    self.fetch(unit + 1, other)

                if follow is not None:
                    @pl.when(unit + 1 == units)
                    def _():
                        follow.fetch(0, other)

                for j in range(count):
                    for copy in self.copies(2 * unit + j, 2 * pair + j):
                        copy.wait()
                for j in range(count):
                    self.compute(2 * unit + j, 2 * pair + j)

            @pl.loop(0, self.tiles // 2)
            def _(unit):
                for at, event in hooks:
                    if at < self.tiles // 2:
                        pl.when(unit == at)(event)
                step(unit, 2)

            for at, event in hooks:
                if at >= self.tiles // 2:
                    event()
            if self.tiles % 2:
                step(jnp.int32(units - 1), 1)

        def run_inner(self, follow, hooks, late):
            @pl.when(inner)
            def _():
                if late:
                    self.prefetch()
                self.run(follow, [(at, event) for at, event, kind in hooks if kind != "E"])

            @pl.when(jnp.logical_not(inner))
            def _():
                if not late:
                    for j in range(2):
                        for copy in self.copies(j, 2 * (self.base % 2) + j):
                            copy.wait()
                follow.fetch(0, (self.base + -(-self.tiles // 2)) % 2)
                for _, event, kind in hooks:
                    if kind != "I":
                        event()

    def dot(a, slot, depth):
        return jnp.dot(a, wbuf[slot, :depth], preferred_element_type=F32)

    def tile_start(i, total):
        return pl.multiple_of(jnp.minimum(i * TILE, total - TILE), 128)

    class Qkv(Op):
        def __init__(self, layer, half):
            self.layer, self.half = layer, half
            self.tiles = 1 + -(-hc // TILE)

        def start(self, i, slot):
            def pair(a, b):
                pltpu.make_async_copy(a, wbuf.at[slot, pl.ds(0, d), pl.ds(0, hd)], wsem.at[slot, 0]).start()
                pltpu.make_async_copy(b, wbuf.at[slot, pl.ds(0, d), pl.ds(hd, hd)], wsem.at[slot, 1]).start()

            @pl.when(i == 0)
            def _():
                pair(w_k.at[self.layer], w_v.at[self.layer])

            @pl.when(i > 0)
            def _():
                h = tile_start(i - 1, hc) // hd
                pair(w_q.at[self.layer, h], w_q.at[self.layer, h + 1])

        def copies(self, i, slot):
            return [pltpu.make_async_copy(w_k.at[self.layer], wbuf.at[slot, pl.ds(0, d), pl.ds(j * hd, hd)], wsem.at[slot, j])
                    for j in range(2)]

        def compute(self, i, slot):
            out = dot(lhs[...], slot, d)

            def turned(x):
                return (x * cos_ref[self.half] + pltpu.roll(x, hd // 2, 1) * sin_ref[self.half]).astype(BF16)

            @pl.when(i == 0)
            def _():
                kvs[self.layer, self.half, 0, :, :hd] = turned(out[:, :hd])
                kvs[self.layer, self.half, 0, :, hd:] = out[:, hd:].astype(BF16)

            @pl.when(i > 0)
            def _():
                h = tile_start(i - 1, hc) // hd
                for j in range(2):
                    q = turned(out[:, j * hd : (j + 1) * hd])
                    for p in range(n):
                        qs[p, row_block(h + j)] = q[p * rows : (p + 1) * rows]

    class Wo(Op):
        everywhere = False

        def __init__(self, layer, half):
            self.layer, self.half = layer, half
            self.tiles = wide // TILE

        def copies(self, i, slot):
            at = pl.multiple_of(i * TILE, TILE)
            out = [pltpu.make_async_copy(w_o.at[self.layer, :, pl.ds(pl.multiple_of(wide_at + at, 128), TILE)],
                                         wbuf.at[slot, pl.ds(pl.multiple_of(z * hc, 128), hc)], wsem.at[slot, 0])]
            for k, p in enumerate(others):
                block = pl.ds(pl.multiple_of(p * hc, 128), hc)
                out.append(pltpu.make_async_copy(wo_cols.at[self.layer, block, pl.ds(at, TILE)], wbuf.at[slot, block],
                                                 wsem.at[slot, k + 1]))
            return out

        def compute(self, i, slot):
            cols = pl.ds(pl.multiple_of(i * TILE, TILE), TILE)
            out = dot(stage[...], slot, d) + x_cols[:, cols].astype(F32)
            pieces[self.half, :, cols] = out.astype(BF16)

    class GateUp(Op):
        def __init__(self, layer, half):
            self.layer, self.half = layer, half
            self.tiles = ff // 128

        def copies(self, i, slot):
            cols = pl.ds(pl.multiple_of(i * 128, 128), 128)
            return [pltpu.make_async_copy(w.at[self.layer, :, cols], wbuf.at[slot, pl.ds(0, d), pl.ds(128 * j, 128)], wsem.at[slot, j])
                    for j, w in enumerate((w_gate, w_up))]

        def compute(self, i, slot):
            out = dot(lhs[...], slot, d)
            gate = out[:, :128]
            act[:, pl.ds(pl.multiple_of(i * 128, 128), 128)] = (gate * lax.logistic(gate) * out[:, 128:]).astype(BF16)

    class Down(Op):
        def __init__(self, layer, half):
            self.layer, self.half = layer, half
            self.tiles = d // TILE

        def copies(self, i, slot):
            cols = pl.ds(pl.multiple_of(i * TILE, TILE), TILE)
            return [pltpu.make_async_copy(w_down.at[self.layer, :, cols], wbuf.at[slot, pl.ds(0, ff)], wsem.at[slot, 0])]

        def compute(self, i, slot):
            part[self.half, :, pl.ds(pl.multiple_of(i * TILE, TILE), TILE)] = dot(act[...], slot, ff)

    def kv_copy(layer, half, s):
        return remote(kvs.at[layer, half, 0], kvs.at[layer, half, s], ksend.at[layer, half, s - 1], krecv.at[layer, half, s - 1],
                      cp=ring(c + s, m))

    def kv_start(layer, half):
        for s in range(1, m):
            kv_copy(layer, half, s).start()

    def kv_wait(layer, half):
        for s in range(1, m):
            kv_copy(layer, half, s).wait_recv()

    def attend(layer, half):
        kv_wait(layer, half)
        keys = m * rows
        for s in range(m):
            for g in range(n):
                block = slice(g * rows, (g + 1) * rows)
                ks[half * n + g, s * rows : (s + 1) * rows] = kvs[layer, half, s, block, :hd]
                vs[half * n + g, s * rows : (s + 1) * rows] = kvs[layer, half, s, block, hd:]
        to_log2 = math.log2(math.e) / math.sqrt(hd)
        lanes = range(0, keys, 128)

        @pl.loop(0, n)
        def _(plane):
            count = plane if half == LOW else 2 * n - 1 - plane

            def group(i):
                if half == LOW:
                    return jnp.where(i == 0, plane, i - 1)
                return jnp.where(i == 0, n + plane, jnp.where(i <= n, i - 1, i + plane))

            def score(i):
                return lax.dot_general(qs[plane], ks[group(i)], (((1,), (1,)), ((), ())), preferred_element_type=F32)

            row = lax.broadcasted_iota(jnp.int32, (rows, keys), 0)
            col = lax.broadcasted_iota(jnp.int32, (rows, keys), 1)
            slot = col // rows
            other = lax.rem(c - slot + m, m)
            limit = jnp.where(slot == 0, row, jnp.where((other < c) if half == LOW else (other > c), keys, -1))
            bias = jnp.where(col <= limit, 0.0, -jnp.inf)
            s = (score(0).reshape(heads, rows, keys) + bias[None]).reshape(heads * rows, keys)
            scores[0] = s
            row_max[...] = functools.reduce(jnp.maximum, [s[:, a : a + 128] for a in lanes])

            @pl.loop(1, count + 1)
            def _(i):
                s = score(i)
                scores[i] = s
                row_max[...] = functools.reduce(jnp.maximum, [s[:, a : a + 128] for a in lanes], row_max[...])

            top = jnp.max(row_max[...], axis=-1, keepdims=True) * to_log2
            row_max[...] = jnp.broadcast_to(top, row_max.shape)
            row_sum[...] = jnp.zeros_like(row_sum)
            acc_ref[...] = jnp.zeros_like(acc_ref)

            @pl.loop(0, count + 1)
            def _(i):
                top = row_max[...]
                e = [jnp.exp2(scores[i, :, a : a + 128] * to_log2 - top) for a in lanes]
                row_sum[...] += functools.reduce(jnp.add, e)
                weights = jnp.concatenate([x.astype(BF16) for x in e], axis=-1)
                acc_ref[...] += jnp.dot(weights, vs[group(i)], preferred_element_type=F32)

            out = (acc_ref[...] / jnp.sum(row_sum[...], axis=-1, keepdims=True)).astype(BF16)
            for h in range(heads):
                pieces[half, row_block(plane), h * hd : (h + 1) * hd] = out[h * rows : (h + 1) * rows]

    share = hc // m // groups
    other_chip, other_core = ring(c + 2, m), c + 1 - 2 * lax.rem(c, 2)

    def wo_rows(plane, quarter):
        return pl.ds(pl.multiple_of(plane * hc + quarter * (hc // m), 16), hc // m)

    def wo_share(layer, plane, group):
        return wo_cols.at[layer, pl.ds(pl.multiple_of(plane * hc + c * (hc // m) + group * share, 16), share)]

    def wo_copy(layer, plane, to):
        src = w_o.at[layer, pl.ds(pl.multiple_of(c * (hc // m) + g * share, 16), share), pl.ds((to - 1) * wide, wide)]
        return remote(src, wo_share(layer, plane, g), osend.at[layer, to - 1], orecv.at[layer, plane], tp=to)

    def wo_swap(layer, k):
        here = wo_share(layer, others[k], g)
        return remote(here, here, psend.at[layer, k, 3], precv.at[layer, k, 3], dp=ring(g + 1, groups))

    def wo_pass(layer, k, j):
        here = wo_cols.at[layer, wo_rows(others[k], other_chip if j == 2 else c)]
        return remote(here, here, psend.at[layer, k, j], precv.at[layer, k, j], cp=other_chip if j == 0 else other_core)

    def wo_start(layer, wait=False):
        for here in range(n):
            @pl.when(z == here)
            def _(here=here):
                for to in INNER:
                    if to != here:
                        copy = wo_copy(layer, here, to)
                        copy.wait_send() if wait else copy.start()

    def on_inner(f):
        def run(layer):
            @pl.when(inner)
            def _():
                for k in range(n - 1):
                    f(layer, k)
        return run

    @on_inner
    def wo_groups(layer, k):
        wo_copy(layer, others[k], 1).wait_recv()
        if groups > 1:
            wo_swap(layer, k).start()

    @on_inner
    def wo_chips(layer, k):
        if groups > 1:
            wo_swap(layer, k).wait_recv()
        wo_pass(layer, k, 0).start()
        wo_pass(layer, k, 1).start()

    @on_inner
    def wo_cores(layer, k):
        wo_pass(layer, k, 0).wait_recv()
        wo_pass(layer, k, 2).start()

    @on_inner
    def wo_wait(layer, k):
        wo_pass(layer, k, 1).wait_recv()
        wo_pass(layer, k, 2).wait_recv()

    @on_inner
    def wo_drain(layer, k):
        for j in range(3):
            wo_pass(layer, k, j).wait_send()
        if groups > 1:
            wo_swap(layer, k).wait_send()

    span = d // PARTS

    def sum_slot(way, k):
        return k - 1 if way == UP else (0, 3, 4)[k - 1]

    def sum_copy(layer, half, way, q, k, block):
        cols = pl.ds(q * span, span)
        return remote(part.at[half, row_block(block), cols], sums.at[half, sum_slot(way, k), :, cols],
                      rsend.at[layer, half, way, q, k - 1], rrecv.at[layer, half, way, q, k - 1], tp=above if way == UP else below)

    def sum_send(layer, half, q, k):
        @pl.when(z == 0)
        def _():
            sum_copy(layer, half, UP, q, k, n - k).start()

        @pl.when(z == n - 1)
        def _():
            sum_copy(layer, half, DOWN, q, k, k - 1).start()

    def sum_arrive(layer, half, q, k, here, way):
        block, last = (n - 1 + here - k, n - 1) if way == UP else (here + k - n + 1, 0)
        sum_copy(layer, half, way, q, k, block).wait_recv()
        step = 16

        @pl.loop(0, rows // step)
        def _(i):
            to = pl.ds(pl.multiple_of(block * rows + i * step, step), step)
            frm = pl.ds(pl.multiple_of(i * step, step), step)
            part[half, to, q * span : (q + 1) * span] += sums[half, sum_slot(way, k), frm, q * span : (q + 1) * span]

        if k < n - 1:
            sum_copy(layer, half, way, q, k + 1, block).start()

    def sum_event(layer, half, q, k, side, kind):
        mirrored(lambda here, way: sum_arrive(layer, half, q, k, here, way), side, kind)

    def sum_drain(layer, half):
        for q in range(PARTS):
            for k in range(1, n):
                @pl.when(both(z < n - 1, jnp.logical_or(z == 0, k - 1 >= z)))
                def _(q=q, k=k):
                    sum_copy(layer, half, UP, q, k, 0).wait_send()

                @pl.when(both(z > 0, jnp.logical_or(z == n - 1, k - 1 >= n - 1 - z)))
                def _(q=q, k=k):
                    sum_copy(layer, half, DOWN, q, k, 0).wait_send()

    def finish(half):
        step = 16

        @pl.loop(0, rows // step)
        def _(i):
            r = pl.ds(pl.multiple_of(i * step, step), step)
            mine = part[half, pl.ds(pl.multiple_of(z * rows + i * step, step), step)]
            home[half, r] = (home[half, r].astype(F32) + mine).astype(BF16)

    barrier = pltpu.get_barrier_semaphore()
    partners = [{axis: ring(i + s, size)} for axis, i, size in (("tp", z, n), ("cp", c, m), ("dp", g, groups)) for s in range(1, size)]
    for partner in partners:
        pl.semaphore_signal(barrier, inc=1, device_id=partner, device_id_type=MESH)
    pl.semaphore_wait(barrier, len(partners))

    def put(half):
        copy = pltpu.make_async_copy(home.at[half], y_out.at[pl.ds(half * rows, rows)], lsem.at[0])
        copy.start()
        copy.wait()

    def last_sends():
        for i, half in halves:
            if i == 0:
                gx[i, half].drain(True)
            for gather in (gx[i, half], go[i, half], *gh[i, half]):
                gather.drain(False)
            for s in range(1, m):
                kv_copy(i, half, s).wait_send()
        for i in range(layers):
            wo_start(i, wait=True)
            wo_drain(i)
        for half in (LOW, HIGH):
            sum_drain(layers - 1, half)

    actions = {
        "x_start": lambda l, h: gx[l, h].start(), "x": lambda l, h, *more: gx[l, h].event(*more), "norm_x": norm_x,
        "o_start": lambda l, h: go[l, h].start(), "o": lambda l, h, *more: go[l, h].event(*more), "load_o": load_o,
        "h_start": lambda l, h, j: gh[l, h][j].start(), "h": lambda l, h, j, *more: gh[l, h][j].event(*more), "norm_h": norm_h,
        "kv_start": kv_start, "attend": attend, "finish": lambda l, h: finish(h), "put": lambda l, h: put(h),
        "sum_send": sum_send, "sum": sum_event, "sum_drain": sum_drain,
        "wo_start": lambda l, h: wo_start(l), "wo_groups": lambda l, h: wo_groups(l), "wo_chips": lambda l, h: wo_chips(l),
        "wo_cores": lambda l, h: wo_cores(l), "wo_wait": lambda l, h: wo_wait(l),
    }
    kinds = {"qkv": Qkv, "wo": Wo, "gate": GateUp, "down": Down}
    items = []
    for name, l, h, *more in ORDER:
        if name in kinds:
            o = kinds[name](l, h)
            hooks = [((tile * o.tiles // TILES[name] + 1) // 2, event) for tile, *events in more[0] for event in events]
            items.append((f"{name}_{l}{'AB'[h]}", o, hooks, len(more) > 1))
        else:
            items.append((f"{name}_{l}{'AB'[h]}{''.join(map(str, more))}", functools.partial(actions[name], l, h, *more), None, False))

    ops = [item for item in items if item[2] is not None]
    base = 0
    for _, o, _, _ in ops:
        o.base = base % 2
        base += -(-o.tiles // 2)
    follow = {id(o): None if late else o for _, o, _, late in ops}
    after = {id(a[1]): follow[id(b[1])] for a, b in zip(ops, ops[1:])}
    for name, o, hooks, late in items:
        with jax.named_scope(name):
            if hooks is None:
                o()
                continue
            hooks = [(at, functools.partial(actions[event], *args), "E" if event == "sum_send" else args[-1])
                     for at, (event, *args) in hooks]
            if not o.everywhere:
                o.run_inner(after[id(o)], hooks, late)
                continue
            if late:
                o.prefetch()
            o.run(after.get(id(o)), [(at, event) for at, event, _ in hooks])
    last_sends()


def solution(mesh):
    n = mesh.shape['tp']
    m = mesh.shape['cp']
    groups = mesh.shape['dp']
    row_spec = P(('dp', 'tp', 'cp'), None)
    gain_spec = P(None, None)
    q_spec = P(None, None, 'tp', None)
    col_spec = P(None, None, 'tp')
    o_spec = P(None, 'tp', None, None)
    down_spec = P(None, 'tp', None)

    def body(tokens, norm_attn, norm_mlp, w_q, w_k, w_v, w_o, w_gate, w_up, w_down):
        layers, d, heads, hd = w_q.shape
        rows = tokens.shape[0] // 2
        hc = heads * hd
        width = d // n
        ff = w_gate.shape[2]
        all_rows = n * rows
        c = lax.axis_index('cp')

        inv_freq = 500000.0 ** (-(jnp.arange(hd // 2, dtype=F32) * 2.0 / hd))
        seg = jnp.arange(n) * m + c
        seg = jnp.stack([seg, 2 * n * m - 1 - seg])
        pos = (seg[:, :, None] * rows + jnp.arange(rows)).reshape(2, all_rows)
        angle = pos.astype(F32)[..., None] * inv_freq
        cos, sin = jnp.cos(angle), jnp.sin(angle)
        cos, sin = jnp.concatenate([cos, cos], -1), jnp.concatenate([-sin, sin], -1)

        hbm = pl.BlockSpec(memory_space=pl.ANY)
        vmem = pl.BlockSpec(memory_space=pltpu.VMEM)
        dma = pltpu.SemaphoreType.DMA
        out = pl.pallas_call(
            functools.partial(kernel, n, m, groups, layers),
            out_shape=(
                jax.ShapeDtypeStruct(tokens.shape, BF16),
                jax.ShapeDtypeStruct((layers, 2, n, rows, d), BF16),
                jax.ShapeDtypeStruct((layers, 2, n, all_rows, hc), BF16),
                jax.ShapeDtypeStruct((layers, 2, n, all_rows, width), BF16),
                jax.ShapeDtypeStruct((layers, n * hc, 2 * width), BF16),
            ),
            in_specs=[hbm, vmem, vmem, vmem, vmem] + [hbm] * 7,
            out_specs=(hbm,) * 5,
            scratch_shapes=[
                pltpu.VMEM((all_rows, d), BF16),
                pltpu.VMEM((all_rows, d), BF16),
                pltpu.VMEM((all_rows, ff), BF16),
                pltpu.VMEM((2, all_rows, d), F32),
                pltpu.VMEM((2, 5, rows, d), F32),
                pltpu.VMEM((2 * n, heads * rows, m * rows), F32),
                pltpu.VMEM((2 * n, m * rows, hd), BF16),
                pltpu.VMEM((2 * n, m * rows, hd), BF16),
                pltpu.VMEM((layers, 2, m, all_rows, 2 * hd), BF16),
                pltpu.VMEM((n, heads * rows, hd), BF16),
                pltpu.VMEM((all_rows, 2 * width), BF16),
                pltpu.VMEM((2, all_rows, 2 * width), BF16),
                pltpu.VMEM((2, rows, d), BF16),
                pltpu.VMEM((SLOTS, max(d, ff), TILE), BF16),
                pltpu.VMEM((heads * rows, 128), F32),
                pltpu.VMEM((heads * rows, 128), F32),
                pltpu.VMEM((heads * rows, hd), F32),
                dma((SLOTS, n)),
                dma((2 * n,)),
                dma((layers * 8, 2, n - 1)),
                dma((layers * 8, 2, n - 1)),
                dma((layers, 2, m - 1)),
                dma((layers, 2, m - 1)),
                dma((layers, 2, 2, PARTS, n - 1)),
                dma((layers, 2, 2, PARTS, n - 1)),
                dma((layers, 2)),
                dma((layers, n)),
                dma((layers, n - 1, 4)),
                dma((layers, n - 1, 4)),
            ],
            compiler_params=pltpu.CompilerParams(collective_id=0, has_side_effects=True, vmem_limit_bytes=67043328),
            name="two_layers",
        )(tokens, norm_attn, norm_mlp, cos, sin, jnp.swapaxes(w_q, 1, 2), w_k, w_v, w_o.reshape(layers, hc, d), w_gate, w_up, w_down)
        return out[0]

    return jax.shard_map(
        body,
        mesh=mesh,
        in_specs=(row_spec, gain_spec, gain_spec, q_spec, col_spec, col_spec, o_spec, col_spec, col_spec, down_spec),
        out_specs=row_spec,
        check_vma=False,
    )
```

```python
import functools
import math
import jax
import jax.numpy as jnp
from jax import lax
from jax.experimental import pallas as pl
from jax.experimental.pallas import tpu as pltpu
from jax.sharding import PartitionSpec as P

F32 = jnp.float32
BF16 = jnp.bfloat16
MESH = pl.DeviceIdType.MESH
UP, DOWN = 0, 1
LOW, HIGH = 0, 1
SLOTS = 5
PARTS = 2
TILE = 256


def ring(i, n):
    return lax.rem(i + n, n)


def both(*conditions):
    out = conditions[0]
    for c in conditions[1:]:
        out = jnp.logical_and(out, c)
    return out


TILES = {"qkv": 5, "wo": 7, "gate": 37, "down": 14}
ORDER = (
    ("x_start", 0, 0),
    ("x", 0, 0, 1, "R", "E"),
    ("x", 0, 0, 1, "L", "I"),
    ("x", 0, 0, 1, "R", "I"),
    ("wo_start", 0, 0),
    ("x", 0, 0, 2, "R", "I"),
    ("x_start", 0, 1),
    ("x", 0, 0, 2, "R", "E"),
    ("x", 0, 0, 3, "R", "E"),
    ("norm_x", 0, 0),
    ("qkv", 0, 0, ((2, ("kv_start", 0, 0), ("wo_groups", 0, 0)), (3, ("x", 0, 1, 1, "L", "I")), (4, ("x", 0, 1, 1, "R", "E")),), "late"),
    ("wo_chips", 0, 0),
    ("x", 0, 1, 1, "R", "I"),
    ("attend", 0, 0),
    ("o_start", 0, 0),
    ("x", 0, 1, 2, "R", "I"),
    ("x", 0, 1, 2, "R", "E"),
    ("x", 0, 1, 3, "R", "E"),
    ("norm_x", 0, 1),
    ("o", 0, 0, 1, "L", "I"),
    ("qkv", 0, 1, ((2, ("wo_cores", 0, 0)), (4, ("o", 0, 0, 1, "R", "I")),)),
    ("o", 0, 0, 2, "R", "I"),
    ("load_o", 0, 0),
    ("wo_wait", 0, 0),
    ("wo", 0, 0, ((4, ("h_start", 0, 0, 0)),), "late"),
    ("h", 0, 0, 0, 1, "R", "E"),
    ("h_start", 0, 0, 1),
    ("kv_start", 0, 1),
    ("h", 0, 0, 0, 1, "R", "I"),
    ("attend", 0, 1),
    ("h", 0, 0, 0, 2, "R", "E"),
    ("h", 0, 0, 1, 1, "R", "I"),
    ("h", 0, 0, 1, 1, "R", "E"),
    ("o_start", 0, 1),
    ("h", 0, 0, 1, 2, "R", "E"),
    ("norm_h", 0, 0),
    ("gate", 0, 0, ((5, ("wo_start", 1, 0)), (26, ("o", 0, 1, 1, "R", "I")), (31, ("o", 0, 1, 1, "L", "I")), (35, ("o", 0, 1, 2, "R", "I")),)),
    ("load_o", 0, 1),
    ("wo", 0, 1, ((4, ("wo_groups", 1, 0)), (5, ("h_start", 0, 1, 0)),)),
    ("down", 0, 0, ((7, ("sum_send", 0, 0, 0, 1)), (11, ("h_start", 0, 1, 1), ("sum", 0, 0, 0, 1, "L", "I")), (12, ("h", 0, 1, 0, 1, "R", "E")), (13, ("h", 0, 1, 0, 1, "R", "I"), ("h", 0, 1, 1, 1, "R", "I")),)),
    ("sum_send", 0, 0, 1, 1),
    ("h", 0, 1, 1, 1, "R", "E"),
    ("sum_send", 0, 0, 0, 2),
    ("h", 0, 1, 0, 2, "R", "E"),
    ("sum_send", 0, 0, 1, 2),
    ("h", 0, 1, 1, 2, "R", "E"),
    ("norm_h", 0, 1),
    ("sum_send", 0, 0, 0, 3),
    ("gate", 0, 1, ((3, ("sum_send", 0, 0, 1, 3)), (6, ("sum", 0, 0, 1, 1, "L", "I")), (11, ("sum", 0, 0, 0, 2, "R", "I")), (13, ("wo_chips", 1, 0), ("sum", 0, 0, 0, 3, "R", "E")), (15, ("sum", 0, 0, 0, 2, "L", "I"), ("sum", 0, 0, 1, 2, "R", "I")), (18, ("sum", 0, 0, 1, 2, "L", "I")), (30, ("sum", 0, 0, 0, 3, "R", "I")), (33, ("sum", 0, 0, 0, 3, "L", "I"), ("sum", 0, 0, 1, 3, "R", "I")),)),
    ("sum", 0, 0, 1, 3, "L", "I"),
    ("sum", 0, 0, 1, 3, "R", "E"),
    ("finish", 0, 0),
    ("x_start", 1, 0),
    ("down", 0, 1, ((2, ("x", 1, 0, 1, "L", "I"), ("sum_drain", 0, 0)), (3, ("wo_cores", 1, 0)), (7, ("x", 1, 0, 1, "R", "I"), ("sum_send", 0, 1, 0, 1)), (10, ("sum", 0, 1, 0, 1, "L", "I"), ("x", 1, 0, 1, "R", "E"), ("x", 1, 0, 2, "R", "I")), (13, ("sum", 0, 1, 0, 2, "L", "I"), ("sum_send", 0, 1, 0, 2), ("wo_wait", 1, 0)),)),
    ("x", 1, 0, 2, "R", "E"),
    ("sum_send", 0, 1, 1, 1),
    ("sum_send", 0, 1, 1, 2),
    ("sum_send", 0, 1, 1, 3),
    ("x", 1, 0, 3, "R", "E"),
    ("norm_x", 1, 0),
    ("qkv", 1, 0, ((2, ("sum", 0, 1, 1, 1, "L", "I"), ("sum", 0, 1, 0, 2, "R", "I"), ("sum", 0, 1, 0, 3, "R", "I")), (4, ("kv_start", 1, 0), ("sum", 0, 1, 0, 3, "R", "E"), ("sum_send", 0, 1, 0, 3), ("sum", 0, 1, 1, 2, "L", "I"), ("sum", 0, 1, 1, 2, "R", "I")),)),
    ("attend", 1, 0),
    ("sum", 0, 1, 1, 3, "L", "I"),
    ("o_start", 1, 0),
    ("sum", 0, 1, 1, 3, "R", "E"),
    ("sum", 0, 1, 1, 3, "R", "I"),
    ("sum", 0, 1, 0, 3, "L", "I"),
    ("finish", 0, 1),
    ("x_start", 1, 1),
    ("x", 1, 1, 1, "R", "E"),
    ("o", 1, 0, 1, "L", "I"),
    ("x", 1, 1, 1, "R", "I"),
    ("o", 1, 0, 1, "R", "I"),
    ("o", 1, 0, 2, "R", "I"),
    ("x", 1, 1, 2, "R", "E"),
    ("x", 1, 1, 3, "R", "E"),
    ("load_o", 1, 0),
    ("x", 1, 1, 1, "L", "I"),
    ("wo", 1, 0, ((4, ("h_start", 1, 0, 0)), (5, ("x", 1, 1, 2, "R", "I")),)),
    ("norm_x", 1, 1),
    ("qkv", 1, 1, ((1, ("h", 1, 0, 0, 1, "R", "I")), (2, ("kv_start", 1, 1)), (3, ("h_start", 1, 0, 1)),)),
    ("attend", 1, 1),
    ("h", 1, 0, 1, 1, "R", "I"),
    ("o_start", 1, 1),
    ("h", 1, 0, 0, 1, "R", "E"),
    ("h", 1, 0, 0, 2, "R", "E"),
    ("h", 1, 0, 1, 1, "R", "E"),
    ("h", 1, 0, 1, 2, "R", "E"),
    ("norm_h", 1, 0),
    ("gate", 1, 0, ((18, ("o", 1, 1, 1, "R", "I")), (24, ("o", 1, 1, 1, "L", "I")),)),
    ("o", 1, 1, 2, "R", "I"),
    ("load_o", 1, 1),
    ("wo", 1, 1, ((4, ("h_start", 1, 1, 0)),)),
    ("down", 1, 0, ((2, ("h_start", 1, 1, 1)), (6, ("h", 1, 1, 0, 1, "R", "I")), (7, ("sum_send", 1, 0, 0, 1), ("sum_drain", 0, 1)), (10, ("h", 1, 1, 1, 1, "R", "I")), (11, ("sum_send", 1, 0, 0, 2), ("h", 1, 1, 1, 1, "R", "E")),)),
    ("sum_send", 1, 0, 1, 1),
    ("h", 1, 1, 0, 1, "R", "E"),
    ("h", 1, 1, 0, 2, "R", "E"),
    ("sum_send", 1, 0, 1, 2),
    ("sum", 1, 0, 1, 1, "L", "I"),
    ("h", 1, 1, 1, 2, "R", "E"),
    ("norm_h", 1, 1),
    ("gate", 1, 1, ((10, ("sum_send", 1, 0, 1, 3)), (12, ("sum", 1, 0, 1, 2, "L", "I")), (16, ("sum", 1, 0, 0, 1, "L", "I")), (19, ("sum", 1, 0, 1, 2, "R", "I")), (28, ("sum_send", 1, 0, 0, 3)),)),
    ("down", 1, 1, ((1, ("sum", 1, 0, 0, 2, "L", "I")), (7, ("sum", 1, 0, 0, 2, "R", "I"), ("sum_send", 1, 1, 0, 1), ("sum_send", 1, 1, 0, 2)), (8, ("sum", 1, 1, 0, 1, "L", "I"), ("sum", 1, 0, 1, 3, "L", "I")), (9, ("sum", 1, 0, 0, 3, "R", "E")), (10, ("sum", 1, 1, 0, 2, "L", "I"), ("sum", 1, 0, 0, 3, "R", "I")), (12, ("sum", 1, 1, 0, 2, "R", "I"), ("sum", 1, 1, 0, 3, "R", "I")), (13, ("sum", 1, 0, 1, 3, "R", "I")),)),
    ("sum_send", 1, 1, 1, 1),
    ("sum_send", 1, 1, 1, 2),
    ("sum", 1, 1, 0, 3, "R", "E"),
    ("sum", 1, 1, 1, 1, "L", "I"),
    ("sum", 1, 1, 1, 2, "L", "I"),
    ("sum", 1, 0, 0, 3, "L", "I"),
    ("sum", 1, 1, 1, 2, "R", "I"),
    ("sum", 1, 0, 1, 3, "R", "E"),
    ("sum_send", 1, 1, 0, 3),
    ("sum", 1, 1, 0, 3, "L", "I"),
    ("sum_send", 1, 1, 1, 3),
    ("sum", 1, 1, 1, 3, "R", "E"),
    ("finish", 1, 0),
    ("put", 1, 0),
    ("sum", 1, 1, 1, 3, "R", "I"),
    ("sum", 1, 1, 1, 3, "L", "I"),
    ("finish", 1, 1),
    ("put", 1, 1),
)


def kernel(n, m, groups, layers, tokens, gain_a, gain_m, cos_ref, sin_ref, w_q, w_k, w_v, w_o, w_gate, w_up, w_down,
           y_out, g_x, g_o, g_h, wo_cols,
           stage, x_cols, act, part, sums, scores, ks, vs, kvs, qs, pieces, home, wbuf, row_max, row_sum, acc_ref,
           wsem, lsem, gsend, grecv, ksend, krecv, rsend, rrecv, osend, orecv, psend, precv):
    z = lax.axis_index("tp")
    c = lax.axis_index("cp")
    g = lax.axis_index("dp")
    rows = tokens.shape[0] // 2
    d = tokens.shape[1]
    all_rows = n * rows
    heads, hd = w_q.shape[1], w_q.shape[3]
    hc = heads * hd
    width = d // n
    ff = w_gate.shape[2]
    above = jnp.minimum(z + 1, n - 1)
    below = jnp.maximum(z - 1, 0)

    def remote(src, dst, send, recv, **where):
        return pltpu.make_async_remote_copy(src_ref=src, dst_ref=dst, send_sem=send, recv_sem=recv, device_id=where,
                                            device_id_type=MESH)

    def row_block(p):
        return pl.ds(pl.multiple_of(p * rows, 16), rows)

    def col_block(p, w):
        return pl.ds(pl.multiple_of(p * w, 128), w)

    def mirrored(f, side, kind):
        low = 0 if kind == "E" else 1
        for here, way in ((low, UP if side == "L" else DOWN), (n - 1 - low, DOWN if side == "L" else UP)):
            @pl.when(z == here)
            def _(here=here, way=way):
                f(here, way)

    class Gather:
        def __init__(self, i, buf, own):
            self.i, self.buf, self.own = i, buf, own

        def copy(self, way, k, piece):
            src = self.own if k == 0 else self.buf.at[piece]
            return remote(src, self.buf.at[piece], gsend.at[self.i, way, k], grecv.at[self.i, way, k],
                          tp=above if way == UP else below)

        def sends(self, here):
            return ([(UP, k, here - k) for k in range(here + 1) if here < n - 1]
                    + [(DOWN, k, here + k) for k in range(n - here) if here > 0])

        def piece(self, here, k, way):
            return here - k if way == UP else here + k

        def start(self):
            for here in range(n):
                @pl.when(z == here)
                def _(here=here):
                    for way, k, piece in self.sends(here):
                        if k == 0:
                            self.copy(way, k, piece).start()

        def event(self, k, side, kind):
            def arrive(here, way):
                piece = self.piece(here, k, way)
                self.copy(way, k - 1, piece).wait_recv()
                if (way, k, piece) in self.sends(here):
                    self.copy(way, k, piece).start()

            mirrored(arrive, side, kind)

        def drain(self, own):
            for here in range(n):
                @pl.when(z == here)
                def _(here=here):
                    for way, k, piece in self.sends(here):
                        if (k == 0) == own:
                            self.copy(way, k, piece).wait_send()

    class ToInner(Gather):
        def sends(self, here):
            way = UP if here < n // 2 else DOWN
            return [(way, 0, here)] + ([(way, 1, 0 if way == UP else n - 1)] if here in INNER else [])

    class FromInner(Gather):
        def __init__(self, i, buf, own, j):
            super().__init__(i, buf, own)
            self.j = j

        def sends(self, here):
            if here not in INNER:
                return []
            mine, other = 2 * (here - 1) + self.j, 2 * (n - 2 - here) + self.j
            return [(UP, 0, mine), (DOWN, 0, mine), (DOWN if here < n // 2 else UP, 1, other)]

        def piece(self, here, k, way):
            return 2 * ((here - k if way == UP else here + k) - 1) + self.j

    INNER = (1, n - 2)
    inner = both(z >= 1, z <= n - 2)
    wide = 2 * width
    wide_at = jnp.clip(z - 1, 0, 1) * wide

    def own_x(layer, half):
        return tokens.at[pl.ds(half * rows, rows)] if layer == 0 else home.at[half]

    halves = [(l, h) for l in range(layers) for h in (LOW, HIGH)]
    gx = {(l, h): Gather((l * 2 + h) * 4, g_x.at[l, h], own_x(l, h)) for l, h in halves}
    go = {(l, h): ToInner((l * 2 + h) * 4 + 1, g_o.at[l, h], pieces.at[h, :, pl.ds(0, hc)]) for l, h in halves}
    gh = {(l, h): [FromInner((l * 2 + h) * 4 + 2 + j, g_h.at[l, h], pieces.at[h, :, pl.ds(j * width, width)], j) for j in range(2)]
          for l, h in halves}

    def fetch(*pairs):
        copies = [pltpu.make_async_copy(src, dst, lsem.at[i]) for i, (src, dst) in enumerate(pairs)]
        for copy in copies:
            copy.start()
        for copy in copies:
            copy.wait()

    others = [ring(z + k, n) for k in range(1, n)]

    def norm(gain):
        step = 32

        @pl.loop(0, all_rows // step)
        def _(i):
            r = pl.ds(pl.multiple_of(i * step, step), step)
            x = stage[r].astype(F32)
            inv = lax.rsqrt(jnp.mean(x * x, axis=-1, keepdims=True) + 1e-5)
            stage[r] = (x * inv * gain[...].astype(F32)).astype(BF16)

    def norm_x(layer, half):
        x = gx[layer, half]
        fetch((x.own, stage.at[row_block(z)]), *((x.buf.at[p], stage.at[row_block(p)]) for p in others))
        norm(gain_a.at[pl.ds(layer, 1)])

    def load_o(layer, half):
        @pl.when(inner)
        def _():
            x, o = gx[layer, half], go[layer, half]
            cols = pl.ds(pl.multiple_of(wide_at, 128), wide)
            fetch((o.own, stage.at[:, col_block(z, hc)]), *((o.buf.at[p], stage.at[:, col_block(p, hc)]) for p in others),
                  (x.own.at[:, cols], x_cols.at[row_block(z)]), *((x.buf.at[p, :, cols], x_cols.at[row_block(p)]) for p in others))
            o.drain(True)

    def norm_h(layer, half):
        buf = g_h.at[layer, half]

        @pl.when(inner)
        def _():
            rest = [2 * (n - 2 - z) + j for j in range(2)]
            fetch((pieces.at[half], stage.at[:, pl.ds(pl.multiple_of(wide_at, 128), wide)]),
                  *((buf.at[p], stage.at[:, col_block(p, width)]) for p in rest))

        @pl.when(jnp.logical_not(inner))
        def _():
            fetch(*((buf.at[p], stage.at[:, col_block(p, width)]) for p in range(n)))
            go[layer, half].drain(True)

        for h in gh[layer, half]:
            h.drain(True)
        if layer > 0:
            gx[layer, half].drain(True)
        home[half] = stage[row_block(z)]
        norm(gain_m.at[pl.ds(layer, 1)])

    class Op:
        base = None
        everywhere = True

        def start(self, i, slot):
            for copy in self.copies(i, slot):
                copy.start()

        def fetch(self, i):
            slot = lax.rem(self.base + i, SLOTS)

            @pl.when(i < self.tiles)
            def _():
                self.start(i, slot)

            if self.follow is not None:
                @pl.when(i >= self.tiles)
                def _():
                    self.follow.start(i - self.tiles, slot)

        def prefetch(self):
            for i in range(AHEAD):
                self.start(i, (self.base + i) % SLOTS)

        def run(self, hooks):
            @pl.loop(0, self.tiles)
            def _(i):
                for at, event in hooks:
                    pl.when(i == at)(event)
                self.fetch(i + AHEAD)
                slot = lax.rem(self.base + i, SLOTS)
                for copy in self.copies(i, slot):
                    copy.wait()
                self.compute(i, slot)

        def run_inner(self, hooks, late):
            @pl.when(inner)
            def _():
                if late:
                    self.prefetch()
                self.run([(at, event) for at, event, kind in hooks if kind != "E"])

            @pl.when(jnp.logical_not(inner))
            def _():
                if not late:
                    for i in range(AHEAD):
                        for copy in self.copies(i, (self.base + i) % SLOTS):
                            copy.wait()
                for i in range(AHEAD):
                    self.follow.start(i, (self.base + self.tiles + i) % SLOTS)
                for _, event, kind in hooks:
                    if kind != "I":
                        event()

    def dot(a, slot, depth):
        return jnp.dot(a, wbuf[slot, :depth], preferred_element_type=F32)

    def tile_start(i, total):
        return pl.multiple_of(jnp.minimum(i * TILE, total - TILE), 128)

    class Qkv(Op):
        def __init__(self, layer, half):
            self.layer, self.half = layer, half
            self.tiles = 1 + -(-hc // TILE)

        def start(self, i, slot):
            def pair(a, b):
                pltpu.make_async_copy(a, wbuf.at[slot, pl.ds(0, d), pl.ds(0, hd)], wsem.at[slot, 0]).start()
                pltpu.make_async_copy(b, wbuf.at[slot, pl.ds(0, d), pl.ds(hd, hd)], wsem.at[slot, 1]).start()

            @pl.when(i == 0)
            def _():
                pair(w_k.at[self.layer], w_v.at[self.layer])

            @pl.when(i > 0)
            def _():
                h = tile_start(i - 1, hc) // hd
                pair(w_q.at[self.layer, h], w_q.at[self.layer, h + 1])

        def copies(self, i, slot):
            return [pltpu.make_async_copy(w_k.at[self.layer], wbuf.at[slot, pl.ds(0, d), pl.ds(j * hd, hd)], wsem.at[slot, j])
                    for j in range(2)]

        def compute(self, i, slot):
            out = dot(stage[...], slot, d)

            def turned(x):
                return (x * cos_ref[self.half] + pltpu.roll(x, hd // 2, 1) * sin_ref[self.half]).astype(BF16)

            @pl.when(i == 0)
            def _():
                kvs[self.layer, self.half, 0, :, :hd] = turned(out[:, :hd])
                kvs[self.layer, self.half, 0, :, hd:] = out[:, hd:].astype(BF16)

            @pl.when(i > 0)
            def _():
                h = tile_start(i - 1, hc) // hd
                for j in range(2):
                    q = turned(out[:, j * hd : (j + 1) * hd])
                    for p in range(n):
                        qs[p, row_block(h + j)] = q[p * rows : (p + 1) * rows]

    class Wo(Op):
        everywhere = False

        def __init__(self, layer, half):
            self.layer, self.half = layer, half
            self.tiles = wide // TILE

        def copies(self, i, slot):
            at = pl.multiple_of(i * TILE, TILE)
            out = [pltpu.make_async_copy(w_o.at[self.layer, :, pl.ds(pl.multiple_of(wide_at + at, 128), TILE)],
                                         wbuf.at[slot, pl.ds(pl.multiple_of(z * hc, 128), hc)], wsem.at[slot, 0])]
            for k, p in enumerate(others):
                block = pl.ds(pl.multiple_of(p * hc, 128), hc)
                out.append(pltpu.make_async_copy(wo_cols.at[self.layer, block, pl.ds(at, TILE)], wbuf.at[slot, block],
                                                 wsem.at[slot, k + 1]))
            return out

        def compute(self, i, slot):
            cols = pl.ds(pl.multiple_of(i * TILE, TILE), TILE)
            out = dot(stage[...], slot, d) + x_cols[:, cols].astype(F32)
            pieces[self.half, :, cols] = out.astype(BF16)

    class GateUp(Op):
        def __init__(self, layer, half):
            self.layer, self.half = layer, half
            self.tiles = ff // 128

        def copies(self, i, slot):
            cols = pl.ds(pl.multiple_of(i * 128, 128), 128)
            return [pltpu.make_async_copy(w.at[self.layer, :, cols], wbuf.at[slot, pl.ds(0, d), pl.ds(128 * j, 128)], wsem.at[slot, j])
                    for j, w in enumerate((w_gate, w_up))]

        def compute(self, i, slot):
            out = dot(stage[...], slot, d)
            gate = out[:, :128]
            act[:, pl.ds(pl.multiple_of(i * 128, 128), 128)] = (gate * lax.logistic(gate) * out[:, 128:]).astype(BF16)

    class Down(Op):
        def __init__(self, layer, half):
            self.layer, self.half = layer, half
            self.tiles = d // TILE

        def copies(self, i, slot):
            cols = pl.ds(pl.multiple_of(i * TILE, TILE), TILE)
            return [pltpu.make_async_copy(w_down.at[self.layer, :, cols], wbuf.at[slot, pl.ds(0, ff)], wsem.at[slot, 0])]

        def compute(self, i, slot):
            part[self.half, :, pl.ds(pl.multiple_of(i * TILE, TILE), TILE)] = dot(act[...], slot, ff)

    def kv_copy(layer, half, s):
        return remote(kvs.at[layer, half, 0], kvs.at[layer, half, s], ksend.at[layer, half, s - 1], krecv.at[layer, half, s - 1],
                      cp=ring(c + s, m))

    def kv_start(layer, half):
        for s in range(1, m):
            kv_copy(layer, half, s).start()

    def kv_wait(layer, half):
        for s in range(1, m):
            kv_copy(layer, half, s).wait_recv()

    def attend(layer, half):
        kv_wait(layer, half)
        keys = m * rows
        for s in range(m):
            for g in range(n):
                block = slice(g * rows, (g + 1) * rows)
                ks[half * n + g, s * rows : (s + 1) * rows] = kvs[layer, half, s, block, :hd]
                vs[half * n + g, s * rows : (s + 1) * rows] = kvs[layer, half, s, block, hd:]
        to_log2 = math.log2(math.e) / math.sqrt(hd)
        lanes = range(0, keys, 128)

        @pl.loop(0, n)
        def _(plane):
            count = plane if half == LOW else 2 * n - 1 - plane

            def group(i):
                if half == LOW:
                    return jnp.where(i == 0, plane, i - 1)
                return jnp.where(i == 0, n + plane, jnp.where(i <= n, i - 1, i + plane))

            def score(i):
                return lax.dot_general(qs[plane], ks[group(i)], (((1,), (1,)), ((), ())), preferred_element_type=F32)

            row = lax.broadcasted_iota(jnp.int32, (rows, keys), 0)
            col = lax.broadcasted_iota(jnp.int32, (rows, keys), 1)
            slot = col // rows
            other = lax.rem(c - slot + m, m)
            limit = jnp.where(slot == 0, row, jnp.where((other < c) if half == LOW else (other > c), keys, -1))
            bias = jnp.where(col <= limit, 0.0, -jnp.inf)
            s = (score(0).reshape(heads, rows, keys) + bias[None]).reshape(heads * rows, keys)
            scores[0] = s
            row_max[...] = functools.reduce(jnp.maximum, [s[:, a : a + 128] for a in lanes])

            @pl.loop(1, count + 1)
            def _(i):
                s = score(i)
                scores[i] = s
                row_max[...] = functools.reduce(jnp.maximum, [s[:, a : a + 128] for a in lanes], row_max[...])

            top = jnp.max(row_max[...], axis=-1, keepdims=True) * to_log2
            row_max[...] = jnp.broadcast_to(top, row_max.shape)
            row_sum[...] = jnp.zeros_like(row_sum)
            acc_ref[...] = jnp.zeros_like(acc_ref)

            @pl.loop(0, count + 1)
            def _(i):
                top = row_max[...]
                e = [jnp.exp2(scores[i, :, a : a + 128] * to_log2 - top) for a in lanes]
                row_sum[...] += functools.reduce(jnp.add, e)
                weights = jnp.concatenate([x.astype(BF16) for x in e], axis=-1)
                acc_ref[...] += jnp.dot(weights, vs[group(i)], preferred_element_type=F32)

            out = (acc_ref[...] / jnp.sum(row_sum[...], axis=-1, keepdims=True)).astype(BF16)
            for h in range(heads):
                pieces[half, row_block(plane), h * hd : (h + 1) * hd] = out[h * rows : (h + 1) * rows]

    share = hc // m // groups
    other_chip, other_core = ring(c + 2, m), c + 1 - 2 * lax.rem(c, 2)

    def wo_rows(plane, quarter):
        return pl.ds(pl.multiple_of(plane * hc + quarter * (hc // m), 16), hc // m)

    def wo_share(layer, plane, group):
        return wo_cols.at[layer, pl.ds(pl.multiple_of(plane * hc + c * (hc // m) + group * share, 16), share)]

    def wo_copy(layer, plane, to):
        src = w_o.at[layer, pl.ds(pl.multiple_of(c * (hc // m) + g * share, 16), share), pl.ds((to - 1) * wide, wide)]
        return remote(src, wo_share(layer, plane, g), osend.at[layer, to - 1], orecv.at[layer, plane], tp=to)

    def wo_swap(layer, k):
        here = wo_share(layer, others[k], g)
        return remote(here, here, psend.at[layer, k, 3], precv.at[layer, k, 3], dp=ring(g + 1, groups))

    def wo_pass(layer, k, j):
        here = wo_cols.at[layer, wo_rows(others[k], other_chip if j == 2 else c)]
        return remote(here, here, psend.at[layer, k, j], precv.at[layer, k, j], cp=other_chip if j == 0 else other_core)

    def wo_start(layer, wait=False):
        for here in range(n):
            @pl.when(z == here)
            def _(here=here):
                for to in INNER:
                    if to != here:
                        copy = wo_copy(layer, here, to)
                        copy.wait_send() if wait else copy.start()

    def on_inner(f):
        def run(layer):
            @pl.when(inner)
            def _():
                for k in range(n - 1):
                    f(layer, k)
        return run

    @on_inner
    def wo_groups(layer, k):
        wo_copy(layer, others[k], 1).wait_recv()
        if groups > 1:
            wo_swap(layer, k).start()

    @on_inner
    def wo_chips(layer, k):
        if groups > 1:
            wo_swap(layer, k).wait_recv()
        wo_pass(layer, k, 0).start()
        wo_pass(layer, k, 1).start()

    @on_inner
    def wo_cores(layer, k):
        wo_pass(layer, k, 0).wait_recv()
        wo_pass(layer, k, 2).start()

    @on_inner
    def wo_wait(layer, k):
        wo_pass(layer, k, 1).wait_recv()
        wo_pass(layer, k, 2).wait_recv()

    @on_inner
    def wo_drain(layer, k):
        for j in range(3):
            wo_pass(layer, k, j).wait_send()
        if groups > 1:
            wo_swap(layer, k).wait_send()

    span = d // PARTS

    def sum_slot(way, k):
        return k - 1 if way == UP else (0, 3, 4)[k - 1]

    def sum_copy(layer, half, way, q, k, block):
        cols = pl.ds(q * span, span)
        return remote(part.at[half, row_block(block), cols], sums.at[half, sum_slot(way, k), :, cols],
                      rsend.at[layer, half, way, q, k - 1], rrecv.at[layer, half, way, q, k - 1], tp=above if way == UP else below)

    def sum_send(layer, half, q, k):
        @pl.when(z == 0)
        def _():
            sum_copy(layer, half, UP, q, k, n - k).start()

        @pl.when(z == n - 1)
        def _():
            sum_copy(layer, half, DOWN, q, k, k - 1).start()

    def sum_arrive(layer, half, q, k, here, way):
        block, last = (n - 1 + here - k, n - 1) if way == UP else (here + k - n + 1, 0)
        sum_copy(layer, half, way, q, k, block).wait_recv()
        step = 16

        @pl.loop(0, rows // step)
        def _(i):
            to = pl.ds(pl.multiple_of(block * rows + i * step, step), step)
            frm = pl.ds(pl.multiple_of(i * step, step), step)
            part[half, to, q * span : (q + 1) * span] += sums[half, sum_slot(way, k), frm, q * span : (q + 1) * span]

        if k < n - 1:
            sum_copy(layer, half, way, q, k + 1, block).start()

    def sum_event(layer, half, q, k, side, kind):
        mirrored(lambda here, way: sum_arrive(layer, half, q, k, here, way), side, kind)

    def sum_drain(layer, half):
        for q in range(PARTS):
            for k in range(1, n):
                @pl.when(both(z < n - 1, jnp.logical_or(z == 0, k - 1 >= z)))
                def _(q=q, k=k):
                    sum_copy(layer, half, UP, q, k, 0).wait_send()

                @pl.when(both(z > 0, jnp.logical_or(z == n - 1, k - 1 >= n - 1 - z)))
                def _(q=q, k=k):
                    sum_copy(layer, half, DOWN, q, k, 0).wait_send()

    def finish(half):
        step = 16

        @pl.loop(0, rows // step)
        def _(i):
            r = pl.ds(pl.multiple_of(i * step, step), step)
            mine = part[half, pl.ds(pl.multiple_of(z * rows + i * step, step), step)]
            home[half, r] = (home[half, r].astype(F32) + mine).astype(BF16)

    barrier = pltpu.get_barrier_semaphore()
    partners = [{axis: ring(i + s, size)} for axis, i, size in (("tp", z, n), ("cp", c, m), ("dp", g, groups)) for s in range(1, size)]
    for partner in partners:
        pl.semaphore_signal(barrier, inc=1, device_id=partner, device_id_type=MESH)
    pl.semaphore_wait(barrier, len(partners))

    def put(half):
        copy = pltpu.make_async_copy(home.at[half], y_out.at[pl.ds(half * rows, rows)], lsem.at[0])
        copy.start()
        copy.wait()

    def last_sends():
        for i, half in halves:
            if i == 0:
                gx[i, half].drain(True)
            for gather in (gx[i, half], go[i, half], *gh[i, half]):
                gather.drain(False)
            for s in range(1, m):
                kv_copy(i, half, s).wait_send()
        for i in range(layers):
            wo_start(i, wait=True)
            wo_drain(i)
        for half in (LOW, HIGH):
            sum_drain(layers - 1, half)

    actions = {
        "x_start": lambda l, h: gx[l, h].start(), "x": lambda l, h, *more: gx[l, h].event(*more), "norm_x": norm_x,
        "o_start": lambda l, h: go[l, h].start(), "o": lambda l, h, *more: go[l, h].event(*more), "load_o": load_o,
        "h_start": lambda l, h, j: gh[l, h][j].start(), "h": lambda l, h, j, *more: gh[l, h][j].event(*more), "norm_h": norm_h,
        "kv_start": kv_start, "attend": attend, "finish": lambda l, h: finish(h), "put": lambda l, h: put(h),
        "sum_send": sum_send, "sum": sum_event, "sum_drain": sum_drain,
        "wo_start": lambda l, h: wo_start(l), "wo_groups": lambda l, h: wo_groups(l), "wo_chips": lambda l, h: wo_chips(l),
        "wo_cores": lambda l, h: wo_cores(l), "wo_wait": lambda l, h: wo_wait(l),
    }
    kinds = {"qkv": Qkv, "wo": Wo, "gate": GateUp, "down": Down}
    items = []
    for name, l, h, *more in ORDER:
        if name in kinds:
            o = kinds[name](l, h)
            hooks = [(tile * o.tiles // TILES[name], event) for tile, *events in more[0] for event in events]
            items.append((f"{name}_{l}{'AB'[h]}", o, hooks, len(more) > 1))
        else:
            items.append((f"{name}_{l}{'AB'[h]}{''.join(map(str, more))}", functools.partial(actions[name], l, h, *more), None, False))

    ops = [item for item in items if item[2] is not None]
    base = 0
    for (_, o, _, _), (_, follow, _, late) in zip(ops, ops[1:] + [(None, None, None, True)]):
        o.base, o.follow = base % SLOTS, None if late else follow
        base += o.tiles
    AHEAD = min(SLOTS - 1, *(o.tiles for _, o, _, _ in ops))
    for name, o, hooks, late in items:
        with jax.named_scope(name):
            if hooks is None:
                o()
                continue
            hooks = [(at, functools.partial(actions[event], *args), "E" if event == "sum_send" else args[-1])
                     for at, (event, *args) in hooks]
            if not o.everywhere:
                o.run_inner(hooks, late)
                continue
            if late:
                o.prefetch()
            o.run([(at, event) for at, event, _ in hooks])
    last_sends()


def solution(mesh):
    n = mesh.shape['tp']
    m = mesh.shape['cp']
    groups = mesh.shape['dp']
    row_spec = P(('dp', 'tp', 'cp'), None)
    gain_spec = P(None, None)
    q_spec = P(None, None, 'tp', None)
    col_spec = P(None, None, 'tp')
    o_spec = P(None, 'tp', None, None)
    down_spec = P(None, 'tp', None)

    def body(tokens, norm_attn, norm_mlp, w_q, w_k, w_v, w_o, w_gate, w_up, w_down):
        layers, d, heads, hd = w_q.shape
        rows = tokens.shape[0] // 2
        hc = heads * hd
        width = d // n
        ff = w_gate.shape[2]
        all_rows = n * rows
        c = lax.axis_index('cp')

        inv_freq = 500000.0 ** (-(jnp.arange(hd // 2, dtype=F32) * 2.0 / hd))
        seg = jnp.arange(n) * m + c
        seg = jnp.stack([seg, 2 * n * m - 1 - seg])
        pos = (seg[:, :, None] * rows + jnp.arange(rows)).reshape(2, all_rows)
        angle = pos.astype(F32)[..., None] * inv_freq
        cos, sin = jnp.cos(angle), jnp.sin(angle)
        cos, sin = jnp.concatenate([cos, cos], -1), jnp.concatenate([-sin, sin], -1)

        hbm = pl.BlockSpec(memory_space=pl.ANY)
        vmem = pl.BlockSpec(memory_space=pltpu.VMEM)
        dma = pltpu.SemaphoreType.DMA
        out = pl.pallas_call(
            functools.partial(kernel, n, m, groups, layers),
            out_shape=(
                jax.ShapeDtypeStruct(tokens.shape, BF16),
                jax.ShapeDtypeStruct((layers, 2, n, rows, d), BF16),
                jax.ShapeDtypeStruct((layers, 2, n, all_rows, hc), BF16),
                jax.ShapeDtypeStruct((layers, 2, n, all_rows, width), BF16),
                jax.ShapeDtypeStruct((layers, n * hc, 2 * width), BF16),
            ),
            in_specs=[hbm, vmem, vmem, vmem, vmem] + [hbm] * 7,
            out_specs=(hbm,) * 5,
            scratch_shapes=[
                pltpu.VMEM((all_rows, d), BF16),
                pltpu.VMEM((all_rows, 2 * width), BF16),
                pltpu.VMEM((all_rows, ff), BF16),
                pltpu.VMEM((2, all_rows, d), F32),
                pltpu.VMEM((2, 5, rows, d), F32),
                pltpu.VMEM((2 * n, heads * rows, m * rows), F32),
                pltpu.VMEM((2 * n, m * rows, hd), BF16),
                pltpu.VMEM((2 * n, m * rows, hd), BF16),
                pltpu.VMEM((layers, 2, m, all_rows, 2 * hd), BF16),
                pltpu.VMEM((n, heads * rows, hd), BF16),
                pltpu.VMEM((2, all_rows, 2 * width), BF16),
                pltpu.VMEM((2, rows, d), BF16),
                pltpu.VMEM((SLOTS, max(d, ff), TILE), BF16),
                pltpu.VMEM((heads * rows, 128), F32),
                pltpu.VMEM((heads * rows, 128), F32),
                pltpu.VMEM((heads * rows, hd), F32),
                dma((SLOTS, n)),
                dma((2 * n,)),
                dma((layers * 8, 2, n - 1)),
                dma((layers * 8, 2, n - 1)),
                dma((layers, 2, m - 1)),
                dma((layers, 2, m - 1)),
                dma((layers, 2, 2, PARTS, n - 1)),
                dma((layers, 2, 2, PARTS, n - 1)),
                dma((layers, 2)),
                dma((layers, n)),
                dma((layers, n - 1, 4)),
                dma((layers, n - 1, 4)),
            ],
            compiler_params=pltpu.CompilerParams(collective_id=0, has_side_effects=True, vmem_limit_bytes=67043328),
            name="two_layers",
        )(tokens, norm_attn, norm_mlp, cos, sin, jnp.swapaxes(w_q, 1, 2), w_k, w_v, w_o.reshape(layers, hc, d), w_gate, w_up, w_down)
        return out[0]

    return jax.shard_map(
        body,
        mesh=mesh,
        in_specs=(row_spec, gain_spec, gain_spec, q_spec, col_spec, col_spec, o_spec, col_spec, col_spec, down_spec),
        out_specs=row_spec,
        check_vma=False,
    )
```

```python
import functools
import math
import jax
import jax.numpy as jnp
from jax import lax
from jax.experimental import pallas as pl
from jax.experimental.pallas import tpu as pltpu
from jax.sharding import PartitionSpec as P

F32 = jnp.float32
BF16 = jnp.bfloat16
MESH = pl.DeviceIdType.MESH
UP, DOWN = 0, 1
LOW, HIGH = 0, 1
SLOTS = 3
TILE = 512
HALF = 256


def ring(i, n):
    return lax.rem(i + n, n)


def both(*conditions):
    out = conditions[0]
    for c in conditions[1:]:
        out = jnp.logical_and(out, c)
    return out


TILES = {"qkv": 5, "wo": 7, "gate": 37, "down": 14}
ORDER = (
    ("x_start", 0, 0),
    ("x", 0, 0, 1, "L", "I"),
    ("x", 0, 0, 1, "R", "I"),
    ("x", 0, 0, 2, "R", "I"),
    ("x", 0, 0, 1, "R", "E"),
    ("wo_start", 0, 0),
    ("x_start", 0, 1),
    ("x", 0, 0, 2, "R", "E"),
    ("x", 0, 0, 3, "R", "E"),
    ("norm_x", 0, 0),
    ("qkv", (0, 0), ((2, ("kv_start", 0, 0), ("wo_groups", 0, 0)), (3, ("x", 0, 1, 1, "L", "I")),), "late"),
    ("wo_chips", 0, 0),
    ("attend", 0, 0),
    ("x", 0, 1, 1, "R", "E"),
    ("x", 0, 1, 1, "R", "I"),
    ("x", 0, 1, 2, "R", "I"),
    ("o_start", 0, 0),
    ("x", 0, 1, 2, "R", "E"),
    ("x", 0, 1, 3, "R", "E"),
    ("norm_x", 0, 1),
    ("o", 0, 0, 1, "L", "I"),
    ("qkv", (0, 1), ((3, ("wo_cores", 0, 0), ("wo_start", 1, 0), ("o", 0, 0, 1, "R", "I")), (4, ("kv_start", 0, 1), ("o", 0, 0, 2, "R", "I")),)),
    ("load_o", 0, 0, 0),
    ("wo_wait", 0, 0),
    ("wo", (0, 0, 0), (), "late"),
    ("h_start", 0, 0, 0),
    ("attend", 0, 1),
    ("h", 0, 0, 0, 1, "R", "I"),
    ("load_o", 0, 0, 1),
    ("wo", (0, 0, 1), ((2, ("h", 0, 0, 0, 1, "R", "E"), ("h", 0, 0, 0, 2, "R", "E")), (3, ("o_start", 0, 1)),)),
    ("norm_h", 0, 0, 0),
    ("gate", (0, 0, 0), ((2, ("h_start", 0, 0, 1)), (5, ("o", 0, 1, 1, "R", "I")), (16, ("o", 0, 1, 1, "L", "I")), (20, ("h", 0, 0, 1, 1, "R", "I")),)),
    ("o", 0, 1, 2, "R", "I"),
    ("load_o", 0, 1, 0),
    ("wo", (0, 1, 0), ()),
    ("down", (0, 0, 0), ((1, ("h_start", 0, 1, 0)), (4, ("h", 0, 0, 1, 1, "R", "E")),)),
    ("load_o", 0, 1, 1),
    ("sum_send", 0, 0, 0, 1),
    ("wo", (0, 1, 1), ((2, ("h", 0, 0, 1, 2, "R", "E")), (5, ("sum", 0, 0, 0, 1, "L", "I"), ("wo_groups", 1, 0)),)),
    ("h", 0, 1, 0, 1, "R", "I"),
    ("norm_h", 0, 0, 1),
    ("gate", (0, 0, 1), ((3, ("sum_send", 0, 0, 0, 2)), (15, ("h_start", 0, 1, 1)), (20, ("sum_send", 0, 0, 0, 3)), (21, ("sum", 0, 0, 0, 2, "L", "I")), (35, ("wo_chips", 1, 0)),)),
    ("down", (0, 0, 1), ((2, ("h", 0, 1, 1, 1, "R", "I"), ("sum", 0, 0, 0, 2, "R", "I")), (4, ("h", 0, 1, 0, 1, "R", "E")), (9, ("h", 0, 1, 0, 2, "R", "E")),)),
    ("sum_send", 0, 0, 1, 1),
    ("sum", 0, 0, 1, 1, "L", "I"),
    ("norm_h", 0, 1, 0),
    ("gate", (0, 1, 0), ((7, ("sum_send", 0, 0, 1, 2)), (20, ("h", 0, 1, 1, 1, "R", "E")), (21, ("sum_send", 0, 0, 1, 3), ("sum", 0, 0, 1, 2, "L", "I")), (27, ("sum", 0, 0, 1, 2, "R", "I")),)),
    ("down", (0, 1, 0), ((4, ("sum", 0, 0, 0, 3, "L", "I")),)),
    ("sum_send", 0, 1, 0, 1),
    ("sum", 0, 0, 0, 3, "R", "E"),
    ("sum", 0, 0, 0, 3, "R", "I"),
    ("h", 0, 1, 1, 2, "R", "E"),
    ("finish", 0, 0, 0),
    ("sum", 0, 0, 1, 3, "R", "I"),
    ("norm_h", 0, 1, 1),
    ("sum", 0, 0, 1, 3, "L", "I"),
    ("sum", 0, 0, 1, 3, "R", "E"),
    ("finish", 0, 0, 1),
    ("x_start", 1, 0),
    ("x", 1, 0, 1, "L", "I"),
    ("sum_send", 0, 1, 0, 2),
    ("sum", 0, 1, 0, 1, "L", "I"),
    ("gate", (0, 1, 1), ((8, ("x", 1, 0, 1, "R", "I")), (24, ("sum", 0, 1, 0, 2, "L", "I")), (30, ("wo_cores", 1, 0)), (33, ("x", 1, 0, 2, "R", "I")), (36, ("sum_send", 0, 1, 0, 3)),)),
    ("down", (0, 1, 1), ((10, ("x", 1, 0, 1, "R", "E")), (12, ("sum", 0, 1, 0, 3, "L", "I"), ("sum", 0, 1, 0, 2, "R", "I")),)),
    ("sum_send", 0, 1, 1, 1),
    ("wo_wait", 1, 0),
    ("sum", 0, 1, 1, 1, "L", "I"),
    ("sum_send", 0, 1, 1, 2),
    ("x", 1, 0, 2, "R", "E"),
    ("x", 1, 0, 3, "R", "E"),
    ("norm_x", 1, 0),
    ("qkv", (1, 0), ((3, ("kv_start", 1, 0), ("sum", 0, 1, 1, 2, "L", "I"), ("sum", 0, 1, 0, 3, "R", "I"), ("sum_send", 0, 1, 1, 3)),)),
    ("attend", 1, 0),
    ("o_start", 1, 0),
    ("sum", 0, 1, 1, 3, "R", "E"),
    ("sum", 0, 1, 0, 3, "R", "E"),
    ("sum", 0, 1, 1, 3, "L", "I"),
    ("sum", 0, 1, 1, 2, "R", "I"),
    ("sum", 0, 1, 1, 3, "R", "I"),
    ("o", 1, 0, 1, "L", "I"),
    ("finish", 0, 1, 0),
    ("sum_drain", 0, 0, 1),
    ("finish", 0, 1, 1),
    ("o", 1, 0, 1, "R", "I"),
    ("x_start", 1, 1),
    ("o", 1, 0, 2, "R", "I"),
    ("x", 1, 1, 1, "R", "E"),
    ("load_o", 1, 0, 0),
    ("x", 1, 1, 1, "L", "I"),
    ("wo", (1, 0, 0), ((6, ("x", 1, 1, 2, "R", "E"), ("x", 1, 1, 3, "R", "E")),)),
    ("x", 1, 1, 1, "R", "I"),
    ("x", 1, 1, 2, "R", "I"),
    ("norm_x", 1, 1),
    ("qkv", (1, 1), ((2, ("kv_start", 1, 1)),)),
    ("load_o", 1, 0, 1),
    ("wo", (1, 0, 1), ((3, ("h_start", 1, 0, 0)), (6, ("h", 1, 0, 0, 1, "R", "E")),)),
    ("attend", 1, 1),
    ("o_start", 1, 1),
    ("h", 1, 0, 0, 2, "R", "E"),
    ("h", 1, 0, 0, 1, "R", "I"),
    ("norm_h", 1, 0, 0),
    ("gate", (1, 0, 0), ((3, ("sum_drain", 0, 0, 0)), (4, ("sum_drain", 0, 1, 1)), (13, ("h_start", 1, 0, 1)), (14, ("o", 1, 1, 1, "R", "I")), (33, ("h", 1, 0, 1, 1, "R", "E")), (35, ("o", 1, 1, 1, "L", "I")),)),
    ("down", (1, 0, 0), ((4, ("h", 1, 0, 1, 1, "R", "I")),)),
    ("sum_send", 1, 0, 0, 1),
    ("o", 1, 1, 2, "R", "I"),
    ("load_o", 1, 1, 0),
    ("wo", (1, 1, 0), ()),
    ("h_start", 1, 1, 0),
    ("h", 1, 0, 1, 2, "R", "E"),
    ("norm_h", 1, 0, 1),
    ("gate", (1, 0, 1), ((9, ("sum_send", 1, 0, 0, 2)), (25, ("h", 1, 1, 0, 1, "R", "E"), ("h", 1, 1, 0, 1, "R", "I")),)),
    ("load_o", 1, 1, 1),
    ("sum_send", 1, 0, 0, 3),
    ("wo", (1, 1, 1), ()),
    ("down", (1, 0, 1), ((1, ("h_start", 1, 1, 1)), (2, ("sum", 1, 0, 0, 1, "L", "I")), (13, ("h", 1, 1, 0, 2, "R", "E")),)),
    ("norm_h", 1, 1, 0),
    ("gate", (1, 1, 0), ((1, ("sum_send", 1, 0, 1, 1)), (3, ("h", 1, 1, 1, 1, "R", "I")), (15, ("sum", 1, 0, 0, 2, "L", "I")), (17, ("sum_send", 1, 0, 1, 2)), (22, ("sum_drain", 0, 1, 0)), (25, ("h", 1, 1, 1, 1, "R", "E"), ("sum", 1, 0, 1, 1, "L", "I")), (32, ("sum_send", 1, 0, 1, 3), ("sum", 1, 0, 0, 2, "R", "I")),)),
    ("sum", 1, 0, 1, 2, "L", "I"),
    ("down", (1, 1, 0), ((3, ("h", 1, 1, 1, 2, "R", "E")), (9, ("sum", 1, 0, 1, 2, "R", "I")),)),
    ("norm_h", 1, 1, 1),
    ("gate", (1, 1, 1), ((2, ("sum_send", 1, 1, 0, 1), ("sum_send", 1, 1, 0, 2)), (3, ("sum", 1, 0, 0, 3, "R", "I")), (12, ("sum", 1, 1, 0, 1, "L", "I")), (23, ("sum", 1, 0, 0, 3, "L", "I")), (29, ("sum", 1, 1, 0, 2, "L", "I")), (32, ("sum", 1, 0, 1, 3, "R", "I")),)),
    ("down", (1, 1, 1), ((6, ("sum", 1, 0, 0, 3, "R", "E")), (13, ("sum", 1, 0, 1, 3, "L", "I")),)),
    ("sum_send", 1, 1, 1, 1),
    ("sum_send", 1, 1, 1, 2),
    ("finish", 1, 0, 0),
    ("sum", 1, 1, 1, 1, "L", "I"),
    ("sum", 1, 0, 1, 3, "R", "E"),
    ("sum", 1, 1, 0, 2, "R", "I"),
    ("finish", 1, 0, 1),
    ("put", 1, 0),
    ("sum", 1, 1, 0, 3, "R", "I"),
    ("sum", 1, 1, 1, 2, "R", "I"),
    ("sum", 1, 1, 1, 2, "L", "I"),
    ("sum", 1, 1, 0, 3, "L", "I"),
    ("sum_send", 1, 1, 0, 3),
    ("sum_send", 1, 1, 1, 3),
    ("sum", 1, 1, 1, 3, "R", "I"),
    ("sum", 1, 1, 0, 3, "R", "E"),
    ("finish", 1, 1, 0),
    ("sum", 1, 1, 1, 3, "L", "I"),
    ("sum", 1, 1, 1, 3, "R", "E"),
    ("finish", 1, 1, 1),
    ("put", 1, 1),
)


def kernel(n, m, groups, layers, tokens, gain_a, gain_m, turns, w_q, w_k, w_v, w_o, w_gate, w_up, w_down,
           y_out, g_x, g_o, g_h, wo_cols,
           stage, act, part, sums, scores, ks, vs, kvs, qs, pieces, home, wbuf, row_max, row_sum, acc_ref,
           wsem, lsem, xsend, xrecv, gsend, grecv, ksend, krecv, rsend, rrecv, osend, orecv, psend, precv):
    z = lax.axis_index("tp")
    c = lax.axis_index("cp")
    g = lax.axis_index("dp")
    rows = tokens.shape[0] // 2
    sub = rows // 2
    d = tokens.shape[1]
    all_rows, sub_rows = n * rows, n * sub
    heads, hd = w_q.shape[1], w_q.shape[3]
    hc = heads * hd
    width = d // n
    ff = w_gate.shape[2]
    above = jnp.minimum(z + 1, n - 1)
    below = jnp.maximum(z - 1, 0)

    def remote(src, dst, send, recv, **where):
        return pltpu.make_async_remote_copy(src_ref=src, dst_ref=dst, send_sem=send, recv_sem=recv, device_id=where,
                                            device_id_type=MESH)

    def row_block(p):
        return pl.ds(pl.multiple_of(p * rows, 16), rows)

    def sub_block(p):
        return pl.ds(pl.multiple_of(p * sub, 16), sub)

    def col_block(p, w):
        return pl.ds(pl.multiple_of(p * w, 128), w)

    def mirrored(f, side, kind):
        low = 0 if kind == "E" else 1
        for here, way in ((low, UP if side == "L" else DOWN), (n - 1 - low, DOWN if side == "L" else UP)):
            @pl.when(z == here)
            def _(here=here, way=way):
                f(here, way)

    class Gather:
        sems = None

        def __init__(self, i, buf, own):
            self.i, self.buf, self.own = i, buf, own

        def copy(self, way, k, piece):
            src = self.own if k == 0 else self.buf.at[piece]
            return remote(src, self.buf.at[piece], self.sems[0].at[self.i, way, k], self.sems[1].at[self.i, way, k],
                          tp=above if way == UP else below)

        def sends(self, here):
            return ([(UP, k, here - k) for k in range(here + 1) if here < n - 1]
                    + [(DOWN, k, here + k) for k in range(n - here) if here > 0])

        def piece(self, here, k, way):
            return here - k if way == UP else here + k

        def start(self):
            for here in range(n):
                @pl.when(z == here)
                def _(here=here):
                    for way, k, piece in self.sends(here):
                        if k == 0:
                            self.copy(way, k, piece).start()

        def event(self, k, side, kind):
            def arrive(here, way):
                piece = self.piece(here, k, way)
                self.copy(way, k - 1, piece).wait_recv()
                if (way, k, piece) in self.sends(here):
                    self.copy(way, k, piece).start()

            mirrored(arrive, side, kind)

        def drain(self, own):
            for here in range(n):
                @pl.when(z == here)
                def _(here=here):
                    for way, k, piece in self.sends(here):
                        if (k == 0) == own:
                            self.copy(way, k, piece).wait_send()

    class ToInner(Gather):
        def sends(self, here):
            way = UP if here < n // 2 else DOWN
            return [(way, 0, here)] + ([(way, 1, 0 if way == UP else n - 1)] if here in INNER else [])

    class FromInner(Gather):
        def sends(self, here):
            if here not in INNER:
                return []
            mine, other = here - 1, n - 2 - here
            return [(UP, 0, mine), (DOWN, 0, mine), (DOWN if here < n // 2 else UP, 1, other)]

        def piece(self, here, k, way):
            return (here - k if way == UP else here + k) - 1

    INNER = (1, n - 2)
    inner = both(z >= 1, z <= n - 2)
    wide = 2 * width
    wide_at = jnp.clip(z - 1, 0, 1) * wide

    def own_x(layer, half):
        return tokens.at[pl.ds(half * rows, rows)] if layer == 0 else home.at[half]

    halves = [(l, h) for l in range(layers) for h in (LOW, HIGH)]
    quarters = [(l, h, s) for l, h in halves for s in range(2)]
    Gather.sems = xsend, xrecv
    ToInner.sems = FromInner.sems = gsend, grecv
    gx = {(l, h): Gather(2 * l + h, g_x.at[l, h], own_x(l, h)) for l, h in halves}
    go = {(l, h): ToInner(6 * l + 3 * h, g_o.at[l, h], pieces.at[h, :, :, pl.ds(0, hc)]) for l, h in halves}
    gh = {(l, h, s): FromInner(6 * l + 3 * h + s + 1, g_h.at[l, h, s], pieces.at[h, s]) for l, h, s in quarters}

    def fetch(*pairs):
        copies = [pltpu.make_async_copy(src, dst, lsem.at[i]) for i, (src, dst) in enumerate(pairs)]
        for copy in copies:
            copy.start()
        for copy in copies:
            copy.wait()

    others = [ring(z + k, n) for k in range(1, n)]

    def norm(gain, count):
        step = 32

        @pl.loop(0, count // step)
        def _(i):
            r = pl.ds(pl.multiple_of(i * step, step), step)
            x = stage[r].astype(F32)
            inv = lax.rsqrt(jnp.mean(x * x, axis=-1, keepdims=True) + 1e-5)
            stage[r] = (x * inv * gain[...].astype(F32)).astype(BF16)

    def norm_x(layer, half):
        x = gx[layer, half]
        fetch((x.own, stage.at[row_block(z)]), *((x.buf.at[p], stage.at[row_block(p)]) for p in others))
        norm(gain_a.at[pl.ds(layer, 1)], all_rows)

    few = pl.ds(0, sub_rows)

    def below_o(p):
        return stage.at[pl.ds(pl.multiple_of(sub_rows + p * sub, 16), sub), pl.ds(0, wide)]

    def load_o(layer, half, s):
        @pl.when(inner)
        def _():
            x, o = gx[layer, half], go[layer, half]
            cols = pl.ds(pl.multiple_of(wide_at, 128), wide)
            mine = pl.ds(s * sub, sub)
            fetch((pieces.at[half, s, :, pl.ds(0, hc)], stage.at[few, col_block(z, hc)]),
                  *((o.buf.at[p, s], stage.at[few, col_block(p, hc)]) for p in others),
                  (x.own.at[mine, cols], below_o(z)), *((x.buf.at[p, mine, cols], below_o(p)) for p in others))
            if s == 0:
                o.drain(True)

    def norm_h(layer, half, s):
        h = gh[layer, half, s]

        def to(piece):
            return stage.at[few, pl.ds(pl.multiple_of(piece * wide, 128), wide)]

        @pl.when(inner)
        def _():
            fetch((h.own, to(z - 1)), (h.buf.at[n - 2 - z], to(n - 2 - z)))

        @pl.when(jnp.logical_not(inner))
        def _():
            fetch((h.buf.at[0], to(0)), (h.buf.at[1], to(1)))
            if s == 0:
                go[layer, half].drain(True)

        h.drain(True)
        if layer > 0 and s == 0:
            gx[layer, half].drain(True)
        home[half, pl.ds(s * sub, sub)] = stage[sub_block(z)]
        norm(gain_m.at[pl.ds(layer, 1)], sub_rows)

    class Op:
        base = None
        everywhere = True

        def start(self, i, slot):
            for copy in self.copies(i, slot):
                copy.start()

        def fetch(self, i):
            slot = lax.rem(self.base + i, SLOTS)

            @pl.when(i < self.tiles)
            def _():
                self.start(i, slot)

            if self.follow is not None:
                @pl.when(i >= self.tiles)
                def _():
                    self.follow.start(i - self.tiles, slot)

        def prefetch(self):
            for i in range(AHEAD):
                self.start(i, (self.base + i) % SLOTS)

        def run(self, hooks):
            @pl.loop(0, self.tiles)
            def _(i):
                for at in sorted({at for at, _ in hooks if at < self.tiles}):
                    @pl.when(i == at)
                    def _(at=at):
                        for where, event in hooks:
                            if where == at:
                                event()
                self.fetch(i + AHEAD)
                slot = lax.rem(self.base + i, SLOTS)
                for copy in self.copies(i, slot):
                    copy.wait()
                self.compute(i, slot)

            for at, event in hooks:
                if at >= self.tiles:
                    event()

        def run_inner(self, hooks, late):
            @pl.when(inner)
            def _():
                if late:
                    self.prefetch()
                self.run([(at, event) for at, event, kind in hooks if kind != "E"])

            @pl.when(jnp.logical_not(inner))
            def _():
                if not late:
                    for i in range(AHEAD):
                        for copy in self.copies(i, (self.base + i) % SLOTS):
                            copy.wait()
                for i in range(AHEAD):
                    self.follow.start(i, (self.base + self.tiles + i) % SLOTS)
                for _, event, kind in hooks:
                    if kind != "I":
                        event()

    def dot(a, slot, depth, at):
        return jnp.dot(a, wbuf[slot, :depth, pl.ds(at, HALF)], preferred_element_type=F32)

    def tile_start(i, width, total):
        return pl.multiple_of(jnp.minimum(i * width, total - width), 128)

    class Qkv(Op):
        def __init__(self, layer, half):
            self.layer, self.half = layer, half
            self.tiles = 1 + -(-(heads - 2) // 4)

        def first(self, i):
            return jnp.minimum(4 * i - 2, heads - 4)

        def copy(self, src, slot, j):
            return pltpu.make_async_copy(src, wbuf.at[slot, pl.ds(0, d), pl.ds(j * hd, hd)], wsem.at[slot, j])

        def start(self, i, slot):
            @pl.when(i == 0)
            def _():
                for j, src in enumerate((w_k.at[self.layer], w_v.at[self.layer], w_q.at[self.layer, 0], w_q.at[self.layer, 1])):
                    self.copy(src, slot, j).start()

            @pl.when(i > 0)
            def _():
                for j in range(4):
                    self.copy(w_q.at[self.layer, self.first(i) + j], slot, j).start()

        def copies(self, i, slot):
            return [self.copy(w_k.at[self.layer], slot, j) for j in range(4)]

        def compute(self, i, slot):
            cos_sin = turns[self.half]
            sin_cos = pltpu.roll(cos_sin, hd // 2, 1)
            first = lax.broadcasted_iota(jnp.int32, cos_sin.shape, 1) < hd // 2
            cos, sin = jnp.where(first, cos_sin, sin_cos), jnp.where(first, sin_cos * -1.0, cos_sin)

            def turned(x):
                return (x * cos + pltpu.roll(x, hd // 2, 1) * sin).astype(BF16)

            @pl.loop(0, 2)
            def _(j):
                out = dot(stage[...], slot, d, pl.multiple_of(j * HALF, HALF))
                head = jnp.where(i == 0, 2 * j - 2, self.first(i) + 2 * j)

                @pl.when(head < 0)
                def _():
                    kvs[self.layer, self.half, 0, :, :hd] = turned(out[:, :hd])
                    kvs[self.layer, self.half, 0, :, hd:] = out[:, hd:].astype(BF16)

                @pl.when(head >= 0)
                def _():
                    for t in range(2):
                        q = turned(out[:, t * hd : (t + 1) * hd])
                        for p in range(n):
                            qs[p, row_block(jnp.maximum(head, 0) + t)] = q[p * rows : (p + 1) * rows]

    class Wo(Op):
        everywhere = False

        def __init__(self, layer, half, s):
            self.layer, self.half, self.s = layer, half, s
            self.tiles = -(-wide // TILE)

        def copies(self, i, slot):
            cols = pl.ds(tile_start(i, TILE, wide), TILE)
            return [pltpu.make_async_copy(wo_cols.at[self.layer, :, cols], wbuf.at[slot, pl.ds(0, d)], wsem.at[slot, 0])]

        def compute(self, i, slot):
            @pl.loop(0, 2)
            def _(j):
                cols = pl.ds(pl.multiple_of(tile_start(i, TILE, wide) + j * HALF, 128), HALF)
                out = dot(stage[few], slot, d, pl.multiple_of(j * HALF, HALF)) + stage[pl.ds(sub_rows, sub_rows), cols].astype(F32)
                pieces[self.half, self.s, :, cols] = out.astype(BF16)

    class GateUp(Op):
        def __init__(self, layer, half, s):
            self.layer, self.half, self.s = layer, half, s
            self.tiles = -(-ff // HALF)

        def copies(self, i, slot):
            cols = pl.ds(tile_start(i, HALF, ff), HALF)
            return [pltpu.make_async_copy(w.at[self.layer, :, cols], wbuf.at[slot, pl.ds(0, d), pl.ds(HALF * j, HALF)], wsem.at[slot, j])
                    for j, w in enumerate((w_gate, w_up))]

        def compute(self, i, slot):
            out = jnp.dot(stage[few], wbuf[slot, :d], preferred_element_type=F32)
            gate = out[:, :HALF]
            act[:, pl.ds(tile_start(i, HALF, ff), HALF)] = (gate * lax.logistic(gate) * out[:, HALF:]).astype(BF16)

    class Down(Op):
        def __init__(self, layer, half, s):
            self.layer, self.half, self.s = layer, half, s
            self.tiles = d // TILE

        def copies(self, i, slot):
            cols = pl.ds(pl.multiple_of(i * TILE, TILE), TILE)
            return [pltpu.make_async_copy(w_down.at[self.layer, :, cols], wbuf.at[slot, pl.ds(0, ff)], wsem.at[slot, 0])]

        def compute(self, i, slot):
            part[self.half, self.s, :, pl.ds(pl.multiple_of(i * TILE, TILE), TILE)] = jnp.dot(
                act[...], wbuf[slot, :ff], preferred_element_type=F32)

    def kv_copy(layer, half, s):
        return remote(kvs.at[layer, half, 0], kvs.at[layer, half, s], ksend.at[layer, half, s - 1], krecv.at[layer, half, s - 1],
                      cp=ring(c + s, m))

    def kv_start(layer, half):
        for s in range(1, m):
            kv_copy(layer, half, s).start()

    def kv_wait(layer, half):
        for s in range(1, m):
            kv_copy(layer, half, s).wait_recv()

    def attend(layer, half):
        kv_wait(layer, half)
        keys = m * rows
        mine = slice(half * n, (half + 1) * n)
        for s in range(m):
            kv = kvs[layer, half, s].reshape(n, rows, 2 * hd)
            ks[mine, s * rows : (s + 1) * rows] = kv[..., :hd]
            vs[mine, s * rows : (s + 1) * rows] = kv[..., hd:]
        to_log2 = math.log2(math.e) / math.sqrt(hd)
        lanes = range(0, keys, 128)

        @pl.loop(0, n)
        def _(plane):
            count = plane if half == LOW else 2 * n - 1 - plane

            def group(i):
                if half == LOW:
                    return jnp.where(i == 0, plane, i - 1)
                return jnp.where(i == 0, n + plane, jnp.where(i <= n, i - 1, i + plane))

            def score(i):
                return lax.dot_general(qs[plane], ks[group(i)], (((1,), (1,)), ((), ())), preferred_element_type=F32)

            row = lax.broadcasted_iota(jnp.int32, (rows, keys), 0)
            col = lax.broadcasted_iota(jnp.int32, (rows, keys), 1)
            slot = col // rows
            other = lax.rem(c - slot + m, m)
            limit = jnp.where(slot == 0, row, jnp.where((other < c) if half == LOW else (other > c), keys, -1))
            bias = jnp.where(col <= limit, 0.0, -jnp.inf)
            s = (score(0).reshape(heads, rows, keys) + bias[None]).reshape(heads * rows, keys)
            scores[0] = s
            row_max[...] = functools.reduce(jnp.maximum, [s[:, a : a + 128] for a in lanes])

            @pl.loop(1, count + 1)
            def _(i):
                s = score(i)
                scores[i] = s
                row_max[...] = functools.reduce(jnp.maximum, [s[:, a : a + 128] for a in lanes], row_max[...])

            top = jnp.max(row_max[...], axis=-1, keepdims=True) * to_log2
            row_max[...] = jnp.broadcast_to(top, row_max.shape)
            row_sum[...] = jnp.zeros_like(row_sum)
            acc_ref[...] = jnp.zeros_like(acc_ref)

            @pl.loop(0, count + 1)
            def _(i):
                top = row_max[...]
                s = scores[i]
                e = [jnp.exp2(s[:, a : a + 128] * to_log2 - top) for a in lanes]
                row_sum[...] += functools.reduce(jnp.add, e)
                weights = jnp.concatenate([x.astype(BF16) for x in e], axis=-1)
                acc_ref[...] += jnp.dot(weights, vs[group(i)], preferred_element_type=F32)

            out = (acc_ref[...] / jnp.sum(row_sum[...], axis=-1, keepdims=True)).astype(BF16)
            for h in range(heads):
                for s in range(2):
                    pieces[half, s, sub_block(plane), h * hd : (h + 1) * hd] = out[h * rows + s * sub : h * rows + (s + 1) * sub]

    share = hc // m // groups
    other_chip, other_core = ring(c + 2, m), c + 1 - 2 * lax.rem(c, 2)

    def wo_rows(plane, quarter):
        return pl.ds(pl.multiple_of(plane * hc + quarter * (hc // m), 16), hc // m)

    def wo_share(layer, plane, group):
        return wo_cols.at[layer, pl.ds(pl.multiple_of(plane * hc + c * (hc // m) + group * share, 16), share)]

    def wo_copy(layer, plane, to):
        src = w_o.at[layer, pl.ds(pl.multiple_of(c * (hc // m) + g * share, 16), share), pl.ds((to - 1) * wide, wide)]
        return remote(src, wo_share(layer, plane, g), osend.at[layer, to - 1], orecv.at[layer, plane], tp=to)

    def wo_swap(layer, k):
        here = wo_share(layer, others[k], g)
        return remote(here, here, psend.at[layer, k, 3], precv.at[layer, k, 3], dp=ring(g + 1, groups))

    def wo_pass(layer, k, j):
        here = wo_cols.at[layer, wo_rows(others[k], other_chip if j == 2 else c)]
        return remote(here, here, psend.at[layer, k, j], precv.at[layer, k, j], cp=other_chip if j == 0 else other_core)

    def wo_mine(layer):
        return pltpu.make_async_copy(w_o.at[layer, :, pl.ds(pl.multiple_of(wide_at, 128), wide)],
                                     wo_cols.at[layer, pl.ds(pl.multiple_of(z * hc, 128), hc)], lsem.at[2 * n + layer])

    def wo_start(layer, wait=False):
        if not wait:
            @pl.when(inner)
            def _():
                wo_mine(layer).start()

        for here in range(n):
            @pl.when(z == here)
            def _(here=here):
                for to in INNER:
                    if to != here:
                        copy = wo_copy(layer, here, to)
                        copy.wait_send() if wait else copy.start()

    def on_inner(f):
        def run(layer):
            @pl.when(inner)
            def _():
                for k in range(n - 1):
                    f(layer, k)
        return run

    @on_inner
    def wo_groups(layer, k):
        wo_copy(layer, others[k], 1).wait_recv()
        if groups > 1:
            wo_swap(layer, k).start()

    @on_inner
    def wo_chips(layer, k):
        if groups > 1:
            wo_swap(layer, k).wait_recv()
        wo_pass(layer, k, 0).start()
        wo_pass(layer, k, 1).start()

    @on_inner
    def wo_cores(layer, k):
        wo_pass(layer, k, 0).wait_recv()
        wo_pass(layer, k, 2).start()

    @on_inner
    def wo_wait(layer, k):
        if k == 0:
            wo_mine(layer).wait()
        wo_pass(layer, k, 1).wait_recv()
        wo_pass(layer, k, 2).wait_recv()

    @on_inner
    def wo_drain(layer, k):
        for j in range(3):
            wo_pass(layer, k, j).wait_send()
        if groups > 1:
            wo_swap(layer, k).wait_send()

    def sum_slot(way, k):
        return k - 1 if way == UP else (0, 3, 4)[k - 1]

    def sum_copy(layer, half, s, way, k, block):
        return remote(part.at[half, s, sub_block(block)], sums.at[half, s, sum_slot(way, k)],
                      rsend.at[half, s, way, k - 1], rrecv.at[half, s, way, k - 1], tp=above if way == UP else below)

    def sum_send(layer, half, s, k):
        @pl.when(z == 0)
        def _():
            sum_copy(layer, half, s, UP, k, n - k).start()

        @pl.when(z == n - 1)
        def _():
            sum_copy(layer, half, s, DOWN, k, k - 1).start()

    def sum_arrive(layer, half, s, k, here, way):
        block, last = (n - 1 + here - k, n - 1) if way == UP else (here + k - n + 1, 0)
        sum_copy(layer, half, s, way, k, block).wait_recv()
        step = sub // 2

        @pl.loop(0, sub // step)
        def _(i):
            to = pl.ds(pl.multiple_of(block * sub + i * step, 8), step)
            part[half, s, to] += sums[half, s, sum_slot(way, k), pl.ds(pl.multiple_of(i * step, 8), step)]

        if k < n - 1:
            sum_copy(layer, half, s, way, k + 1, block).start()

    def sum_event(layer, half, s, k, side, kind):
        mirrored(lambda here, way: sum_arrive(layer, half, s, k, here, way), side, kind)

    def sum_drain(layer, half, s):
        for k in range(1, n):
            @pl.when(both(z < n - 1, jnp.logical_or(z == 0, k - 1 >= z)))
            def _(k=k):
                sum_copy(layer, half, s, UP, k, 0).wait_send()

            @pl.when(both(z > 0, jnp.logical_or(z == n - 1, k - 1 >= n - 1 - z)))
            def _(k=k):
                sum_copy(layer, half, s, DOWN, k, 0).wait_send()

    def finish(half, s):
        step = 16

        @pl.loop(0, sub // step)
        def _(i):
            r = pl.ds(pl.multiple_of(s * sub + i * step, step), step)
            mine = part[half, s, pl.ds(pl.multiple_of(z * sub + i * step, step), step)]
            home[half, r] = (home[half, r].astype(F32) + mine).astype(BF16)

    barrier = pltpu.get_barrier_semaphore()
    partners = [{axis: ring(i + s, size)} for axis, i, size in (("tp", z, n), ("cp", c, m), ("dp", g, groups)) for s in range(1, size)]
    for partner in partners:
        pl.semaphore_signal(barrier, inc=1, device_id=partner, device_id_type=MESH)
    pl.semaphore_wait(barrier, len(partners))

    def put(half):
        copy = pltpu.make_async_copy(home.at[half], y_out.at[pl.ds(half * rows, rows)], lsem.at[0])
        copy.start()
        copy.wait()

    def last_sends():
        for l, h in halves:
            if l == 0:
                gx[l, h].drain(True)
            for gather in (gx[l, h], go[l, h], gh[l, h, 0], gh[l, h, 1]):
                gather.drain(False)
            for j in range(1, m):
                kv_copy(l, h, j).wait_send()
            if l == layers - 1:
                for s in range(2):
                    sum_drain(l, h, s)
        for l in range(layers):
            wo_start(l, wait=True)
            wo_drain(l)

    actions = {
        "x_start": lambda l, h: gx[l, h].start(), "x": lambda l, h, *more: gx[l, h].event(*more), "norm_x": norm_x,
        "o_start": lambda l, h: go[l, h].start(), "o": lambda l, h, *more: go[l, h].event(*more), "load_o": load_o,
        "h_start": lambda l, h, s: gh[l, h, s].start(), "h": lambda l, h, s, *more: gh[l, h, s].event(*more), "norm_h": norm_h,
        "kv_start": kv_start, "attend": attend, "finish": lambda l, h, s: finish(h, s), "put": lambda l, h: put(h),
        "sum_send": sum_send, "sum": sum_event, "sum_drain": sum_drain,
        "wo_start": lambda l, h: wo_start(l), "wo_groups": lambda l, h: wo_groups(l), "wo_chips": lambda l, h: wo_chips(l),
        "wo_cores": lambda l, h: wo_cores(l), "wo_wait": lambda l, h: wo_wait(l),
    }
    kinds = {"qkv": Qkv, "wo": Wo, "gate": GateUp, "down": Down}
    items = []
    for name, *args in ORDER:
        if name in kinds:
            place, hooks, *late = args
            o = kinds[name](*place)
            hooks = [(-(-tile * o.tiles // TILES[name]), event) for tile, *events in hooks for event in events]
            items.append((name + "_" + "".join(map(str, place)), o, hooks, bool(late)))
        else:
            items.append((name + "_" + "".join(map(str, args)), functools.partial(actions[name], *args), None, False))

    ops = [item for item in items if item[2] is not None]
    base = 0
    for (_, o, _, _), (_, follow, _, late) in zip(ops, ops[1:] + [(None, None, None, True)]):
        o.base, o.follow = base % SLOTS, None if late else follow
        base += o.tiles
    AHEAD = min(SLOTS - 1, *(o.tiles for _, o, _, _ in ops))
    for name, o, hooks, late in items:
        with jax.named_scope(name):
            if hooks is None:
                o()
                continue
            hooks = [(at, functools.partial(actions[event], *args), "E" if event == "sum_send" else args[-1])
                     for at, (event, *args) in hooks]
            if not o.everywhere:
                o.run_inner(hooks, late)
                continue
            if late:
                o.prefetch()
            o.run([(at, event) for at, event, _ in hooks])
    last_sends()


def solution(mesh):
    n = mesh.shape['tp']
    m = mesh.shape['cp']
    groups = mesh.shape['dp']
    row_spec = P(('dp', 'tp', 'cp'), None)
    gain_spec = P(None, None)
    q_spec = P(None, None, 'tp', None)
    col_spec = P(None, None, 'tp')
    o_spec = P(None, 'tp', None, None)
    down_spec = P(None, 'tp', None)

    def body(tokens, norm_attn, norm_mlp, w_q, w_k, w_v, w_o, w_gate, w_up, w_down):
        layers, d, heads, hd = w_q.shape
        rows = tokens.shape[0] // 2
        hc = heads * hd
        width = d // n
        ff = w_gate.shape[2]
        all_rows = n * rows
        c = lax.axis_index('cp')

        inv_freq = 500000.0 ** (-(jnp.arange(hd // 2, dtype=F32) * 2.0 / hd))
        seg = jnp.arange(n) * m + c
        seg = jnp.stack([seg, 2 * n * m - 1 - seg])
        pos = (seg[:, :, None] * rows + jnp.arange(rows)).reshape(2, all_rows)
        angle = pos.astype(F32)[..., None] * inv_freq
        turns = jnp.concatenate([jnp.cos(angle), jnp.sin(angle)], -1)

        hbm = pl.BlockSpec(memory_space=pl.ANY)
        vmem = pl.BlockSpec(memory_space=pltpu.VMEM)
        dma = pltpu.SemaphoreType.DMA
        out = pl.pallas_call(
            functools.partial(kernel, n, m, groups, layers),
            out_shape=(
                jax.ShapeDtypeStruct(tokens.shape, BF16),
                jax.ShapeDtypeStruct((layers, 2, n, rows, d), BF16),
                jax.ShapeDtypeStruct((layers, 2, n, 2, all_rows // 2, hc), BF16),
                jax.ShapeDtypeStruct((layers, 2, 2, 2, all_rows // 2, 2 * width), BF16),
                jax.ShapeDtypeStruct((layers, n * hc, 2 * width), BF16),
            ),
            in_specs=[hbm, vmem, vmem, vmem] + [hbm] * 7,
            out_specs=(hbm,) * 5,
            scratch_shapes=[
                pltpu.VMEM((all_rows, d), BF16),
                pltpu.VMEM((all_rows // 2, ff), BF16),
                pltpu.VMEM((2, 2, all_rows // 2, d), F32),
                pltpu.VMEM((2, 2, 5, rows // 2, d), F32),
                pltpu.VMEM((2 * n, heads * rows, m * rows), F32),
                pltpu.VMEM((2 * n, m * rows, hd), BF16),
                pltpu.VMEM((2 * n, m * rows, hd), BF16),
                pltpu.VMEM((layers, 2, m, all_rows, 2 * hd), BF16),
                pltpu.VMEM((n, heads * rows, hd), BF16),
                pltpu.VMEM((2, 2, all_rows // 2, 2 * width), BF16),
                pltpu.VMEM((2, rows, d), BF16),
                pltpu.VMEM((SLOTS, max(d, ff), TILE), BF16),
                pltpu.VMEM((heads * rows, 128), F32),
                pltpu.VMEM((heads * rows, 128), F32),
                pltpu.VMEM((heads * rows, hd), F32),
                dma((SLOTS, n)),
                dma((2 * n + layers,)),
                dma((layers * 2, 2, n - 1)),
                dma((layers * 2, 2, n - 1)),
                dma((layers * 6, 2, 2)),
                dma((layers * 6, 2, 2)),
                dma((layers, 2, m - 1)),
                dma((layers, 2, m - 1)),
                dma((2, 2, 2, n - 1)),
                dma((2, 2, 2, n - 1)),
                dma((layers, 2)),
                dma((layers, n)),
                dma((layers, n - 1, 4)),
                dma((layers, n - 1, 4)),
            ],
            compiler_params=pltpu.CompilerParams(collective_id=0, has_side_effects=True, vmem_limit_bytes=67043328),
            name="two_layers",
        )(tokens, norm_attn, norm_mlp, turns, jnp.swapaxes(w_q, 1, 2), w_k, w_v, w_o.reshape(layers, hc, d), w_gate, w_up, w_down)
        return out[0]

    return jax.shard_map(
        body,
        mesh=mesh,
        in_specs=(row_spec, gain_spec, gain_spec, q_spec, col_spec, col_spec, o_spec, col_spec, col_spec, down_spec),
        out_specs=row_spec,
        check_vma=False,
    )
```
